32 devices in a mesh: dp: 8 (over y, x, core), tensor: 4 (over z).
Axes of the slice: x: 2, y: 2, z: 4, core: 2. Of those that a mesh axis runs over, the one named last changes fastest.
Arguments:
- tokens_in: bfloat16 [8192, 1024], P(('dp', 'tensor')), may hold values from -6 to 6
- starts: int32 [8, 4], P('dp'), may hold values from 0 to 768, as said below
- ln1_gain: float32 [1024], P(('dp', 'tensor')), may hold values from 0.25 to 1.75
- ln1_bias: float32 [1024], P(('dp', 'tensor')), may hold values from -4 to 4
- w_qkv: bfloat16 [1024, 3072], P('dp', 'tensor'), may hold values from -0.25 to 0.25
- b_qv: bfloat16 [128, 16], P('tensor', 'dp'), may hold values from -6 to 6
- w_out: bfloat16 [1024, 1024], P('tensor', 'dp'), may hold values from -0.75 to 0.75
- b_out: float32 [1024], P(('dp', 'tensor')), may hold values from -6 to 6
- ln2_gain: float32 [1024], P(('dp', 'tensor')), may hold values from 0.25 to 1.75
- ln2_bias: float32 [1024], P(('dp', 'tensor')), may hold values from -4 to 4
- w_up: bfloat16 [1024, 4096], P('dp', 'tensor'), may hold values from -0.1875 to 0.1875
- b_up: bfloat16 [256, 16], P('tensor', 'dp'), may hold values from -6 to 6
- w_down: bfloat16 [4096, 1024], P('tensor', 'dp'), may hold values from -0.09375 to 0.09375
- b_down: float32 [1024], P(('dp', 'tensor')), may hold values from -6 to 6
- grad_out: bfloat16 [8192, 1024], P(('dp', 'tensor')), may hold values from -6 to 6
Outputs:
- output: bfloat16 [8192, 1024], P(('dp', 'tensor'))
- grad_tokens: bfloat16 [8192, 1024], P(('dp', 'tensor'))
- grad_ln1_gain: float32 [1024], P(('dp', 'tensor'))
- grad_ln1_bias: float32 [1024], P(('dp', 'tensor'))
- grad_w_qkv: float32 [1024, 3072], P('dp', 'tensor')
- grad_b_qv: float32 [128, 16], P('tensor', 'dp')
- grad_w_out: float32 [1024, 1024], P('tensor', 'dp')
- grad_b_out: float32 [1024], P(('dp', 'tensor'))
- grad_ln2_gain: float32 [1024], P(('dp', 'tensor'))
- grad_ln2_bias: float32 [1024], P(('dp', 'tensor'))
- grad_w_up: float32 [1024, 4096], P('dp', 'tensor')
- grad_b_up: float32 [256, 16], P('tensor', 'dp')
- grad_w_down: float32 [4096, 1024], P('tensor', 'dp')
- grad_b_down: float32 [1024], P(('dp', 'tensor'))
The draws below stay inside these ranges and needn't reach their ends.
Inputs may be any that keep to these rules, and one draw needn't show every extreme that they name: starts[s, p] lies in the p-th of 4 equal regions of the sequence, and the span of 256 tokens from it ends inside that region.
All inputs are finite; a program needn't handle non-finite values.
Results may differ from the reference program's by a relative error of at most 0.02.
Values may be sent and summed in bfloat16 or wider, within the bound.
A program may use at most 128 MiB of HBM per device.

```python
import jax
import jax.numpy as jnp
from jax import lax

D = 1024
H = 16
HD = 64
FF = 4096
PIECE = 256
NPIC = 4
QBLOCK = 512
SEQ_LEN = 1024
NSEQ = 8
TOKENS = 8192
N_TENSOR = 4


def draw_starts(key, part):
    region = SEQ_LEN // NPIC
    offsets = jax.random.randint(key, (NSEQ, NPIC), 0, region - PIECE + 1, dtype=jnp.int32)
    return (offsets + region * jnp.arange(NPIC, dtype=jnp.int32)[None, :]).astype(jnp.int32)


def block_levels(key, dims, split, smallest, top_value):
    def one(axis_at, shards_of):
        steps = jax.random.uniform(jax.random.fold_in(jax.random.fold_in(key, 6), axis_at), (shards_of,), jnp.float32, smallest / len(split), top_value / len(split))
        return jnp.repeat(jnp.exp(steps), dims[axis_at] // shards_of).reshape((-1,) + (1,) * (len(dims) - axis_at - 1))

    loudness = one(*split[0])
    for cut in split[1:]:
        loudness = loudness * one(*cut)
    return loudness


def centred(rng, extent, deviation, reach, cuts=(), kind=jnp.bfloat16):
    loudness = block_levels(rng, extent, cuts, -0.22, 0.18) if cuts else 1.0
    drawn = jax.random.normal(rng, extent, jnp.float32) * deviation * loudness
    return jnp.minimum(jnp.maximum(drawn, -reach), reach).astype(kind)


def setup_inputs(seed: int = 0) -> dict:
    splits = jax.random.split(jax.random.key(seed), 16)
    tokens_in = centred(splits[0], (TOKENS, D), 1.0, 6.0, ((0, 32),))
    starts = draw_starts(jax.random.fold_in(splits[15], 71), 0)
    ln1_gain = jnp.clip(1.0 + 0.15 * jax.random.normal(splits[2], (D,), jnp.float32), 0.25, 1.75)
    ln1_bias = centred(splits[3], (D,), 0.3, 4.0, ((0, 32),), jnp.float32)
    w_qkv = centred(splits[4], (D, 3 * D), (D // 2) ** -0.5, 0.25, ((0, 8), (1, 4)))
    b_qv = centred(splits[5], (2 * D // 16, 16), 0.5, 6.0, ((0, 4), (1, 8)))
    w_out = centred(splits[6], (D, D), (D // 16) ** -0.5, 0.75, ((0, 4), (1, 8)))
    b_out = centred(splits[7], (D,), 0.5, 6.0, ((0, 32),), jnp.float32)
    ln2_gain = jnp.clip(1.0 + 0.15 * jax.random.normal(splits[8], (D,), jnp.float32), 0.25, 1.75)
    ln2_bias = centred(splits[9], (D,), 0.3, 4.0, ((0, 32),), jnp.float32)
    w_up = centred(splits[10], (D, FF), D ** -0.5, 0.1875, ((0, 8), (1, 4)))
    b_up = centred(splits[11], (FF // 16, 16), 0.5, 6.0, ((0, 4), (1, 8)))
    w_down = centred(splits[12], (FF, D), FF ** -0.5, 0.09375, ((0, 4), (1, 8)))
    b_down = centred(splits[13], (D,), 0.5, 6.0, ((0, 32),), jnp.float32)
    grad_out = centred(splits[14], (TOKENS, D), 1.0, 6.0, ((0, 32),))
    return dict(tokens_in=tokens_in, starts=starts, ln1_gain=ln1_gain, ln1_bias=ln1_bias, w_qkv=w_qkv, b_qv=b_qv, w_out=w_out, b_out=b_out, ln2_gain=ln2_gain, ln2_bias=ln2_bias, w_up=w_up, b_up=b_up, w_down=w_down, b_down=b_down, grad_out=grad_out)


EPS = 1e-05
ROOT = 0.7978845608028654

@jax.custom_vjp
def low(v):
    return lax.optimization_barrier(v.astype(jnp.bfloat16)).astype(jnp.float32)

@jax.custom_vjp
def low_back(v):
    return v

def low_keep(v):
    return (low(v), None)

def low_pass(kept, grad):
    return (grad,)

def back_keep(v):
    return (v, None)

def back_low(kept, grad):
    return (low(grad),)
low.defvjp(low_keep, low_pass)
low_back.defvjp(back_keep, back_low)

def dot_high(left, right):
    return jnp.dot(left, right, precision=lax.Precision.HIGHEST, preferred_element_type=jnp.float32)

def layer_norm(values, gain, shift):
    center = lax.optimization_barrier(jnp.mean(values, axis=-1, keepdims=True))
    shifted = values - center
    spread = lax.optimization_barrier(jnp.mean(shifted * shifted, axis=-1, keepdims=True))
    return shifted * lax.rsqrt(spread + EPS) * gain + shift

def gelu_tanh(values):
    return 0.5 * values * (1.0 + jnp.tanh(ROOT * (values + 0.044715 * values * values * values)))

def group_sum(left, right):
    width = right.shape[0] // N_TENSOR
    total = jnp.zeros((left.shape[0], right.shape[1]), jnp.float32)
    for index in range(N_TENSOR):
        partial_term = dot_high(left[:, index * width:(index + 1) * width], right[index * width:(index + 1) * width])
        total = total + low(partial_term)
    return total

def group_project(normed, weight):
    width = weight.shape[1] // N_TENSOR
    pieces = []
    for index in range(N_TENSOR):
        pieces.append(dot_high(low_back(normed), weight[:, index * width:(index + 1) * width]))
    return jnp.concatenate(pieces, axis=1)

def piece_ids(start_row, length):
    places = jnp.arange(length, dtype=jnp.int32)
    inside = (places[:, None] >= start_row[None, :]) & (places[:, None] < start_row[None, :] + PIECE)
    labels = jnp.arange(1, start_row.shape[0] + 1, dtype=jnp.int32)
    return lax.optimization_barrier(jnp.sum(jnp.where(inside, labels[None, :], 0), axis=1)).astype(jnp.int32)

def allowed_block(row_ids, row_places, key_ids, key_places):
    causal = key_places[None, :] <= row_places[:, None]
    picture = (row_ids[:, None] == key_ids[None, :]) & (row_ids[:, None] > 0)
    return causal | picture

def forward(hidden_in, key_ids, params):
    gain_one, shift_one, weight_qkv, bias_qv, weight_out, bias_out, gain_two, shift_two, weight_up, bias_up, weight_down, bias_down = params
    length = hidden_in.shape[0]
    normed_one = low(layer_norm(hidden_in, gain_one, shift_one))
    bias_pair = bias_qv.reshape(H, 2, HD)
    full_bias = jnp.stack([bias_pair[:, 0], jnp.zeros_like(bias_pair[:, 0]), bias_pair[:, 1]], axis=1)
    projected = low_back(low(group_project(normed_one, weight_qkv).reshape(length, H, 3, HD) + full_bias))
    query_all = projected[:, :, 0]
    key_all = projected[:, :, 1]
    value_all = projected[:, :, 2]
    places = jnp.arange(length, dtype=jnp.int32)

    def attend(block_index):
        first_row = block_index * QBLOCK
        query_rows = lax.dynamic_slice_in_dim(query_all, first_row, QBLOCK, 0)
        row_places = first_row + jnp.arange(QBLOCK, dtype=jnp.int32)
        row_ids = lax.dynamic_slice_in_dim(key_ids, first_row, QBLOCK, 0)
        scores = jnp.einsum('qhd,khd->hqk', query_rows, key_all, precision=lax.Precision.HIGHEST) * 0.125
        scores = low_back(scores)
        scores = jnp.where(allowed_block(row_ids, row_places, key_ids, places)[None], scores, -1e+30)
        probs = jax.nn.softmax(scores, axis=-1)
        return jnp.einsum('hqk,khd->qhd', low(probs), value_all, precision=lax.Precision.HIGHEST)
    blocks = lax.map(jax.checkpoint(attend), jnp.arange(length // QBLOCK, dtype=jnp.int32))
    heads_out = low_back(low(blocks.reshape(length, D)))
    middle = hidden_in + (low_back(group_sum(heads_out, weight_out)) + bias_out)
    normed_two = low(layer_norm(middle, gain_two, shift_two))
    up_proj = low_back(group_project(normed_two, weight_up) + bias_up)
    hidden_act = low(gelu_tanh(up_proj))
    return middle + low_back(group_sum(hidden_act, weight_down)) + bias_down

def reference(tokens_in, starts, ln1_gain, ln1_bias, w_qkv, b_qv, w_out, b_out, ln2_gain, ln2_bias, w_up, b_up, w_down, b_down, grad_out):
    params = (ln1_gain, ln1_bias, w_qkv.astype(jnp.float32), b_qv.astype(jnp.float32).reshape(2 * D), w_out.astype(jnp.float32), b_out, ln2_gain, ln2_bias, w_up.astype(jnp.float32), b_up.astype(jnp.float32).reshape(FF), w_down.astype(jnp.float32), b_down)
    inputs = tokens_in.astype(jnp.float32).reshape(NSEQ, SEQ_LEN, D)
    cotangent = grad_out.astype(jnp.float32).reshape(NSEQ, SEQ_LEN, D)

    def one_seq(carry, item):
        seq_input, seq_grad, start_row = item
        key_ids = piece_ids(start_row, SEQ_LEN)
        result, pull = jax.vjp(lambda hidden_in, weights: forward(hidden_in, key_ids, weights), seq_input, params)
        grad_input, grad_params = pull(seq_grad)
        return (jax.tree.map(jnp.add, carry, grad_params), (result, grad_input))
    zeros = jax.tree.map(jnp.zeros_like, params)
    totals, (results, grad_inputs) = lax.scan(one_seq, zeros, (inputs, cotangent, starts))
    return (results.reshape(TOKENS, D).astype(jnp.bfloat16), grad_inputs.reshape(TOKENS, D).astype(jnp.bfloat16), totals[0], totals[1], totals[2], totals[3].reshape(2 * D // 16, 16), totals[4], totals[5], totals[6], totals[7], totals[8], totals[9].reshape(FF // 16, 16), totals[10], totals[11])
```

```python
import functools

import jax
import jax.numpy as jnp
from jax import lax
from jax.experimental import pallas as pl
from jax.experimental.pallas import tpu as pltpu
from jax.sharding import PartitionSpec as P

HD = 64
PIECE = 256
QBLOCK = 512


EPS = 1e-05
ROOT = 0.7978845608028654


def gelu_tanh(values):
    return 0.5 * values * (1.0 + jnp.tanh(ROOT * (values + 0.044715 * values * values * values)))


def normalize(values):
    center = jnp.mean(values, axis=-1, keepdims=True)
    shifted = values - center
    inverse = lax.rsqrt(jnp.mean(shifted * shifted, axis=-1, keepdims=True) + EPS)
    return (shifted * inverse, inverse)


def norm_back(grad_normed, normed, inverse, gain):
    scaled = grad_normed * gain
    return inverse * (
        scaled
        - jnp.mean(scaled, axis=-1, keepdims=True)
        - normed * jnp.mean(scaled * normed, axis=-1, keepdims=True)
    )


def dot_last(left, right):
    return lax.dot_general(
        left, right, (((1,), (1,)), ((), ())), preferred_element_type=jnp.float32
    )


def dot_first(left, right):
    return lax.dot_general(
        left, right, (((0,), (0,)), ((), ())), preferred_element_type=jnp.float32
    )


def gather_rows(values):
    return lax.all_gather(values, "tensor", axis=0, tiled=True)


def gather_grads(values):
    return lax.all_gather(values, "tensor", axis=0, tiled=True)


def reduce_rows(left, weight, rows):

    def term(start, count):
        return jnp.dot(left, weight, preferred_element_type=jnp.float32)

    return lax.psum_scatter(
        term(jnp.int32(0), lax.axis_size("tensor") * rows).astype(jnp.bfloat16),
        "tensor",
        scatter_dimension=0,
        tiled=True,
    ).astype(jnp.float32)


def reduce_grads(left, weight, rows):

    def term(start, count):
        return dot_last(left, weight)

    return lax.psum_scatter(
        term(jnp.int32(0), lax.axis_size("tensor") * rows).astype(jnp.bfloat16),
        "tensor",
        scatter_dimension=0,
        tiled=True,
    ).astype(jnp.float32)


def piece_ids(start_row, length):
    places = jnp.arange(length, dtype=jnp.int32)
    inside = (places[:, None] >= start_row[None, :]) & (
        places[:, None] < start_row[None, :] + PIECE
    )
    labels = jnp.arange(1, start_row.shape[0] + 1, dtype=jnp.int32)
    return jnp.sum(jnp.where(inside, labels[None, :], 0), axis=1)


def allowed_block(row_ids, row_places, key_ids, key_places):
    causal = key_places[None, :] <= row_places[:, None]
    picture = (row_ids[:, None] == key_ids[None, :]) & (row_ids[:, None] > 0)
    return causal | picture


def block_scores(by_seq, start_rows, block_index):
    length = by_seq.shape[1]
    per_seq = length // QBLOCK
    seq_index = block_index // per_seq
    first_row = block_index % per_seq * QBLOCK
    sequence = lax.dynamic_index_in_dim(by_seq, seq_index, 0, keepdims=False)
    key_ids = piece_ids(lax.dynamic_index_in_dim(start_rows, seq_index, 0, keepdims=False), length)
    query_rows = lax.dynamic_slice_in_dim(sequence, first_row, QBLOCK, 0)[:, :, 0]
    key_rows = sequence[:, :, 1]
    value_rows = sequence[:, :, 2]
    row_ids = lax.dynamic_slice_in_dim(key_ids, first_row, QBLOCK, 0)
    row_places = first_row + jnp.arange(QBLOCK, dtype=jnp.int32)
    scores = (
        jnp.einsum("qhd,khd->hqk", query_rows, key_rows, preferred_element_type=jnp.float32) * 0.125
    )
    places = jnp.arange(length, dtype=jnp.int32)
    scores = jnp.where(allowed_block(row_ids, row_places, key_ids, places)[None], scores, -1e30)
    return (seq_index, first_row, query_rows, key_rows, value_rows, scores)


def attention_forward(by_seq, start_rows):
    total_blocks = by_seq.shape[0] * (by_seq.shape[1] // QBLOCK)

    def attend(block_index):
        _, _, query_rows, key_rows, value_rows, scores = block_scores(
            by_seq, start_rows, block_index
        )
        peak = jnp.max(scores, axis=-1, keepdims=True)
        log_total = peak + jnp.log(jnp.sum(jnp.exp(scores - peak), axis=-1, keepdims=True))
        probs = jnp.exp(scores - log_total)
        heads = jnp.einsum(
            "hqk,khd->qhd",
            probs.astype(jnp.bfloat16),
            value_rows,
            preferred_element_type=jnp.float32,
        )
        return (heads.astype(jnp.bfloat16), log_total)

    return lax.map(attend, jnp.arange(total_blocks, dtype=jnp.int32))


def attention_backward(by_seq, start_rows, log_totals, grad_heads):
    total_blocks = by_seq.shape[0] * (by_seq.shape[1] // QBLOCK)
    empty = jnp.zeros(by_seq.shape[:3] + (HD,), jnp.float32)

    def step(carry, item):
        grad_keys, grad_values = carry
        block_index, log_total = item
        seq_index, first_row, query_rows, key_rows, value_rows, scores = block_scores(
            by_seq, start_rows, block_index
        )
        grad_seq = lax.dynamic_index_in_dim(grad_heads, seq_index, 0, keepdims=False)
        grad_rows = lax.dynamic_slice_in_dim(grad_seq, first_row, QBLOCK, 0)
        probs = jnp.exp(scores - log_total)
        grad_probs = jnp.einsum(
            "qhd,khd->hqk", grad_rows, value_rows, preferred_element_type=jnp.float32
        )
        inner = jnp.sum(probs * grad_probs, axis=-1, keepdims=True)
        grad_scores = (probs * (grad_probs - inner)).astype(jnp.bfloat16)
        grad_query = (
            jnp.einsum("hqk,khd->qhd", grad_scores, key_rows, preferred_element_type=jnp.float32)
            * 0.125
        )
        key_term = (
            jnp.einsum("hqk,qhd->khd", grad_scores, query_rows, preferred_element_type=jnp.float32)
            * 0.125
        )
        value_term = jnp.einsum(
            "hqk,qhd->khd",
            probs.astype(jnp.bfloat16),
            grad_rows,
            preferred_element_type=jnp.float32,
        )
        grad_keys = lax.dynamic_update_index_in_dim(
            grad_keys,
            lax.dynamic_index_in_dim(grad_keys, seq_index, 0, keepdims=False) + key_term,
            seq_index,
            0,
        )
        grad_values = lax.dynamic_update_index_in_dim(
            grad_values,
            lax.dynamic_index_in_dim(grad_values, seq_index, 0, keepdims=False) + value_term,
            seq_index,
            0,
        )
        return ((grad_keys, grad_values), grad_query)

    (grad_keys, grad_values), grad_query = lax.scan(
        step, (empty, empty), (jnp.arange(total_blocks, dtype=jnp.int32), log_totals)
    )
    return (grad_query, grad_keys, grad_values)


def per_device(
    tokens_in,
    starts,
    ln1_gain,
    ln1_bias,
    w_qkv,
    b_qv,
    w_out,
    b_out,
    ln2_gain,
    ln2_bias,
    w_up,
    b_up,
    w_down,
    b_down,
    grad_out,
):
    rows = tokens_in.shape[0]
    gain_one, shift_one, bias_out, gain_two, shift_two, bias_down = (
        lax.all_gather(ln1_gain, ("dp", "tensor"), axis=0, tiled=True),
        lax.all_gather(ln1_bias, ("dp", "tensor"), axis=0, tiled=True),
        lax.all_gather(b_out, ("dp", "tensor"), axis=0, tiled=True),
        lax.all_gather(ln2_gain, ("dp", "tensor"), axis=0, tiled=True),
        lax.all_gather(ln2_bias, ("dp", "tensor"), axis=0, tiled=True),
        lax.all_gather(b_down, ("dp", "tensor"), axis=0, tiled=True),
    )
    weight_qkv, bias_qv, weight_out = (
        lax.all_gather(w_qkv, "dp", axis=0, tiled=True),
        lax.all_gather(b_qv, "dp", axis=1, tiled=True),
        lax.all_gather(w_out, "dp", axis=1, tiled=True),
    )
    weight_up, bias_up, weight_down = (
        lax.all_gather(w_up, "dp", axis=0, tiled=True),
        lax.all_gather(b_up, "dp", axis=1, tiled=True),
        lax.all_gather(w_down, "dp", axis=1, tiled=True),
    )
    local_heads = weight_qkv.shape[1] // (3 * HD)
    seq_count = starts.shape[0]
    inputs = tokens_in.astype(jnp.float32)
    normed_one, inverse_one = normalize(inputs)
    gathered_one = gather_rows((normed_one * gain_one + shift_one).astype(jnp.bfloat16))
    group = gathered_one.shape[0]
    length = group // seq_count
    bias_pair = bias_qv.astype(jnp.float32).reshape(local_heads, 2, HD)
    full_bias = jnp.stack(
        [bias_pair[:, 0], jnp.zeros_like(bias_pair[:, 0]), bias_pair[:, 1]], axis=1
    )
    projected = (
        jnp.dot(gathered_one, weight_qkv, preferred_element_type=jnp.float32).reshape(
            group, local_heads, 3, HD
        )
        + full_bias
    ).astype(jnp.bfloat16)
    by_seq = projected.reshape(seq_count, length, local_heads, 3, HD)
    heads_blocks, log_totals = attention_forward(by_seq, starts)
    heads_out = heads_blocks.reshape(group, local_heads * HD)
    middle = inputs + (reduce_rows(heads_out, weight_out, rows) + bias_out)
    normed_two, inverse_two = normalize(middle)
    rounded_two = (normed_two * gain_two + shift_two).astype(jnp.bfloat16)
    grad_final = grad_out.astype(jnp.float32)
    grad_bias_down = jnp.sum(grad_final, axis=0)
    gathered_two = gather_rows(rounded_two)
    up_proj = jnp.dot(gathered_two, weight_up, preferred_element_type=jnp.float32) + bias_up.astype(
        jnp.float32
    ).reshape(-1)
    hidden_act, gelu_pull = jax.vjp(gelu_tanh, up_proj)
    hidden_low = hidden_act.astype(jnp.bfloat16)
    output = (middle + reduce_rows(hidden_low, weight_down, rows) + bias_down).astype(jnp.bfloat16)
    grad_branch = gather_grads(grad_out)
    grad_w_down = dot_first(hidden_low, grad_branch)
    grad_up = gelu_pull(dot_last(grad_branch, weight_down))[0].astype(jnp.bfloat16)
    grad_b_up = jnp.sum(grad_up, axis=0, dtype=jnp.float32).reshape(bias_up.shape)
    grad_w_up = dot_first(gathered_two, grad_up)
    grad_two = reduce_grads(grad_up, weight_up, rows)
    grad_w_up, grad_b_up, grad_w_down = (
        lax.psum_scatter(
            grad_w_up.astype(jnp.bfloat16), "dp", scatter_dimension=0, tiled=True
        ).astype(jnp.float32),
        lax.psum_scatter(
            grad_b_up.astype(jnp.bfloat16), "dp", scatter_dimension=1, tiled=True
        ).astype(jnp.float32),
        lax.psum_scatter(
            grad_w_down.astype(jnp.bfloat16), "dp", scatter_dimension=1, tiled=True
        ).astype(jnp.float32),
    )
    grad_gain_two = jnp.sum(grad_two * normed_two, axis=0)
    grad_shift_two = jnp.sum(grad_two, axis=0)
    grad_middle = grad_final + norm_back(grad_two, normed_two, inverse_two, gain_two)
    grad_bias_out = jnp.sum(grad_middle, axis=0)
    grad_attn = gather_grads(grad_middle.astype(jnp.bfloat16))
    grad_w_out = dot_first(heads_out, grad_attn)
    grad_heads = (
        dot_last(grad_attn, weight_out)
        .astype(jnp.bfloat16)
        .reshape(seq_count, length, local_heads, HD)
    )
    grad_query, grad_keys, grad_values = attention_backward(by_seq, starts, log_totals, grad_heads)
    grad_proj = jnp.stack(
        [
            grad_query.reshape(group, local_heads, HD),
            grad_keys.reshape(group, local_heads, HD),
            grad_values.reshape(group, local_heads, HD),
        ],
        axis=2,
    ).astype(jnp.bfloat16)
    grad_b_qv = jnp.sum(grad_proj[:, :, 0::2], axis=0, dtype=jnp.float32).reshape(bias_qv.shape)
    grad_flat = grad_proj.reshape(group, 3 * local_heads * HD)
    grad_w_qkv = dot_first(gathered_one, grad_flat)
    grad_one = reduce_grads(grad_flat, weight_qkv, rows)
    grad_w_qkv, grad_b_qv, grad_w_out = (
        lax.psum_scatter(
            grad_w_qkv.astype(jnp.bfloat16), "dp", scatter_dimension=0, tiled=True
        ).astype(jnp.float32),
        lax.psum_scatter(
            grad_b_qv.astype(jnp.bfloat16), "dp", scatter_dimension=1, tiled=True
        ).astype(jnp.float32),
        lax.psum_scatter(
            grad_w_out.astype(jnp.bfloat16), "dp", scatter_dimension=1, tiled=True
        ).astype(jnp.float32),
    )
    grad_gain_one = jnp.sum(grad_one * normed_one, axis=0)
    grad_shift_one = jnp.sum(grad_one, axis=0)
    grad_tokens = (grad_middle + norm_back(grad_one, normed_one, inverse_one, gain_one)).astype(
        jnp.bfloat16
    )
    summed = (
        lax.psum_scatter(grad_gain_one, ("dp", "tensor"), scatter_dimension=0, tiled=True),
        lax.psum_scatter(grad_shift_one, ("dp", "tensor"), scatter_dimension=0, tiled=True),
        lax.psum_scatter(grad_bias_out, ("dp", "tensor"), scatter_dimension=0, tiled=True),
        lax.psum_scatter(grad_gain_two, ("dp", "tensor"), scatter_dimension=0, tiled=True),
        lax.psum_scatter(grad_shift_two, ("dp", "tensor"), scatter_dimension=0, tiled=True),
        lax.psum_scatter(grad_bias_down, ("dp", "tensor"), scatter_dimension=0, tiled=True),
    )
    return (
        output,
        grad_tokens,
        summed[0],
        summed[1],
        grad_w_qkv,
        grad_b_qv,
        grad_w_out,
        summed[2],
        summed[3],
        summed[4],
        grad_w_up,
        grad_b_up,
        grad_w_down,
        summed[5],
    )


MESH = pl.DeviceIdType.MESH
CH = 2


class Fused:
    def __init__(self, names, refs):
        for name, ref in zip(names, refs):
            setattr(self, name, ref)
        self.next_sem = 0
        self.unsent = []
        self.groups = {0: [], 1: []}
        dp, self.z = lax.axis_index("dp"), lax.axis_index("tensor")
        self.y, self.x, self.c = dp // 4, (dp // 2) % 2, dp % 2
        self.j = 2 * self.x + self.c
        self.q = self.quarter(self.j)
        self.sib = self.dev(self.y, self.x, 1 - self.c, self.z)
        self.across = self.dev(self.y, 1 - self.x, self.c, self.z)
        self.q_sib = self.quarter(2 * self.x + 1 - self.c)
        self.q_x = self.quarter(2 * (1 - self.x) + self.c)
        self.q_d = self.quarter(2 * (1 - self.x) + 1 - self.c)
        self.rows = self.tok.shape[0]
        self.width = self.tok.shape[1]
        self.part = self.width // 8

    def dev(self, y, x, c, z):
        return ((y * 2 + x) * 2 + c, z)

    def quarter(self, member):
        return (member - self.z + 4) % 4

    def sem(self):
        index = self.next_sem
        self.next_sem += 1
        return index

    def copy(self, src, dst, device, index):
        return pltpu.make_async_remote_copy(
            src_ref=src,
            dst_ref=dst,
            send_sem=self.ssem.at[index],
            recv_sem=self.rsem.at[index],
            device_id=device,
            device_id_type=MESH,
        )

    def send(self, src, dst, device, index, group=None):
        copy = self.copy(src, dst, device, index)
        copy.start()
        (self.unsent if group is None else self.groups[group]).append(copy)

    def arrived(self, dst, index):
        self.copy(dst, dst, self.sib, index).wait_recv()

    def drain(self):
        for copy in self.unsent + self.groups[0] + self.groups[1]:
            copy.wait_send()

    def at_quarter(self, quarter, chunk=None):
        if chunk is None:
            return pl.ds(pl.multiple_of(quarter * self.rows, self.rows), self.rows)
        size = self.rows // CH
        return pl.ds(pl.multiple_of(quarter * self.rows + chunk * size, size), size)

    def at_chunk(self, chunk):
        size = self.rows // CH
        return pl.ds(chunk * size, size)

    def barrier(self):
        me = lax.axis_index("dp") * 4 + self.z
        bar = pltpu.get_barrier_semaphore()

        def greet(step, carry):
            other = (me + step) % 32
            pl.semaphore_signal(
                bar, inc=1, device_id=(other // 4, other % 4), device_id_type=MESH
            )
            return carry

        lax.fori_loop(1, 32, greet, 0)
        pl.semaphore_wait(bar, 31)

    def homes(self):
        plane = 2 * self.y + self.x
        member = (plane + self.z) % 4
        worker = (self.c, member // 2, member % 2, plane)
        owner = (self.z // 2, self.z % 2, self.y, self.q)
        same = (
            (worker[0] == self.y)
            & (worker[1] == self.x)
            & (worker[2] == self.c)
            & (worker[3] == self.z)
        )
        return self.dev(*worker), self.dev(*owner), same

    def move_start(self, src, dst, outward, index):
        worker, owner, same = self.homes()
        copy = self.copy(src, dst, worker if outward else owner, index)
        local = pltpu.make_async_copy(src, dst, self.lsem.at[index])

        @pl.when(jnp.logical_not(same))
        def _():
            copy.start()

        @pl.when(same)
        def _():
            local.start()

    def move_wait(self, src, dst, index):
        same = self.homes()[2]
        copy = self.copy(src, dst, self.sib, index)
        local = pltpu.make_async_copy(src, dst, self.lsem.at[index])

        @pl.when(jnp.logical_not(same))
        def _():
            copy.wait_send()
            copy.wait_recv()

        @pl.when(same)
        def _():
            local.wait()

    def span(self, half):
        return pl.ds(pl.multiple_of(half * 4 * self.part, 4 * self.part), 4 * self.part)

    def place(self, source):
        return pl.ds(pl.multiple_of(source * self.part, self.part), self.part)

    def cut(self, kind, ref, zc, where):
        if kind == "q":
            return ref.at[:, zc, :, where]
        if kind == "u":
            return ref.at[zc, where, :]
        return ref.at[zc, :, where]

    def piece(self, kind, ref, member):
        if kind == "u":
            wide = self.wbuf["u"].shape[2]
            return ref.at[:, pl.ds(pl.multiple_of(member * wide, wide), wide)]
        return ref.at[member]

    def weights_one(self, kind):
        source = self.dev(self.y, self.x, self.c, self.z)[0]
        here = self.cut(kind, self.wbuf[kind], self.z, self.place(source))
        self.one[kind] = []
        for step in range(1, 4):
            member = (self.j + step) % 4
            index = self.sem()
            self.send(
                self.piece(kind, self.shard[kind], member),
                here,
                self.dev(self.y, member // 2, member % 2, self.z),
                index,
            )
            sender = self.y * 4 + (self.j - step + 4) % 4
            self.one[kind].append(
                (self.cut(kind, self.wbuf[kind], self.z, self.place(sender)), index)
            )
        index = self.sem()
        local = pltpu.make_async_copy(
            self.piece(kind, self.shard[kind], self.j), here, self.lsem.at[index]
        )
        local.start()
        self.own[kind] = local

    def weights_two(self, kind):
        self.own[kind].wait()
        for view, index in self.one[kind]:
            self.arrived(view, index)
        mine = self.cut(kind, self.wbuf[kind], self.z, self.span(self.y))
        self.two[kind] = []
        for step in range(1, 4):
            plane = (self.z + step) % 4
            index = self.sem()
            self.send(mine, mine, self.dev(self.y, self.x, self.c, plane), index)
            self.two[kind].append(((self.z - step + 4) % 4, index))
        self.three[kind] = []
        self.weights_cross(kind, self.z)

    def weights_cross(self, kind, plane):
        index = self.sem()
        mine = self.cut(kind, self.wbuf[kind], plane, self.span(self.y))
        self.send(mine, mine, self.dev(1 - self.y, self.x, self.c, self.z), index)
        self.three[kind].append((plane, index))

    def weights_three(self, kind):
        for plane, index in self.two[kind]:
            self.arrived(self.cut(kind, self.wbuf[kind], plane, self.span(self.y)), index)
            self.weights_cross(kind, plane)

    def weights_done(self, kind):
        for plane, index in self.three[kind]:
            self.arrived(self.cut(kind, self.wbuf[kind], plane, self.span(1 - self.y)), index)

    def grads_one(self, kind):
        index = self.sem()
        self.back[kind] = index
        for plane in range(4):
            away = self.cut(kind, self.dbuf[kind], plane, self.span(1 - self.y))
            there = self.cut(kind, self.ybuf[kind], plane, slice(None))
            use = index if plane == 0 else self.sem()
            self.send(away, there, self.dev(1 - self.y, self.x, self.c, self.z), use)
            self.backs.setdefault(kind, []).append(use)

    def grads_two(self, kind):
        for plane in range(4):
            there = self.cut(kind, self.ybuf[kind], plane, slice(None))
            self.arrived(there, self.backs[kind][plane])
            mine = self.cut(kind, self.dbuf[kind], plane, self.span(self.y))
            mine[...] = (
                mine[...].astype(jnp.float32) + there[...].astype(jnp.float32)
            ).astype(jnp.bfloat16)
        self.swaps[kind] = []
        for step in range(1, 4):
            plane = (self.z + step) % 4
            index = self.sem()
            self.send(
                self.cut(kind, self.dbuf[kind], plane, self.span(self.y)),
                self.zbuf[kind].at[step - 1],
                self.dev(self.y, self.x, self.c, plane),
                index,
            )
            self.swaps[kind].append(index)

    def grads_three(self, kind):
        mine = self.cut(kind, self.dbuf[kind], self.z, self.span(self.y))
        total = mine[...].astype(jnp.float32)
        for step in range(1, 4):
            there = self.zbuf[kind].at[step - 1]
            self.arrived(there, self.swaps[kind][step - 1])
            total = total + there[...].astype(jnp.float32)
        final = self.fbuf[kind]
        final[...] = total.astype(jnp.bfloat16)
        ends = self.ebuf[kind]
        self.last[kind] = []
        for step in range(1, 4):
            member = (self.j + step) % 4
            index = self.sem()
            self.send(
                self.slab(kind, final, member),
                ends.at[self.j],
                self.dev(self.y, member // 2, member % 2, self.z),
                index,
            )
            self.last[kind].append(((self.j - step + 4) % 4, index))
        index = self.sem()
        local = pltpu.make_async_copy(
            self.slab(kind, final, self.j), ends.at[self.j], self.lsem.at[index]
        )
        local.start()
        self.own[kind] = local

    def slab(self, kind, ref, member):
        where = pl.ds(pl.multiple_of(member * self.part, self.part), self.part)
        if kind == "q":
            return ref.at[:, :, where]
        if kind == "u":
            return ref.at[where, :]
        return ref.at[:, where]

    def grads_done(self, kind):
        self.own[kind].wait()
        for member, index in self.last[kind]:
            self.arrived(self.ebuf[kind].at[member], index)

    def gather_plan(self):
        return {kind: [self.sem() for _ in range(CH)] for kind in ("across", "sib", "pass")}

    def gather_send(self, buf, plan, chunk):
        rows = self.at_quarter(self.q, chunk)
        self.send(buf.at[rows], buf.at[rows], self.across, plan["across"][chunk])
        self.send(buf.at[rows], buf.at[rows], self.sib, plan["sib"][chunk])

    def gather_pass(self, buf, plan):
        for chunk in range(CH):
            rows = self.at_quarter(self.q_x, chunk)
            self.arrived(buf.at[rows], plan["across"][chunk])
            self.send(buf.at[rows], buf.at[rows], self.sib, plan["pass"][chunk])

    def gather_sib(self, buf, plan):
        for chunk in range(CH):
            self.arrived(buf.at[self.at_quarter(self.q_sib, chunk)], plan["sib"][chunk])

    def gather_last(self, buf, plan):
        for chunk in range(CH):
            self.arrived(buf.at[self.at_quarter(self.q_d, chunk)], plan["pass"][chunk])

    def gathered(self, buf, plan, use):
        use(self.q)
        self.gather_sib(buf, plan)
        use(self.q_sib)
        self.gather_pass(buf, plan)
        use(self.q_x)
        self.gather_last(buf, plan)
        use(self.q_d)

    def scatter_start(self, partial, own, which, rx):
        sa, ra, sb, sc, rb = (self.rs.at[which, slot] for slot in range(5))
        plan = [[self.sem() for _ in range(CH)] for _ in range(3)]
        low = jnp.bfloat16
        for copy in self.groups[which]:
            copy.wait_send()
        self.groups[which] = []
        sa[...] = partial(self.q_d).astype(low)
        for chunk in range(CH):
            rows = self.at_chunk(chunk)
            self.send(sa.at[rows], ra.at[rows], self.sib, plan[0][chunk], which)
        held = partial(self.q_x)
        for chunk in range(CH):
            self.arrived(ra.at[self.at_chunk(chunk)], plan[0][chunk])
        sb[...] = (held + ra[...].astype(jnp.float32)).astype(low)
        for chunk in range(CH):
            rows = self.at_chunk(chunk)
            self.send(sb.at[rows], rx.at[rows], self.across, plan[1][chunk], which)
        sc[...] = partial(self.q_sib).astype(low)
        for chunk in range(CH):
            rows = self.at_chunk(chunk)
            self.send(sc.at[rows], rb.at[rows], self.sib, plan[2][chunk], which)
        own[...] = partial(self.q)
        return plan, which, rx

    def scatter_chunk(self, started, own, chunk):
        plan, which, rx = started
        rows = self.at_chunk(chunk)
        rb = self.rs.at[which, 4]
        self.arrived(rb.at[rows], plan[2][chunk])
        self.arrived(rx.at[rows], plan[1][chunk])
        return (
            own[rows, :] + rb[rows, :].astype(jnp.float32) + rx[rows, :].astype(jnp.float32)
        )

    def run(self):
        f32, low = jnp.float32, jnp.bfloat16
        rows, width = self.rows, self.width
        quarters = range(4)
        self.wbuf = dict(q=self.wq, o=self.wo, u=self.wu, d=self.wd)
        self.shard = dict(q=self.in_q, o=self.in_o, u=self.in_u, d=self.in_d)
        self.dbuf = dict(q=self.dq, o=self.do, u=self.du, d=self.dd)
        self.ybuf = dict(q=self.yq, o=self.yo, u=self.yu, d=self.yd)
        self.zbuf = dict(q=self.zq, o=self.zo, u=self.zu, d=self.zd)
        self.fbuf = dict(q=self.fq, o=self.fo, u=self.fu, d=self.fd)
        self.ebuf = dict(q=self.eq, o=self.eo, u=self.eu, d=self.ed)
        self.one, self.two, self.three, self.own = {}, {}, {}, {}
        self.back, self.backs, self.swaps, self.last = {}, {}, {}, {}
        gain_one, shift_one = self.small[0:1, :], self.small[1:2, :]
        bias_out = self.small[2:3, :]
        gain_two, shift_two = self.small[3:4, :], self.small[4:5, :]
        bias_down = self.small[5:6, :]
        heads, dim = self.qh.shape[0], self.qh.shape[2]
        hidden = self.wu.shape[2]

        self.barrier()
        move = [self.sem() for _ in range(4)]
        self.move_start(self.tok, self.xs, True, move[0])
        for kind in "qoud":
            self.weights_one(kind)
        plan_one, plan_two, plan_go, plan_mid = (self.gather_plan() for _ in range(4))
        self.weights_two("q")
        self.move_wait(self.tok, self.xs, move[0])

        for chunk in range(CH):
            part = self.at_chunk(chunk)
            normed, inverse = normalize(self.xs[part, :].astype(f32))
            self.n1[part, :] = normed
            self.i1[part, :] = inverse
            self.h1[self.at_quarter(self.q, chunk), :] = (normed * gain_one + shift_one).astype(low)
            self.gather_send(self.h1, plan_one, chunk)
        for kind in "ou":
            self.weights_two(kind)
        self.move_start(self.go, self.gx, True, move[1])
        self.weights_two("d")
        self.mask_blocks()
        self.weights_three("q")
        self.gather_sib(self.h1, plan_one)
        self.gather_pass(self.h1, plan_one)
        self.weights_done("q")
        self.gather_last(self.h1, plan_one)

        def project(block, carry):
            place = pl.ds(pl.multiple_of(block * rows, rows), rows)
            weight = self.wq[...].reshape(3 * heads * dim, width)
            both = dot_last(self.h1[place, :], weight) + self.bq[...]
            for head in range(heads):
                for slot, ref in enumerate((self.qh, self.kh, self.vh)):
                    first = (slot * heads + head) * dim
                    value = both[:, first : first + dim].astype(low)
                    if slot == 0:
                        value = (value.astype(f32) * 0.125).astype(low)
                    ref[head, place, :] = value
            return carry

        lax.fori_loop(0, 4, project, 0)
        self.weights_three("o")

        def parts_of(block):
            return ([(0, block * rows)] if block else []) + [(block * rows, rows)]

        def attend(head, carry):
            for block in quarters:
                place = pl.ds(block * rows, rows)
                query = self.qh[head, place, :]
                scores = []
                for first, count in parts_of(block):
                    value = dot_last(query, self.kh[head, pl.ds(first, count), :])
                    if first == block * rows:
                        value = value + self.mk[block].astype(f32)
                    scores.append(value)
                peak = functools.reduce(
                    jnp.maximum, [jnp.max(value, axis=1, keepdims=True) for value in scores]
                )
                powers = [jnp.exp(value - peak) for value in scores]
                total = sum(jnp.sum(value, axis=1, keepdims=True) for value in powers)
                scale = 1.0 / total
                result = 0.0
                for (first, count), value in zip(parts_of(block), powers):
                    probs = (value * scale).astype(low)
                    self.pb[block][head, :, pl.ds(first, count)] = probs
                    result = result + jnp.dot(
                        probs,
                        self.vh[head, pl.ds(first, count), :],
                        preferred_element_type=f32,
                    )
                self.hh[head, place, :] = result.astype(low)
            return carry

        lax.fori_loop(0, heads, attend, 0)

        def assemble(target, refs, count):
            def one(block, carry):
                place = pl.ds(pl.multiple_of(block * rows, rows), rows)
                pieces = [ref[head, place, :] for ref in refs for head in range(count)]
                target[place, :] = jnp.concatenate(pieces, axis=1)
                return carry

            lax.fori_loop(0, 4, one, 0)

        assemble(self.ho, (self.hh,), heads)
        self.weights_done("o")
        self.weights_three("u")

        flat_out = lambda: self.wo[...].reshape(heads * dim, width)
        started = self.scatter_start(
            lambda quarter: jnp.dot(
                self.ho[self.at_quarter(quarter), :], flat_out(), preferred_element_type=f32
            ),
            self.own_a,
            0,
            self.rx.at[0],
        )
        for chunk in range(CH):
            part = self.at_chunk(chunk)
            summed = self.scatter_chunk(started, self.own_a, chunk)
            middle = self.xs[part, :].astype(f32) + (summed + bias_out)
            self.mid[part, :] = middle
            normed, inverse = normalize(middle)
            self.n2[part, :] = normed
            self.i2[part, :] = inverse
            self.h2[self.at_quarter(self.q, chunk), :] = (normed * gain_two + shift_two).astype(low)
            self.gather_send(self.h2, plan_two, chunk)
        self.weights_three("d")
        self.weights_done("u")

        def up(quarter):
            place = self.at_quarter(quarter)

            for block in range(4):
                lanes = pl.ds(block * hidden, hidden)
                value = (
                    jnp.dot(self.h2[place, :], self.wu[block], preferred_element_type=f32)
                    + self.bu[:, lanes]
                )
                square = value * value
                bend = jnp.tanh(ROOT * (value + 0.044715 * value * square))
                self.hid[place, lanes] = (0.5 * value * (1.0 + bend)).astype(low)
                slope = 0.5 * (1.0 + bend) + 0.5 * value * (1.0 - bend * bend) * ROOT * (
                    1.0 + 3.0 * 0.044715 * square
                )
                self.gu[place, lanes] = slope.astype(low)

        self.gathered(self.h2, plan_two, up)

        self.move_wait(self.go, self.gx, move[1])
        for chunk in range(CH):
            part = self.at_chunk(chunk)
            self.gg[self.at_quarter(self.q, chunk), :] = self.gx[part, :]
            self.gather_send(self.gg, plan_go, chunk)
        self.weights_done("d")
        flat_down = lambda: self.wd[...].reshape(4 * hidden, width)
        started_down = self.scatter_start(
            lambda quarter: jnp.dot(
                self.hid[self.at_quarter(quarter), :], flat_down(), preferred_element_type=f32
            ),
            self.own_b,
            1,
            self.rx.at[1],
        )

        def to_up(quarter):
            place = self.at_quarter(quarter)
            value = dot_last(self.gg[place, :], flat_down())
            self.gu[place, :] = (self.gu[place, :].astype(f32) * value).astype(low)

        self.gathered(self.gg, plan_go, to_up)
        grad_out = self.gx[...].astype(f32)
        self.sums[5:6, :] = jnp.sum(grad_out, axis=0, keepdims=True)

        def two_part(quarter):
            place = self.at_quarter(quarter)
            return sum(
                dot_last(self.gu[place, pl.ds(block * hidden, hidden)], self.wu[block])
                for block in range(4)
            )

        started = self.scatter_start(two_part, self.own_a, 0, self.rx.at[0])

        def down_grad(block, carry):
            lanes = pl.ds(pl.multiple_of(block * hidden, hidden), hidden)
            self.dd[block] = dot_first(self.hid[:, lanes], self.gg[...]).astype(low)
            return carry

        lax.fori_loop(0, 4, down_grad, 0)
        self.grads_one("d")
        step = width // 4

        def up_grad(block, carry):
            lanes = pl.ds(pl.multiple_of(block * step, step), step)
            value = dot_first(self.h2[:, lanes], self.gu[...]).astype(low)
            for plane in range(4):
                self.du[plane, lanes, :] = value[:, plane * hidden : (plane + 1) * hidden]
            return carry

        lax.fori_loop(0, 4, up_grad, 0)
        self.grads_one("u")
        totals = [0.0] * 3
        for chunk in range(CH):
            part = self.at_chunk(chunk)
            grad_two = self.scatter_chunk(started, self.own_a, chunk)
            normed = self.n2[part, :]
            middle = self.gx[part, :].astype(f32) + norm_back(
                grad_two, normed, self.i2[part, :], gain_two
            )
            self.gm[part, :] = middle
            self.ga[self.at_quarter(self.q, chunk), :] = middle.astype(low)
            self.gather_send(self.ga, plan_mid, chunk)
            for place, value in enumerate((grad_two * normed, grad_two, middle)):
                totals[place] = totals[place] + jnp.sum(value, axis=0, keepdims=True)
        self.sums[3:4, :] = totals[0]
        self.sums[4:5, :] = totals[1]
        self.sums[2:3, :] = totals[2]
        self.bsum[0:1, :] = jnp.sum(self.gu[...].astype(f32), axis=0, keepdims=True)
        for chunk in range(CH):
            part = self.at_chunk(chunk)
            summed = self.scatter_chunk(started_down, self.own_b, chunk)
            self.ox[part, :] = (self.mid[part, :] + summed + bias_down).astype(low)
        self.move_start(self.ox, self.out, False, move[2])
        self.grads_two("d")

        def to_heads(quarter):
            place = self.at_quarter(quarter)
            value = dot_last(self.ga[place, :], flat_out()).astype(low)
            for head in range(heads):
                self.hh[head, place, :] = value[:, head * dim : (head + 1) * dim]

        self.gathered(self.ga, plan_mid, to_heads)
        self.grads_two("u")
        self.do[...] = dot_first(self.ho[...], self.ga[...]).astype(low).reshape(self.do.shape)
        self.grads_one("o")

        def attend_back(head, carry):
            self.ka[...] = jnp.zeros_like(self.ka)
            self.va[...] = jnp.zeros_like(self.va)
            for block in quarters:
                place = pl.ds(block * rows, rows)
                query = self.qh[head, place, :]
                grads = self.hh[head, place, :]
                probs, values = [], []
                inner = 0.0
                for first, count in parts_of(block):
                    span = pl.ds(first, count)
                    prob = self.pb[block][head, :, span]
                    value = dot_last(grads, self.vh[head, span, :])
                    self.va[span, :] += dot_first(prob, grads)
                    prob = prob.astype(f32)
                    inner = inner + jnp.sum(prob * value, axis=1, keepdims=True)
                    probs.append(prob)
                    values.append(value)
                result = 0.0
                for (first, count), prob, value in zip(parts_of(block), probs, values):
                    span = pl.ds(first, count)
                    score = (prob * (value - inner)).astype(low)
                    result = result + jnp.dot(
                        score, self.kh[head, span, :], preferred_element_type=f32
                    )
                    self.ka[span, :] += dot_first(score, query)
                self.qh[head, place, :] = (result * 0.125).astype(low)
            self.kh[head] = self.ka[...].astype(low)
            self.vh[head] = self.va[...].astype(low)
            return carry

        lax.fori_loop(0, heads, attend_back, 0)
        assemble(self.gp, (self.qh, self.kh, self.vh), heads)
        self.grads_three("d")
        self.grads_three("u")

        def project_grad(slot, carry):
            lanes = pl.ds(pl.multiple_of(slot * heads * dim, heads * dim), heads * dim)
            value = dot_first(self.gp[:, lanes], self.h1[...]).astype(low)
            self.dq[slot] = value.reshape(heads, dim, width)
            return carry

        lax.fori_loop(0, 3, project_grad, 0)
        self.grads_one("q")
        self.grads_two("o")
        started = self.scatter_start(
            lambda quarter: jnp.dot(
                self.gp[self.at_quarter(quarter), :],
                self.wq[...].reshape(3 * heads * dim, width),
                preferred_element_type=f32,
            ),
            self.own_b,
            1,
            self.rx.at[2],
        )
        self.bsum[1:2, : 3 * heads * dim] = jnp.sum(
            self.gp[...].astype(f32), axis=0, keepdims=True
        )
        self.grads_two("q")
        self.grads_three("o")
        totals = [0.0] * 2
        for chunk in range(CH):
            part = self.at_chunk(chunk)
            grad_one = self.scatter_chunk(started, self.own_b, chunk)
            normed = self.n1[part, :]
            self.xs[part, :] = (
                self.gm[part, :] + norm_back(grad_one, normed, self.i1[part, :], gain_one)
            ).astype(low)
            for place, value in enumerate((grad_one * normed, grad_one)):
                totals[place] = totals[place] + jnp.sum(value, axis=0, keepdims=True)
        self.move_start(self.xs, self.gtok, False, move[3])
        self.sums[0:1, :] = totals[0]
        self.sums[1:2, :] = totals[1]
        self.sums[6:8, :] = jnp.zeros((2, width), f32)
        self.grads_three("q")
        for kind in "duoq":
            self.grads_done(kind)
        self.move_wait(self.ox, self.out, move[2])
        self.move_wait(self.xs, self.gtok, move[3])
        self.drain()

    def mask_blocks(self):
        rows = self.rows
        for block in range(4):
            down = block * rows + lax.broadcasted_iota(jnp.int32, (rows, 1), 0)
            side = block * rows + lax.broadcasted_iota(jnp.int32, (1, rows), 1)

            def ids(places):
                total = jnp.zeros_like(places)
                for piece in range(4):
                    first = self.st[piece]
                    inside = (places >= first) & (places < first + PIECE)
                    total = jnp.where(inside, piece + 1, total)
                return total

            mine, theirs = ids(down), ids(side)
            seen = (side <= down) | ((mine == theirs) & (mine > 0))
            self.mk[block] = jnp.where(seen, 0.0, -1e30).astype(jnp.bfloat16)


IN_NAMES = ("st", "tok", "go", "in_q", "in_o", "in_u", "in_d", "small", "bq", "bu")
OUT_NAMES = ("out", "gtok", "eq", "eo", "eu", "ed", "sums", "bsum")


def fused_layer(starts_row, tok, go, in_q, in_o, in_u, in_d, small, bq, bu):
    rows, width = tok.shape
    heads, dim = 4, width // 16
    hidden = in_u.shape[1] // 4
    part = width // 8
    n = 4 * rows
    low, f32 = jnp.bfloat16, jnp.float32
    scratch = dict(
        xs=((rows, width), low),
        gx=((rows, width), low),
        wq=((3, 4, dim, width), low),
        wo=((4, dim, width), low),
        wu=((4, width, hidden), low),
        wd=((4, hidden, width), low),
        h1=((n, width), low),
        h2=((n, width), low),
        gg=((n, width), low),
        ga=((n, width), low),
        qh=((heads, n, dim), low),
        kh=((heads, n, dim), low),
        vh=((heads, n, dim), low),
        hh=((heads, n, dim), low),
        ho=((n, heads * dim), low),
        gp=((n, 3 * heads * dim), low),
        ka=((n, dim), f32),
        va=((n, dim), f32),
        mk=((4, rows, rows), low),
        n1=((rows, width), f32),
        n2=((rows, width), f32),
        mid=((rows, width), f32),
        gm=((rows, width), f32),
        i1=((rows, 1), f32),
        i2=((rows, 1), f32),
        own_a=((rows, width), f32),
        own_b=((rows, width), f32),
        hid=((n, 4 * hidden), low),
        gu=((n, 4 * hidden), low),
        ox=((rows, width), low),
        rs=((2, 5, rows, width), low),
        rx=((3, rows, width), low),
        dq=((3, 4, dim, width), low),
        do=((4, dim, width), low),
        du=((4, width, hidden), low),
        dd=((4, hidden, width), low),
        yq=((3, 4, dim, 4 * part), low),
        yo=((4, dim, 4 * part), low),
        yu=((4, 4 * part, hidden), low),
        yd=((4, hidden, 4 * part), low),
        zq=((3, 3, dim, 4 * part), low),
        zo=((3, dim, 4 * part), low),
        zu=((3, 4 * part, hidden), low),
        zd=((3, hidden, 4 * part), low),
        fq=((3, dim, 4 * part), low),
        fo=((dim, 4 * part), low),
        fu=((4 * part, hidden), low),
        fd=((hidden, 4 * part), low),
    )
    probs = [((heads, rows, (block + 1) * rows), low) for block in range(4)]
    names = IN_NAMES + OUT_NAMES + tuple(scratch)

    def kernel(*refs):
        count = len(names)
        state = Fused(names, refs[:count])
        state.pb = refs[count : count + 4]
        state.ssem, state.rsem, state.lsem = refs[count + 4 :]
        state.run()

    hbm = pl.BlockSpec(memory_space=pl.ANY)
    vmem = pl.BlockSpec(memory_space=pltpu.VMEM)
    return pl.pallas_call(
        kernel,
        out_shape=(
            jax.ShapeDtypeStruct((rows, width), low),
            jax.ShapeDtypeStruct((rows, width), low),
            jax.ShapeDtypeStruct((4, 3, dim, part), low),
            jax.ShapeDtypeStruct((4, dim, part), low),
            jax.ShapeDtypeStruct((4, part, hidden), low),
            jax.ShapeDtypeStruct((4, hidden, part), low),
            jax.ShapeDtypeStruct((8, width), f32),
            jax.ShapeDtypeStruct((2, width), f32),
        ),
        in_specs=[pl.BlockSpec(memory_space=pltpu.SMEM)] + [hbm] * 6 + [vmem] * 3,
        out_specs=(hbm,) * 6 + (vmem,) * 2,
        scratch_shapes=[pltpu.VMEM(*spec) for spec in scratch.values()]
        + [pltpu.VMEM(*spec) for spec in probs]
        + [pltpu.SemaphoreType.DMA((SEMS,))] * 3,
        name="fused_layer",
        compiler_params=pltpu.CompilerParams(
            collective_id=0, has_side_effects=True, vmem_limit_bytes=VMEM_LIMIT
        ),
    )(starts_row, tok, go, in_q, in_o, in_u, in_d, small, bq, bu)


SEMS = 192
VMEM_LIMIT = 67043328


def per_device_fused(
    tokens_in, starts, ln1_gain, ln1_bias, w_qkv, b_qv, w_out, b_out,
    ln2_gain, ln2_bias, w_up, b_up, w_down, b_down, grad_out,
):
    rows, width = tokens_in.shape
    f32 = jnp.float32
    dp, z = lax.axis_index("dp"), lax.axis_index("tensor")
    member, y = dp % 4, dp // 4
    part = width // 8
    dim = width // 16
    hidden = w_up.shape[1] // 4
    bit = ln1_gain.shape[0]
    packed = jnp.concatenate(
        [
            ln1_gain, ln1_bias, b_out, ln2_gain, ln2_bias, b_down,
            b_qv.astype(f32).reshape(-1), b_up.astype(f32).reshape(-1),
            starts.astype(f32).reshape(-1),
        ]
    )
    fill = -packed.shape[0] % 128
    packed = jnp.concatenate([packed, jnp.zeros((fill,), f32)])[None]
    every = lax.all_gather(packed, ("dp", "tensor"), axis=0, tiled=True)
    small = every[:, : 6 * bit].reshape(32, 6, bit).transpose(1, 0, 2).reshape(6, width)
    small = jnp.concatenate([small, jnp.zeros((2, width), f32)])
    at = 6 * bit
    qv = every[:, at : at + b_qv.size].reshape(8, 4, *b_qv.shape)
    at += b_qv.size
    ups = every[:, at : at + b_up.size].reshape(8, 4, *b_up.shape)
    at += b_up.size
    first = every[:, at : at + 4].reshape(8, 4, 4)[:, 0]
    starts_row = lax.dynamic_index_in_dim(first, 2 * z + y, 0, keepdims=False).astype(jnp.int32)
    qv = qv.transpose(1, 2, 0, 3).reshape(4, 4, b_qv.shape[0] // 4, 8 * b_qv.shape[1])
    qv = lax.dynamic_index_in_dim(qv, member, 1, keepdims=False).reshape(4, 2, dim)
    bq = jnp.stack([qv[:, 0], jnp.zeros_like(qv[:, 0]), qv[:, 1]]).reshape(1, 3 * 4 * dim)
    ups = ups.transpose(1, 2, 0, 3).reshape(4, 4, b_up.shape[0] // 4, 8 * b_up.shape[1])
    bu = lax.dynamic_index_in_dim(ups, member, 1, keepdims=False).reshape(1, 4 * hidden)
    in_q = w_qkv.reshape(part, 4, 3, dim).transpose(1, 2, 3, 0)
    in_o = w_out.reshape(4, dim, part)
    in_d = w_down.reshape(4, hidden, part)
    out, gtok, eq, eo, eu, ed, sums, bsum = fused_layer(
        starts_row, tokens_in, grad_out, in_q, in_o, w_up, in_d, small, bq, bu
    )
    grad_w_qkv = eq.transpose(3, 0, 1, 2).reshape(part, 3 * 4 * dim).astype(f32)
    grad_w_out = eo.reshape(4 * dim, part).astype(f32)
    grad_w_up = eu.transpose(1, 0, 2).reshape(part, 4 * hidden).astype(f32)
    grad_w_down = ed.reshape(4 * hidden, part).astype(f32)
    up_sum = bsum[0, : 4 * hidden].reshape(4, 1, hidden)
    qv_sum = bsum[1, : 3 * 4 * dim].reshape(3, 4, dim)
    qv_sum = jnp.stack([qv_sum[0], qv_sum[2]], axis=1).reshape(4, 1, 2 * dim)
    spot = (jnp.arange(4) == member)[None, :, None]
    up_sum = jnp.where(spot, up_sum, 0.0)
    qv_sum = jnp.where(spot, qv_sum, 0.0)
    up_sum = up_sum.reshape(4, 4, b_up.shape[0] // 4, 8, b_up.shape[1]).transpose(3, 0, 1, 2, 4)
    qv_sum = qv_sum.reshape(4, 4, b_qv.shape[0] // 4, 8, b_qv.shape[1]).transpose(3, 0, 1, 2, 4)
    vectors = sums[:6].reshape(6, 32, bit).transpose(1, 0, 2).reshape(32, 6 * bit)
    joined = jnp.concatenate(
        [vectors, qv_sum.reshape(32, b_qv.size), up_sum.reshape(32, b_up.size)], axis=1
    )
    mine = lax.psum_scatter(joined, ("dp", "tensor"), scatter_dimension=0, tiled=True)[0]
    take = [mine[k * bit : (k + 1) * bit] for k in range(6)]
    at = 6 * bit
    grad_b_qv = mine[at : at + b_qv.size].reshape(b_qv.shape)
    grad_b_up = mine[at + b_qv.size :].reshape(b_up.shape)
    return (
        out, gtok, take[0], take[1], grad_w_qkv, grad_b_qv, grad_w_out, take[2],
        take[3], take[4], grad_w_up, grad_b_up, grad_w_down, take[5],
    )


def solution(mesh):
    sizes = (mesh.shape["dp"], mesh.shape["tensor"])

    def layer(tokens_in, starts, *others):
        fits = sizes == (8, 4) and tokens_in.shape[0] == PIECE and starts.shape == (1, 4)
        return (per_device_fused if fits else per_device)(tokens_in, starts, *others)

    return jax.shard_map(
        layer,
        mesh=mesh,
        in_specs=(
            P(("dp", "tensor"), None),
            P("dp", None),
            P(("dp", "tensor")),
            P(("dp", "tensor")),
            P("dp", "tensor"),
            P("tensor", "dp"),
            P("tensor", "dp"),
            P(("dp", "tensor")),
            P(("dp", "tensor")),
            P(("dp", "tensor")),
            P("dp", "tensor"),
            P("tensor", "dp"),
            P("tensor", "dp"),
            P(("dp", "tensor")),
            P(("dp", "tensor"), None),
        ),
        out_specs=(
            P(("dp", "tensor"), None),
            P(("dp", "tensor"), None),
            P(("dp", "tensor")),
            P(("dp", "tensor")),
            P("dp", "tensor"),
            P("tensor", "dp"),
            P("tensor", "dp"),
            P(("dp", "tensor")),
            P(("dp", "tensor")),
            P(("dp", "tensor")),
            P("dp", "tensor"),
            P("tensor", "dp"),
            P("tensor", "dp"),
            P(("dp", "tensor")),
        ),
        check_vma=False,
    )
```

```python
import functools

import jax
import jax.numpy as jnp
from jax import lax
from jax.experimental import pallas as pl
from jax.experimental.pallas import tpu as pltpu
from jax.sharding import PartitionSpec as P

HD = 64
PIECE = 256
QBLOCK = 512


EPS = 1e-05
ROOT = 0.7978845608028654


def gelu_tanh(values):
    return 0.5 * values * (1.0 + jnp.tanh(ROOT * (values + 0.044715 * values * values * values)))


def normalize(values):
    center = jnp.mean(values, axis=-1, keepdims=True)
    shifted = values - center
    inverse = lax.rsqrt(jnp.mean(shifted * shifted, axis=-1, keepdims=True) + EPS)
    return (shifted * inverse, inverse)


def norm_back(grad_normed, normed, inverse, gain):
    scaled = grad_normed * gain
    return inverse * (
        scaled
        - jnp.mean(scaled, axis=-1, keepdims=True)
        - normed * jnp.mean(scaled * normed, axis=-1, keepdims=True)
    )


def dot_last(left, right):
    return lax.dot_general(
        left, right, (((1,), (1,)), ((), ())), preferred_element_type=jnp.float32
    )


def dot_first(left, right):
    return lax.dot_general(
        left, right, (((0,), (0,)), ((), ())), preferred_element_type=jnp.float32
    )


def gather_rows(values):
    return lax.all_gather(values, "tensor", axis=0, tiled=True)


def gather_grads(values):
    return lax.all_gather(values, "tensor", axis=0, tiled=True)


def reduce_rows(left, weight, rows):

    def term(start, count):
        return jnp.dot(left, weight, preferred_element_type=jnp.float32)

    return lax.psum_scatter(
        term(jnp.int32(0), lax.axis_size("tensor") * rows).astype(jnp.bfloat16),
        "tensor",
        scatter_dimension=0,
        tiled=True,
    ).astype(jnp.float32)


def reduce_grads(left, weight, rows):

    def term(start, count):
        return dot_last(left, weight)

    return lax.psum_scatter(
        term(jnp.int32(0), lax.axis_size("tensor") * rows).astype(jnp.bfloat16),
        "tensor",
        scatter_dimension=0,
        tiled=True,
    ).astype(jnp.float32)


def piece_ids(start_row, length):
    places = jnp.arange(length, dtype=jnp.int32)
    inside = (places[:, None] >= start_row[None, :]) & (
        places[:, None] < start_row[None, :] + PIECE
    )
    labels = jnp.arange(1, start_row.shape[0] + 1, dtype=jnp.int32)
    return jnp.sum(jnp.where(inside, labels[None, :], 0), axis=1)


def allowed_block(row_ids, row_places, key_ids, key_places):
    causal = key_places[None, :] <= row_places[:, None]
    picture = (row_ids[:, None] == key_ids[None, :]) & (row_ids[:, None] > 0)
    return causal | picture


def block_scores(by_seq, start_rows, block_index):
    length = by_seq.shape[1]
    per_seq = length // QBLOCK
    seq_index = block_index // per_seq
    first_row = block_index % per_seq * QBLOCK
    sequence = lax.dynamic_index_in_dim(by_seq, seq_index, 0, keepdims=False)
    key_ids = piece_ids(lax.dynamic_index_in_dim(start_rows, seq_index, 0, keepdims=False), length)
    query_rows = lax.dynamic_slice_in_dim(sequence, first_row, QBLOCK, 0)[:, :, 0]
    key_rows = sequence[:, :, 1]
    value_rows = sequence[:, :, 2]
    row_ids = lax.dynamic_slice_in_dim(key_ids, first_row, QBLOCK, 0)
    row_places = first_row + jnp.arange(QBLOCK, dtype=jnp.int32)
    scores = (
        jnp.einsum("qhd,khd->hqk", query_rows, key_rows, preferred_element_type=jnp.float32) * 0.125
    )
    places = jnp.arange(length, dtype=jnp.int32)
    scores = jnp.where(allowed_block(row_ids, row_places, key_ids, places)[None], scores, -1e30)
    return (seq_index, first_row, query_rows, key_rows, value_rows, scores)


def attention_forward(by_seq, start_rows):
    total_blocks = by_seq.shape[0] * (by_seq.shape[1] // QBLOCK)

    def attend(block_index):
        _, _, query_rows, key_rows, value_rows, scores = block_scores(
            by_seq, start_rows, block_index
        )
        peak = jnp.max(scores, axis=-1, keepdims=True)
        log_total = peak + jnp.log(jnp.sum(jnp.exp(scores - peak), axis=-1, keepdims=True))
        probs = jnp.exp(scores - log_total)
        heads = jnp.einsum(
            "hqk,khd->qhd",
            probs.astype(jnp.bfloat16),
            value_rows,
            preferred_element_type=jnp.float32,
        )
        return (heads.astype(jnp.bfloat16), log_total)

    return lax.map(attend, jnp.arange(total_blocks, dtype=jnp.int32))


def attention_backward(by_seq, start_rows, log_totals, grad_heads):
    total_blocks = by_seq.shape[0] * (by_seq.shape[1] // QBLOCK)
    empty = jnp.zeros(by_seq.shape[:3] + (HD,), jnp.float32)

    def step(carry, item):
        grad_keys, grad_values = carry
        block_index, log_total = item
        seq_index, first_row, query_rows, key_rows, value_rows, scores = block_scores(
            by_seq, start_rows, block_index
        )
        grad_seq = lax.dynamic_index_in_dim(grad_heads, seq_index, 0, keepdims=False)
        grad_rows = lax.dynamic_slice_in_dim(grad_seq, first_row, QBLOCK, 0)
        probs = jnp.exp(scores - log_total)
        grad_probs = jnp.einsum(
            "qhd,khd->hqk", grad_rows, value_rows, preferred_element_type=jnp.float32
        )
        inner = jnp.sum(probs * grad_probs, axis=-1, keepdims=True)
        grad_scores = (probs * (grad_probs - inner)).astype(jnp.bfloat16)
        grad_query = (
            jnp.einsum("hqk,khd->qhd", grad_scores, key_rows, preferred_element_type=jnp.float32)
            * 0.125
        )
        key_term = (
            jnp.einsum("hqk,qhd->khd", grad_scores, query_rows, preferred_element_type=jnp.float32)
            * 0.125
        )
        value_term = jnp.einsum(
            "hqk,qhd->khd",
            probs.astype(jnp.bfloat16),
            grad_rows,
            preferred_element_type=jnp.float32,
        )
        grad_keys = lax.dynamic_update_index_in_dim(
            grad_keys,
            lax.dynamic_index_in_dim(grad_keys, seq_index, 0, keepdims=False) + key_term,
            seq_index,
            0,
        )
        grad_values = lax.dynamic_update_index_in_dim(
            grad_values,
            lax.dynamic_index_in_dim(grad_values, seq_index, 0, keepdims=False) + value_term,
            seq_index,
            0,
        )
        return ((grad_keys, grad_values), grad_query)

    (grad_keys, grad_values), grad_query = lax.scan(
        step, (empty, empty), (jnp.arange(total_blocks, dtype=jnp.int32), log_totals)
    )
    return (grad_query, grad_keys, grad_values)


def per_device(
    tokens_in,
    starts,
    ln1_gain,
    ln1_bias,
    w_qkv,
    b_qv,
    w_out,
    b_out,
    ln2_gain,
    ln2_bias,
    w_up,
    b_up,
    w_down,
    b_down,
    grad_out,
):
    rows = tokens_in.shape[0]
    gain_one, shift_one, bias_out, gain_two, shift_two, bias_down = (
        lax.all_gather(ln1_gain, ("dp", "tensor"), axis=0, tiled=True),
        lax.all_gather(ln1_bias, ("dp", "tensor"), axis=0, tiled=True),
        lax.all_gather(b_out, ("dp", "tensor"), axis=0, tiled=True),
        lax.all_gather(ln2_gain, ("dp", "tensor"), axis=0, tiled=True),
        lax.all_gather(ln2_bias, ("dp", "tensor"), axis=0, tiled=True),
        lax.all_gather(b_down, ("dp", "tensor"), axis=0, tiled=True),
    )
    weight_qkv, bias_qv, weight_out = (
        lax.all_gather(w_qkv, "dp", axis=0, tiled=True),
        lax.all_gather(b_qv, "dp", axis=1, tiled=True),
        lax.all_gather(w_out, "dp", axis=1, tiled=True),
    )
    weight_up, bias_up, weight_down = (
        lax.all_gather(w_up, "dp", axis=0, tiled=True),
        lax.all_gather(b_up, "dp", axis=1, tiled=True),
        lax.all_gather(w_down, "dp", axis=1, tiled=True),
    )
    local_heads = weight_qkv.shape[1] // (3 * HD)
    seq_count = starts.shape[0]
    inputs = tokens_in.astype(jnp.float32)
    normed_one, inverse_one = normalize(inputs)
    gathered_one = gather_rows((normed_one * gain_one + shift_one).astype(jnp.bfloat16))
    group = gathered_one.shape[0]
    length = group // seq_count
    bias_pair = bias_qv.astype(jnp.float32).reshape(local_heads, 2, HD)
    full_bias = jnp.stack(
        [bias_pair[:, 0], jnp.zeros_like(bias_pair[:, 0]), bias_pair[:, 1]], axis=1
    )
    projected = (
        jnp.dot(gathered_one, weight_qkv, preferred_element_type=jnp.float32).reshape(
            group, local_heads, 3, HD
        )
        + full_bias
    ).astype(jnp.bfloat16)
    by_seq = projected.reshape(seq_count, length, local_heads, 3, HD)
    heads_blocks, log_totals = attention_forward(by_seq, starts)
    heads_out = heads_blocks.reshape(group, local_heads * HD)
    middle = inputs + (reduce_rows(heads_out, weight_out, rows) + bias_out)
    normed_two, inverse_two = normalize(middle)
    rounded_two = (normed_two * gain_two + shift_two).astype(jnp.bfloat16)
    grad_final = grad_out.astype(jnp.float32)
    grad_bias_down = jnp.sum(grad_final, axis=0)
    gathered_two = gather_rows(rounded_two)
    up_proj = jnp.dot(gathered_two, weight_up, preferred_element_type=jnp.float32) + bias_up.astype(
        jnp.float32
    ).reshape(-1)
    hidden_act, gelu_pull = jax.vjp(gelu_tanh, up_proj)
    hidden_low = hidden_act.astype(jnp.bfloat16)
    output = (middle + reduce_rows(hidden_low, weight_down, rows) + bias_down).astype(jnp.bfloat16)
    grad_branch = gather_grads(grad_out)
    grad_w_down = dot_first(hidden_low, grad_branch)
    grad_up = gelu_pull(dot_last(grad_branch, weight_down))[0].astype(jnp.bfloat16)
    grad_b_up = jnp.sum(grad_up, axis=0, dtype=jnp.float32).reshape(bias_up.shape)
    grad_w_up = dot_first(gathered_two, grad_up)
    grad_two = reduce_grads(grad_up, weight_up, rows)
    grad_w_up, grad_b_up, grad_w_down = (
        lax.psum_scatter(
            grad_w_up.astype(jnp.bfloat16), "dp", scatter_dimension=0, tiled=True
        ).astype(jnp.float32),
        lax.psum_scatter(
            grad_b_up.astype(jnp.bfloat16), "dp", scatter_dimension=1, tiled=True
        ).astype(jnp.float32),
        lax.psum_scatter(
            grad_w_down.astype(jnp.bfloat16), "dp", scatter_dimension=1, tiled=True
        ).astype(jnp.float32),
    )
    grad_gain_two = jnp.sum(grad_two * normed_two, axis=0)
    grad_shift_two = jnp.sum(grad_two, axis=0)
    grad_middle = grad_final + norm_back(grad_two, normed_two, inverse_two, gain_two)
    grad_bias_out = jnp.sum(grad_middle, axis=0)
    grad_attn = gather_grads(grad_middle.astype(jnp.bfloat16))
    grad_w_out = dot_first(heads_out, grad_attn)
    grad_heads = (
        dot_last(grad_attn, weight_out)
        .astype(jnp.bfloat16)
        .reshape(seq_count, length, local_heads, HD)
    )
    grad_query, grad_keys, grad_values = attention_backward(by_seq, starts, log_totals, grad_heads)
    grad_proj = jnp.stack(
        [
            grad_query.reshape(group, local_heads, HD),
            grad_keys.reshape(group, local_heads, HD),
            grad_values.reshape(group, local_heads, HD),
        ],
        axis=2,
    ).astype(jnp.bfloat16)
    grad_b_qv = jnp.sum(grad_proj[:, :, 0::2], axis=0, dtype=jnp.float32).reshape(bias_qv.shape)
    grad_flat = grad_proj.reshape(group, 3 * local_heads * HD)
    grad_w_qkv = dot_first(gathered_one, grad_flat)
    grad_one = reduce_grads(grad_flat, weight_qkv, rows)
    grad_w_qkv, grad_b_qv, grad_w_out = (
        lax.psum_scatter(
            grad_w_qkv.astype(jnp.bfloat16), "dp", scatter_dimension=0, tiled=True
        ).astype(jnp.float32),
        lax.psum_scatter(
            grad_b_qv.astype(jnp.bfloat16), "dp", scatter_dimension=1, tiled=True
        ).astype(jnp.float32),
        lax.psum_scatter(
            grad_w_out.astype(jnp.bfloat16), "dp", scatter_dimension=1, tiled=True
        ).astype(jnp.float32),
    )
    grad_gain_one = jnp.sum(grad_one * normed_one, axis=0)
    grad_shift_one = jnp.sum(grad_one, axis=0)
    grad_tokens = (grad_middle + norm_back(grad_one, normed_one, inverse_one, gain_one)).astype(
        jnp.bfloat16
    )
    summed = (
        lax.psum_scatter(grad_gain_one, ("dp", "tensor"), scatter_dimension=0, tiled=True),
        lax.psum_scatter(grad_shift_one, ("dp", "tensor"), scatter_dimension=0, tiled=True),
        lax.psum_scatter(grad_bias_out, ("dp", "tensor"), scatter_dimension=0, tiled=True),
        lax.psum_scatter(grad_gain_two, ("dp", "tensor"), scatter_dimension=0, tiled=True),
        lax.psum_scatter(grad_shift_two, ("dp", "tensor"), scatter_dimension=0, tiled=True),
        lax.psum_scatter(grad_bias_down, ("dp", "tensor"), scatter_dimension=0, tiled=True),
    )
    return (
        output,
        grad_tokens,
        summed[0],
        summed[1],
        grad_w_qkv,
        grad_b_qv,
        grad_w_out,
        summed[2],
        summed[3],
        summed[4],
        grad_w_up,
        grad_b_up,
        grad_w_down,
        summed[5],
    )


MESH = pl.DeviceIdType.MESH
CH = 2


class Fused:
    def __init__(self, names, refs):
        for name, ref in zip(names, refs):
            setattr(self, name, ref)
        self.next_sem = 0
        self.unsent = []
        self.groups = {0: [], 1: []}
        self.unsent_later = []
        dp, self.z = lax.axis_index("dp"), lax.axis_index("tensor")
        self.y, self.x, self.c = dp // 4, (dp // 2) % 2, dp % 2
        self.j = self.member(self.x, self.c)
        self.q = self.quarter(self.j)
        self.sib = self.dev(self.y, self.x, 1 - self.c, self.z)
        self.across = self.dev(self.y, 1 - self.x, self.c, self.z)
        self.q_sib = self.quarter(self.member(self.x, 1 - self.c))
        self.q_x = self.quarter(self.member(1 - self.x, self.c))
        self.q_d = self.quarter(self.member(1 - self.x, 1 - self.c))
        self.rows = self.tok.shape[0]
        self.width = self.tok.shape[1]
        self.part = self.width // 8

    def dev(self, y, x, c, z):
        return ((y * 2 + x) * 2 + c, z)

    def member(self, x, c):
        return 2 * c + x

    def local(self, member):
        return 2 * (member % 2) + member // 2

    def mate(self, member):
        return self.dev(self.y, member % 2, member // 2, self.z)

    def quarter(self, member):
        return (member - self.z + 4) % 4

    def sem(self, count=1):
        index = self.next_sem
        self.next_sem += count
        return index

    def copy(self, src, dst, device, index, sent=None):
        return pltpu.make_async_remote_copy(
            src_ref=src,
            dst_ref=dst,
            send_sem=self.ssem.at[index if sent is None else sent],
            recv_sem=self.rsem.at[index],
            device_id=device,
            device_id_type=MESH,
        )

    def send(self, src, dst, device, index, group=None):
        copy = self.copy(src, dst, device, index)
        copy.start()
        (self.unsent if group is None else self.groups[group]).append(copy)

    def later(self, view, sent, when=None):
        self.unsent_later.append((view, sent, when))

    def arrived(self, dst, index):
        self.copy(dst, dst, self.sib, index).wait_recv()

    def drain(self):
        for copy in self.unsent + self.groups[0] + self.groups[1]:
            copy.wait_send()
        for view, sent, when in self.unsent_later:
            copy = self.copy(view(), view(), self.sib, sent)
            if when is None:
                copy.wait_send()
            else:
                pl.when(when)(copy.wait_send)

    def at_quarter(self, quarter, chunk=None):
        if chunk is None:
            return pl.ds(pl.multiple_of(quarter * self.rows, self.rows), self.rows)
        size = self.rows // CH
        return pl.ds(pl.multiple_of(quarter * self.rows + chunk * size, size), size)

    def at_chunk(self, chunk):
        size = self.rows // CH
        return pl.ds(chunk * size, size)

    def barrier(self):
        me = lax.axis_index("dp") * 4 + self.z
        bar = pltpu.get_barrier_semaphore()

        def greet(step, carry):
            other = (me + step) % 32
            pl.semaphore_signal(
                bar, inc=1, device_id=(other // 4, other % 4), device_id_type=MESH
            )
            return carry

        lax.fori_loop(1, 32, greet, 0)
        pl.semaphore_wait(bar, 31)

    def homes(self):
        plane = 2 * self.y + self.x
        member = (plane + self.z) % 4
        worker = (self.c, member % 2, member // 2, plane)
        owner = (self.z // 2, self.z % 2, self.y, self.q)
        same = (
            (worker[0] == self.y)
            & (worker[1] == self.x)
            & (worker[2] == self.c)
            & (worker[3] == self.z)
        )
        return self.dev(*worker), self.dev(*owner), same

    def move_start(self, src, dst, outward, index):
        worker, owner, same = self.homes()
        copy = self.copy(src, dst, worker if outward else owner, index)
        local = pltpu.make_async_copy(src, dst, self.lsem.at[index])

        @pl.when(jnp.logical_not(same))
        def _():
            copy.start()

        @pl.when(same)
        def _():
            local.start()

    def move_wait(self, src, dst, index):
        same = self.homes()[2]
        copy = self.copy(src, dst, self.sib, index)
        local = pltpu.make_async_copy(src, dst, self.lsem.at[index])

        @pl.when(jnp.logical_not(same))
        def _():
            copy.wait_send()
            copy.wait_recv()

        @pl.when(same)
        def _():
            local.wait()

    def span(self, half):
        return pl.ds(pl.multiple_of(half * 4 * self.part, 4 * self.part), 4 * self.part)

    def place(self, source):
        return pl.ds(pl.multiple_of(source * self.part, self.part), self.part)

    def cut(self, kind, ref, zc, where):
        if kind == "u":
            return ref.at[zc, where, :]
        return ref.at[zc, :, where]

    def piece(self, kind, ref, member):
        if kind == "u":
            wide = self.wbuf["u"].shape[2]
            return ref.at[:, pl.ds(pl.multiple_of(member * wide, wide), wide)]
        return ref.at[member]

    def weights_one(self, kind):
        source = 4 * self.y + self.local(self.j)
        here = self.cut(kind, self.wbuf[kind], self.z, self.place(source))
        self.one[kind] = []
        for step in range(1, 4):
            member = (self.j + step) % 4
            index = self.sem()
            self.send(
                self.piece(kind, self.shard[kind], member), here, self.mate(member), index
            )
            sender = 4 * self.y + self.local((self.j - step + 4) % 4)
            self.one[kind].append(
                (self.cut(kind, self.wbuf[kind], self.z, self.place(sender)), index)
            )
        index = self.sem()
        local = pltpu.make_async_copy(
            self.piece(kind, self.shard[kind], self.j), here, self.lsem.at[index]
        )
        local.start()
        self.own[kind] = local
        self.two[kind] = self.sem(4)
        self.three[kind] = self.sem(4)
        self.pass_sem[kind] = self.sem()

    def mine(self, kind, plane):
        return self.cut(kind, self.wbuf[kind], plane, self.span(self.y))

    def weights_two(self, kind):
        self.own[kind].wait()
        for view, index in self.one[kind]:
            self.arrived(view, index)
        here = self.mine(kind, self.z)
        for step, when in ((2, None), (1, self.z != 3), (3, self.z != 0)):
            plane = (self.z + step) % 4
            index = self.two[kind] + step
            copy = self.copy(here, here, self.dev(self.y, self.x, self.c, plane), index)
            if when is None:
                copy.start()
            else:
                pl.when(when)(copy.start)
            self.later(lambda: self.mine(kind, self.z), index, when)

    def weights_relay(self, kind, guard=None):
        for here, plane, step in ((2, 3, 3), (1, 0, 1)):
            when = self.z == here
            block = self.mine(kind, (here + 2) % 4)
            copy = self.copy(
                block,
                block,
                self.dev(self.y, self.x, self.c, plane),
                self.two[kind] + step,
                self.pass_sem[kind],
            )
            pl.when(when if guard is None else when & guard)(copy.start)

    def relayed(self, kind):
        self.later(
            lambda: self.mine(kind, self.z), self.pass_sem[kind], (self.z == 1) | (self.z == 2)
        )
        for step in range(4):
            self.later(lambda: self.mine(kind, self.z), self.three[kind] + step)

    def weights_cross(self, kind, step):
        mine = self.mine(kind, (self.z - step + 4) % 4)
        self.copy(
            mine,
            mine,
            self.dev(1 - self.y, self.x, self.c, self.z),
            self.three[kind] + step,
        ).start()

    def weights_here(self, kind, step):
        self.arrived(self.mine(kind, (self.z - step + 4) % 4), self.two[kind] + step)

    def weights_three(self, kind, steps=(1, 3)):
        for step in steps:
            self.weights_here(kind, step)
            self.weights_cross(kind, step)

    def weights_start_three(self, kind):
        self.weights_cross(kind, 0)
        self.weights_here(kind, 2)
        self.weights_relay(kind)
        self.weights_cross(kind, 2)

    def weights_ready(self, kind, step):
        plane = (self.z - step + 4) % 4
        self.arrived(
            self.cut(kind, self.wbuf[kind], plane, self.span(1 - self.y)),
            self.three[kind] + step,
        )

    def weights_done(self, kind):
        for step in range(4):
            self.weights_ready(kind, step)

    def grads_one(self, kind):
        index = self.sem()
        self.back[kind] = index
        for plane in range(4):
            away = self.cut(kind, self.dbuf[kind], plane, self.span(1 - self.y))
            there = self.cut(kind, self.ybuf[kind], plane, slice(None))
            use = index if plane == 0 else self.sem()
            self.send(away, there, self.dev(1 - self.y, self.x, self.c, self.z), use)
            self.backs.setdefault(kind, []).append(use)

    def grads_two(self, kind):
        for plane in range(4):
            there = self.cut(kind, self.ybuf[kind], plane, slice(None))
            self.arrived(there, self.backs[kind][plane])
            mine = self.cut(kind, self.dbuf[kind], plane, self.span(self.y))
            mine[...] = (
                mine[...].astype(jnp.float32) + there[...].astype(jnp.float32)
            ).astype(jnp.bfloat16)
        self.swaps[kind] = []
        for step in range(1, 4):
            plane = (self.z + step) % 4
            index = self.sem()
            self.send(
                self.cut(kind, self.dbuf[kind], plane, self.span(self.y)),
                self.zbuf[kind].at[step - 1],
                self.dev(self.y, self.x, self.c, plane),
                index,
            )
            self.swaps[kind].append(index)

    def head_one(self, step, head):
        self.copy(
            self.cut("q", self.dq, head, self.span(1 - self.y)),
            self.cut("q", self.yq, head, slice(None)),
            self.dev(1 - self.y, self.x, self.c, self.z),
            self.head_y + step,
        ).start()

    def head_add(self, step, head):
        there = self.cut("q", self.yq, head, slice(None))
        self.arrived(there, self.head_y + step)
        mine = self.cut("q", self.dq, head, self.span(self.y))
        mine[...] = (mine[...].astype(jnp.float32) + there[...].astype(jnp.float32)).astype(
            jnp.bfloat16
        )

    def head_two(self, step, head):
        self.copy(
            self.cut("q", self.dq, head, self.span(self.y)),
            self.zq.at[step],
            self.dev(self.y, self.x, self.c, head),
            self.head_z + step,
        ).start()

    def grads_three(self, kind):
        mine = self.cut(kind, self.dbuf[kind], self.z, self.span(self.y))
        total = mine[...].astype(jnp.float32)
        for step in range(1, 4):
            there = self.zbuf[kind].at[step - 1]
            self.arrived(there, self.swaps[kind][step - 1])
            total = total + there[...].astype(jnp.float32)
        final = self.fbuf[kind]
        final[...] = total.astype(jnp.bfloat16)
        ends = self.ebuf[kind]
        self.last[kind] = []
        for step in range(1, 4):
            member = (self.j + step) % 4
            index = self.sem()
            self.send(
                self.slab(kind, final, self.local(member)),
                ends.at[self.j],
                self.mate(member),
                index,
            )
            self.last[kind].append(((self.j - step + 4) % 4, index))
        index = self.sem()
        local = pltpu.make_async_copy(
            self.slab(kind, final, self.local(self.j)), ends.at[self.j], self.lsem.at[index]
        )
        local.start()
        self.own[kind] = local

    def slab(self, kind, ref, member):
        where = pl.ds(pl.multiple_of(member * self.part, self.part), self.part)
        if kind == "u":
            return ref.at[where, :]
        return ref.at[:, where]

    def grads_done(self, kind):
        self.own[kind].wait()
        for member, index in self.last[kind]:
            self.arrived(self.ebuf[kind].at[member], index)

    def small_one(self):
        self.sma[self.z] = self.si[...]
        self.small_sem = [self.sem() for _ in range(3)]
        for step in range(1, 4):
            plane = (self.z + step) % 4
            self.send(
                self.si,
                self.sma.at[self.z],
                self.dev(self.y, self.x, self.c, plane),
                self.small_sem[step - 1],
            )

    def around(self, step):
        return (lax.axis_index("dp") + step + 8) % 8

    def small_two(self):
        for step in range(1, 4):
            self.arrived(self.sma.at[(self.z - step + 4) % 4], self.small_sem[step - 1])
        me = self.around(0)
        self.lb[me] = sum(self.sma[plane, 0] for plane in range(4))
        self.bb[me] = self.sma[:, 1 + self.j]
        self.plane_sem = [(self.sem(), self.sem()) for _ in range(7)]
        for step in range(1, 8):
            other = self.around(step)
            member = self.member((other // 2) % 2, other % 2)
            first, second = self.plane_sem[step - 1]
            self.send(self.lb.at[me], self.lb.at[me], (other, self.z), first)
            self.send(self.sma.at[:, 1 + member], self.bb.at[me], (other, self.z), second)

    def small_three(self):
        for step in range(1, 8):
            other = self.around(-step)
            first, second = self.plane_sem[step - 1]
            self.arrived(self.lb.at[other], first)
            self.arrived(self.bb.at[other], second)
        part, dim = self.part, self.qh.shape[2]
        for source in range(8):
            self.small[:, source * part : (source + 1) * part] = self.lb[source]
        bias = sum(self.bb[source] for source in range(8))
        for head in range(4):
            row = bias[head, 0:1]
            self.bq[head, :, 0:dim] = row[:, 0:dim]
            self.bq[head, :, dim : 2 * dim] = jnp.zeros((1, dim), jnp.float32)
            self.bq[head, :, 2 * dim :] = row[:, dim:]
            for half in range(2):
                place = (2 * head + half) * part
                self.bu[:, place : place + part] = bias[head, 1 + half : 2 + half]

    def back_one(self):
        part, me = self.part, self.around(0)
        for target in range(8):
            self.cs[target] = self.sums[:, target * part : (target + 1) * part]
        self.cr[me] = self.cs[me]
        self.cd[me] = self.cb[...]
        self.back_sem = [(self.sem(), self.sem()) for _ in range(7)]
        for step in range(1, 8):
            other = self.around(step)
            first, second = self.back_sem[step - 1]
            self.send(self.cs.at[other], self.cr.at[me], (other, self.z), first)
            self.send(self.cb, self.cd.at[me], (other, self.z), second)

    def back_two(self):
        for step in range(1, 8):
            other = self.around(-step)
            first, second = self.back_sem[step - 1]
            self.arrived(self.cr.at[other], first)
            self.arrived(self.cd.at[other], second)
        self.es[self.z] = sum(self.cr[source] for source in range(8))
        for member in range(4):
            pair = [2 * (member % 2) + member // 2, 4 + 2 * (member % 2) + member // 2]
            self.ed_small[:, member] = self.cd[pair[0]] + self.cd[pair[1]]
        self.eb[self.z] = self.ed_small[self.z]
        self.line_sem = [(self.sem(), self.sem()) for _ in range(3)]
        for step in range(1, 4):
            plane = (self.z + step) % 4
            device = self.dev(self.y, self.x, self.c, plane)
            first, second = self.line_sem[step - 1]
            self.send(self.es.at[self.z], self.es.at[self.z], device, first)
            self.send(self.ed_small.at[plane], self.eb.at[self.z], device, second)

    def back_three(self):
        for step in range(1, 4):
            plane = (self.z - step + 4) % 4
            first, second = self.line_sem[step - 1]
            self.arrived(self.es.at[plane], first)
            self.arrived(self.eb.at[plane], second)
        self.fs[...] = sum(self.es[plane] for plane in range(4))
        self.fb[...] = sum(self.eb[plane] for plane in range(4))

    def gather_plan(self):
        return {kind: [self.sem() for _ in range(CH)] for kind in ("across", "sib", "pass")}

    def gather_send(self, buf, plan, chunk):
        rows = self.at_quarter(self.q, chunk)
        self.send(buf.at[rows], buf.at[rows], self.across, plan["across"][chunk])
        self.send(buf.at[rows], buf.at[rows], self.sib, plan["sib"][chunk])

    def gather_pass(self, buf, plan):
        for chunk in range(CH):
            rows = self.at_quarter(self.q_x, chunk)
            self.arrived(buf.at[rows], plan["across"][chunk])
            self.send(buf.at[rows], buf.at[rows], self.sib, plan["pass"][chunk])

    def gather_sib(self, buf, plan):
        for chunk in range(CH):
            self.arrived(buf.at[self.at_quarter(self.q_sib, chunk)], plan["sib"][chunk])

    def gather_last(self, buf, plan):
        for chunk in range(CH):
            self.arrived(buf.at[self.at_quarter(self.q_d, chunk)], plan["pass"][chunk])

    def gathered(self, buf, plan, use):
        use(self.q)
        self.gather_sib(buf, plan)
        use(self.q_sib)
        self.gather_pass(buf, plan)
        use(self.q_x)
        self.gather_last(buf, plan)
        use(self.q_d)

    def scatter_start(self, partial, own, which, rx):
        sa, ra, sb, sc, rb = (self.rs.at[which, slot] for slot in range(5))
        plan = [[self.sem() for _ in range(CH)] for _ in range(3)]
        low = jnp.bfloat16
        for copy in self.groups[which]:
            copy.wait_send()
        self.groups[which] = []
        sa[...] = partial(self.q_d).astype(low)
        for chunk in range(CH):
            rows = self.at_chunk(chunk)
            self.send(sa.at[rows], ra.at[rows], self.sib, plan[0][chunk], which)
        held = partial(self.q_x)
        for chunk in range(CH):
            self.arrived(ra.at[self.at_chunk(chunk)], plan[0][chunk])
        sb[...] = (held + ra[...].astype(jnp.float32)).astype(low)
        for chunk in range(CH):
            rows = self.at_chunk(chunk)
            self.send(sb.at[rows], rx.at[rows], self.across, plan[1][chunk], which)
        sc[...] = partial(self.q_sib).astype(low)
        for chunk in range(CH):
            rows = self.at_chunk(chunk)
            self.send(sc.at[rows], rb.at[rows], self.sib, plan[2][chunk], which)
        own[...] = partial(self.q)
        return plan, which, rx

    def scatter_chunk(self, started, own, chunk):
        plan, which, rx = started
        rows = self.at_chunk(chunk)
        rb = self.rs.at[which, 4]
        self.arrived(rb.at[rows], plan[2][chunk])
        self.arrived(rx.at[rows], plan[1][chunk])
        return (
            own[rows, :] + rb[rows, :].astype(jnp.float32) + rx[rows, :].astype(jnp.float32)
        )

    def run(self):
        f32, low = jnp.float32, jnp.bfloat16
        rows, width = self.rows, self.width
        quarters = range(4)
        self.wbuf = dict(q=self.wq, o=self.wo, u=self.wu, d=self.wd)
        self.shard = dict(q=self.in_q, o=self.in_o, u=self.in_u, d=self.in_d)
        self.dbuf = dict(q=self.dq, o=self.do, u=self.du, d=self.dd)
        self.ybuf = dict(q=self.yq, o=self.yo, u=self.yu, d=self.yd)
        self.zbuf = dict(q=self.zq, o=self.zo, u=self.zu, d=self.zd)
        self.fbuf = dict(q=self.fq, o=self.fo, u=self.fu, d=self.fd)
        self.ebuf = dict(q=self.eq, o=self.eo, u=self.eu, d=self.ed)
        self.one, self.two, self.three, self.own = {}, {}, {}, {}
        self.back, self.backs, self.swaps, self.last = {}, {}, {}, {}
        self.pass_sem = {}
        heads, dim = self.qh.shape[0], self.qh.shape[2]
        hidden = self.wu.shape[2]

        self.barrier()
        move = [self.sem() for _ in range(4)]
        self.small_one()
        self.move_start(self.tok, self.xs, True, move[0])
        for kind in "qoud":
            self.weights_one(kind)
        plan_one, plan_two, plan_go, plan_mid = (self.gather_plan() for _ in range(4))
        self.weights_two("q")
        self.weights_cross("q", 0)
        self.small_two()
        for kind in "ou":
            self.weights_two(kind)
        landed = pl.ds(pl.multiple_of(self.z * rows, rows), rows)
        own_rows = self.at_quarter(self.q)
        self.move_start(self.go, self.gg.at[landed], True, move[1])
        self.weights_two("d")
        self.small_three()
        gain_one, shift_one = self.small[0:1, :], self.small[1:2, :]
        bias_out = self.small[2:3, :]
        gain_two, shift_two = self.small[3:4, :], self.small[4:5, :]
        bias_down = self.small[5:6, :]
        self.move_wait(self.tok, self.xs, move[0])

        for chunk in range(CH):
            part = self.at_chunk(chunk)
            normed, inverse = normalize(self.xs[part, :].astype(f32))
            self.n1[part, :] = normed
            self.i1[part, :] = inverse
            self.h1[self.at_quarter(self.q, chunk), :] = (normed * gain_one + shift_one).astype(low)
            self.gather_send(self.h1, plan_one, chunk)
        self.mask_blocks()
        self.gather_sib(self.h1, plan_one)
        self.gather_pass(self.h1, plan_one)
        self.gather_last(self.h1, plan_one)

        def parts_of(block):
            return ([(0, block * rows)] if block else []) + [(block * rows, rows)]

        near = 1 + 2 * ((3 - self.z) // 3)

        def turn(step):
            late, odd = step // 2, step % 2
            return (1 - late) * 2 * odd + late * (near + odd * (4 - 2 * near))

        def attend(step, carry):
            back = turn(step)
            head = (self.z - back + 4) % 4
            self.weights_ready("q", back)

            def project(block, carry):
                place = pl.ds(pl.multiple_of(block * rows, rows), rows)
                both = dot_last(self.h1[place, :], self.wq[head]) + self.bq[head]
                for slot, ref in enumerate((self.qh, self.kh, self.vh)):
                    value = both[:, slot * dim : (slot + 1) * dim].astype(low)
                    if slot == 0:
                        value = (value.astype(f32) * 0.125).astype(low)
                    ref[head, place, :] = value
                return carry

            lax.fori_loop(0, 4, project, 0)

            @pl.when(step < 3)
            def _():
                coming = turn(step + 1)
                self.weights_here("q", coming)
                self.weights_relay("q", step == 0)
                self.weights_cross("q", coming)

            @pl.when(step == 2)
            def _():
                self.weights_start_three("o")
                self.weights_three("o")

            @pl.when(step == 3)
            def _():
                self.weights_start_three("u")

            for block in quarters:
                place = pl.ds(block * rows, rows)
                query = self.qh[head, place, :]
                scores = []
                for first, count in parts_of(block):
                    value = dot_last(query, self.kh[head, pl.ds(first, count), :])
                    if first == block * rows:
                        value = value + self.mk[block].astype(f32)
                    scores.append(value)
                peak = functools.reduce(
                    jnp.maximum, [jnp.max(value, axis=1, keepdims=True) for value in scores]
                )
                powers = [jnp.exp(value - peak) for value in scores]
                total = sum(jnp.sum(value, axis=1, keepdims=True) for value in powers)
                scale = 1.0 / total
                result = 0.0
                for (first, count), value in zip(parts_of(block), powers):
                    probs = (value * scale).astype(low)
                    self.pb[block][head, :, pl.ds(first, count)] = probs
                    result = result + jnp.dot(
                        probs,
                        self.vh[head, pl.ds(first, count), :],
                        preferred_element_type=f32,
                    )
                self.hh[head, place, :] = result.astype(low)
            return carry

        lax.fori_loop(0, heads, attend, 0)
        for kind in "qou":
            self.relayed(kind)

        def assemble(target, refs, count):
            def one(block, carry):
                place = pl.ds(pl.multiple_of(block * rows, rows), rows)
                pieces = [ref[head, place, :] for ref in refs for head in range(count)]
                target[place, :] = jnp.concatenate(pieces, axis=1)
                return carry

            lax.fori_loop(0, 4, one, 0)

        assemble(self.ho, (self.hh,), heads)
        self.weights_done("o")

        flat_out = lambda: self.wo[...].reshape(heads * dim, width)
        started = self.scatter_start(
            lambda quarter: jnp.dot(
                self.ho[self.at_quarter(quarter), :], flat_out(), preferred_element_type=f32
            ),
            self.own_a,
            0,
            self.rx.at[0],
        )
        self.weights_three("u")
        for chunk in range(CH):
            part = self.at_chunk(chunk)
            summed = self.scatter_chunk(started, self.own_a, chunk)
            middle = self.xs[part, :].astype(f32) + (summed + bias_out)
            self.mid[part, :] = middle
            normed, inverse = normalize(middle)
            self.n2[part, :] = normed
            self.i2[part, :] = inverse
            self.h2[self.at_quarter(self.q, chunk), :] = (normed * gain_two + shift_two).astype(low)
            self.gather_send(self.h2, plan_two, chunk)
        self.move_wait(self.go, self.gg.at[landed], move[1])
        for chunk in range(CH):
            self.gather_send(self.gg, plan_go, chunk)
        self.weights_done("u")
        self.weights_start_three("d")
        self.relayed("d")

        def up(quarter):
            place = self.at_quarter(quarter)

            for block in range(4):
                lanes = pl.ds(block * hidden, hidden)
                value = (
                    jnp.dot(self.h2[place, :], self.wu[block], preferred_element_type=f32)
                    + self.bu[:, lanes]
                )
                square = value * value
                bend = jnp.tanh(ROOT * (value + 0.044715 * value * square))
                self.hid[place, lanes] = (0.5 * value * (1.0 + bend)).astype(low)
                slope = 0.5 * (1.0 + bend) + 0.5 * value * (1.0 - bend * bend) * ROOT * (
                    1.0 + 3.0 * 0.044715 * square
                )
                self.gu[place, lanes] = slope.astype(low)

        self.gathered(self.h2, plan_two, up)

        self.weights_three("d")
        self.weights_done("d")
        flat_down = lambda: self.wd[...].reshape(4 * hidden, width)
        started_down = self.scatter_start(
            lambda quarter: jnp.dot(
                self.hid[self.at_quarter(quarter), :], flat_down(), preferred_element_type=f32
            ),
            self.own_b,
            1,
            self.rx.at[1],
        )

        def to_up(quarter):
            place = self.at_quarter(quarter)
            value = dot_last(self.gg[place, :], flat_down())
            self.gu[place, :] = (self.gu[place, :].astype(f32) * value).astype(low)

        self.gathered(self.gg, plan_go, to_up)
        grad_out = self.gg[own_rows, :].astype(f32)
        self.sums[5:6, :] = jnp.sum(grad_out, axis=0, keepdims=True)

        def two_part(quarter):
            place = self.at_quarter(quarter)
            return sum(
                dot_last(self.gu[place, pl.ds(block * hidden, hidden)], self.wu[block])
                for block in range(4)
            )

        started = self.scatter_start(two_part, self.own_a, 0, self.rx.at[0])

        def down_grad(block, carry):
            lanes = pl.ds(pl.multiple_of(block * hidden, hidden), hidden)
            self.dd[block] = dot_first(self.hid[:, lanes], self.gg[...]).astype(low)
            return carry

        lax.fori_loop(0, 4, down_grad, 0)
        self.grads_one("d")
        step = width // 4

        def up_grad(block, carry):
            lanes = pl.ds(pl.multiple_of(block * step, step), step)
            value = dot_first(self.h2[:, lanes], self.gu[...]).astype(low)
            for plane in range(4):
                self.du[plane, lanes, :] = value[:, plane * hidden : (plane + 1) * hidden]
            return carry

        lax.fori_loop(0, 4, up_grad, 0)
        self.grads_one("u")
        totals = [0.0] * 3
        for chunk in range(CH):
            part = self.at_chunk(chunk)
            grad_two = self.scatter_chunk(started, self.own_a, chunk)
            normed = self.n2[part, :]
            middle = self.gg[self.at_quarter(self.q, chunk), :].astype(f32) + norm_back(
                grad_two, normed, self.i2[part, :], gain_two
            )
            self.gm[part, :] = middle
            self.ga[self.at_quarter(self.q, chunk), :] = middle.astype(low)
            self.gather_send(self.ga, plan_mid, chunk)
            for place, value in enumerate((grad_two * normed, grad_two, middle)):
                totals[place] = totals[place] + jnp.sum(value, axis=0, keepdims=True)
        self.sums[3:4, :] = totals[0]
        self.sums[4:5, :] = totals[1]
        self.sums[2:3, :] = totals[2]
        up_sum = jnp.sum(self.gu[...].astype(f32), axis=0, keepdims=True)
        lanes = self.part
        for place in range(8):
            self.cb[place // 2, 1 + place % 2 : 2 + place % 2, :] = up_sum[
                :, place * lanes : (place + 1) * lanes
            ]
        for chunk in range(CH):
            part = self.at_chunk(chunk)
            summed = self.scatter_chunk(started_down, self.own_b, chunk)
            self.ox[part, :] = (self.mid[part, :] + summed + bias_down).astype(low)
        self.move_start(self.ox, self.out, False, move[2])
        self.grads_two("d")

        def to_heads(quarter):
            place = self.at_quarter(quarter)
            value = dot_last(self.ga[place, :], flat_out()).astype(low)
            for head in range(heads):
                self.hh[head, place, :] = value[:, head * dim : (head + 1) * dim]

        self.gathered(self.ga, plan_mid, to_heads)
        self.grads_two("u")
        self.do[...] = dot_first(self.ho[...], self.ga[...]).astype(low).reshape(self.do.shape)
        self.grads_one("o")

        self.head_y, self.head_z = self.sem(4), self.sem(3)

        def attend_back(step, carry):
            head = (self.z + 1 + step) % 4
            self.ka[...] = jnp.zeros_like(self.ka)
            self.va[...] = jnp.zeros_like(self.va)
            for block in quarters:
                place = pl.ds(block * rows, rows)
                query = self.qh[head, place, :]
                grads = self.hh[head, place, :]
                probs, values = [], []
                inner = 0.0
                for first, count in parts_of(block):
                    span = pl.ds(first, count)
                    prob = self.pb[block][head, :, span]
                    value = dot_last(grads, self.vh[head, span, :])
                    self.va[span, :] += dot_first(prob, grads)
                    prob = prob.astype(f32)
                    inner = inner + jnp.sum(prob * value, axis=1, keepdims=True)
                    probs.append(prob)
                    values.append(value)
                result = 0.0
                for (first, count), prob, value in zip(parts_of(block), probs, values):
                    span = pl.ds(first, count)
                    score = (prob * (value - inner)).astype(low)
                    result = result + jnp.dot(
                        score, self.kh[head, span, :], preferred_element_type=f32
                    )
                    self.ka[span, :] += dot_first(score, query)
                self.qh[head, place, :] = (result * 0.125).astype(low)
            self.gp[head, :, 0:dim] = self.qh[head]
            self.gp[head, :, dim : 2 * dim] = self.ka[...].astype(low)
            self.gp[head, :, 2 * dim :] = self.va[...].astype(low)
            self.dq[head] = dot_first(self.gp[head], self.h1[...]).astype(low)
            self.head_one(step, head)

            @pl.when(step > 0)
            def _():
                before = (self.z + step) % 4
                self.head_add(step - 1, before)
                self.head_two(step - 1, before)

            return carry

        lax.fori_loop(0, heads, attend_back, 0)
        self.swaps["q"] = [self.head_z + step for step in range(3)]
        for step in range(4):
            self.later(lambda: self.cut("q", self.dq, 0, self.span(0)), self.head_y + step)
        for step in range(3):
            self.later(lambda: self.zq.at[0], self.head_z + step)
        self.grads_three("d")
        self.grads_three("u")
        self.grads_two("o")
        started = self.scatter_start(
            lambda quarter: sum(
                jnp.dot(
                    self.gp[head, self.at_quarter(quarter), :],
                    self.wq[head],
                    preferred_element_type=f32,
                )
                for head in range(heads)
            ),
            self.own_b,
            1,
            self.rx.at[2],
        )
        for head in range(heads):
            total = jnp.sum(self.gp[head].astype(f32), axis=0, keepdims=True)
            self.cb[head, 0:1, 0:dim] = total[:, 0:dim]
            self.cb[head, 0:1, dim:] = total[:, 2 * dim :]
            self.cb[head, 3:, :] = jnp.zeros((5, self.part), f32)
        self.head_add(3, self.z)
        self.grads_three("o")
        totals = [0.0] * 2
        for chunk in range(CH):
            part = self.at_chunk(chunk)
            grad_one = self.scatter_chunk(started, self.own_b, chunk)
            normed = self.n1[part, :]
            self.xs[part, :] = (
                self.gm[part, :] + norm_back(grad_one, normed, self.i1[part, :], gain_one)
            ).astype(low)
            for place, value in enumerate((grad_one * normed, grad_one)):
                totals[place] = totals[place] + jnp.sum(value, axis=0, keepdims=True)
        self.sums[0:1, :] = totals[0]
        self.sums[1:2, :] = totals[1]
        self.sums[6:8, :] = jnp.zeros((2, width), f32)
        self.back_one()
        self.move_start(self.xs, self.gtok, False, move[3])
        self.grads_three("q")
        self.back_two()
        for kind in "duoq":
            self.grads_done(kind)
        self.move_wait(self.ox, self.out, move[2])
        self.back_three()
        self.move_wait(self.xs, self.gtok, move[3])
        self.drain()

    def mask_blocks(self):
        rows = self.rows
        begins = self.lb[2 * self.z + self.y, 6:7, 0:4].astype(jnp.int32)
        for block in range(4):
            down = block * rows + lax.broadcasted_iota(jnp.int32, (rows, 1), 0)
            side = block * rows + lax.broadcasted_iota(jnp.int32, (1, rows), 1)

            def ids(places):
                total = jnp.zeros_like(places)
                for piece in range(4):
                    first = begins[:, piece : piece + 1]
                    inside = (places >= first) & (places < first + PIECE)
                    total = jnp.where(inside, piece + 1, total)
                return total

            mine, theirs = ids(down), ids(side)
            seen = (side <= down) | ((mine == theirs) & (mine > 0))
            self.mk[block] = jnp.where(seen, 0.0, -1e30).astype(jnp.bfloat16)


IN_NAMES = ("tok", "go", "in_q", "in_o", "in_u", "in_d", "si")
OUT_NAMES = ("out", "gtok", "eq", "eo", "eu", "ed", "fs", "fb")


def fused_layer(tok, go, in_q, in_o, in_u, in_d, si):
    rows, width = tok.shape
    heads, dim = 4, width // 16
    hidden = in_u.shape[1] // 4
    part = width // 8
    n = 4 * rows
    low, f32 = jnp.bfloat16, jnp.float32
    scratch = dict(
        xs=((rows, width), low),
        wq=((4, 3 * dim, width), low),
        wo=((4, dim, width), low),
        wu=((4, width, hidden), low),
        wd=((4, hidden, width), low),
        h1=((n, width), low),
        h2=((n, width), low),
        gg=((n, width), low),
        ga=((n, width), low),
        qh=((heads, n, dim), low),
        kh=((heads, n, dim), low),
        vh=((heads, n, dim), low),
        hh=((heads, n, dim), low),
        ho=((n, heads * dim), low),
        gp=((heads, n, 3 * dim), low),
        ka=((n, dim), f32),
        va=((n, dim), f32),
        mk=((4, rows, rows), low),
        n1=((rows, width), f32),
        n2=((rows, width), f32),
        mid=((rows, width), f32),
        gm=((rows, width), f32),
        i1=((rows, 1), f32),
        i2=((rows, 1), f32),
        own_a=((rows, width), f32),
        own_b=((rows, width), f32),
        hid=((n, 4 * hidden), low),
        gu=((n, 4 * hidden), low),
        ox=((rows, width), low),
        rs=((2, 5, rows, width), low),
        rx=((3, rows, width), low),
        dq=((4, 3 * dim, width), low),
        do=((4, dim, width), low),
        du=((4, width, hidden), low),
        dd=((4, hidden, width), low),
        yq=((4, 3 * dim, 4 * part), low),
        yo=((4, dim, 4 * part), low),
        yu=((4, 4 * part, hidden), low),
        yd=((4, hidden, 4 * part), low),
        zq=((3, 3 * dim, 4 * part), low),
        zo=((3, dim, 4 * part), low),
        zu=((3, 4 * part, hidden), low),
        zd=((3, hidden, 4 * part), low),
        fq=((3 * dim, 4 * part), low),
        fo=((dim, 4 * part), low),
        fu=((4 * part, hidden), low),
        fd=((hidden, 4 * part), low),
        small=((8, width), f32),
        sums=((8, width), f32),
        bq=((4, 1, 3 * dim), f32),
        bu=((1, 4 * hidden), f32),
        sma=((4, 5, 8, part), f32),
        lb=((8, 8, part), f32),
        bb=((8, 4, 8, part), f32),
        cs=((8, 8, part), f32),
        cr=((8, 8, part), f32),
        cb=((4, 8, part), f32),
        cd=((8, 4, 8, part), f32),
        es=((4, 8, part), f32),
        ed_small=((4, 4, 8, part), f32),
        eb=((4, 4, 8, part), f32),
    )
    probs = [((heads, rows, (block + 1) * rows), low) for block in range(4)]
    names = IN_NAMES + OUT_NAMES + tuple(scratch)

    def kernel(*refs):
        count = len(names)
        state = Fused(names, refs[:count])
        state.pb = refs[count : count + 4]
        state.ssem, state.rsem, state.lsem = refs[count + 4 :]
        state.run()

    hbm = pl.BlockSpec(memory_space=pl.ANY)
    vmem = pl.BlockSpec(memory_space=pltpu.VMEM)
    return pl.pallas_call(
        kernel,
        out_shape=(
            jax.ShapeDtypeStruct((rows, width), low),
            jax.ShapeDtypeStruct((rows, width), low),
            jax.ShapeDtypeStruct((4, 3 * dim, part), low),
            jax.ShapeDtypeStruct((4, dim, part), low),
            jax.ShapeDtypeStruct((4, part, hidden), low),
            jax.ShapeDtypeStruct((4, hidden, part), low),
            jax.ShapeDtypeStruct((8, part), f32),
            jax.ShapeDtypeStruct((4, 8, part), f32),
        ),
        in_specs=[hbm] * 6 + [vmem],
        out_specs=(hbm,) * 6 + (vmem,) * 2,
        scratch_shapes=[pltpu.VMEM(*spec) for spec in scratch.values()]
        + [pltpu.VMEM(*spec) for spec in probs]
        + [pltpu.SemaphoreType.DMA((SEMS,))] * 3,
        name="fused_layer",
        compiler_params=pltpu.CompilerParams(
            collective_id=0, has_side_effects=True, vmem_limit_bytes=VMEM_LIMIT
        ),
    )(tok, go, in_q, in_o, in_u, in_d, si)


SEMS = 256
VMEM_LIMIT = 67043328


def per_device_fused(
    tokens_in, starts, ln1_gain, ln1_bias, w_qkv, b_qv, w_out, b_out,
    ln2_gain, ln2_bias, w_up, b_up, w_down, b_down, grad_out,
):
    rows, width = tokens_in.shape
    f32 = jnp.float32
    dp, z = lax.axis_index("dp"), lax.axis_index("tensor")
    part = width // 8
    dim = width // 16
    hidden = w_up.shape[1] // 4
    bit = ln1_gain.shape[0]
    here = jnp.arange(part) // bit == z
    vectors = jnp.stack([ln1_gain, ln1_bias, b_out, ln2_gain, ln2_bias, b_down])
    vectors = jnp.where(here, jnp.tile(vectors, (1, part // bit)), 0.0)
    begins = jnp.where(z == 0, starts.astype(f32), 0.0)
    begins = jnp.pad(begins, ((0, 1), (0, part - 4)))
    spot = (jnp.arange(8) == dp)[:, None]

    def spread(bias):
        entries = bias.astype(f32).reshape(4, -1, 1, bias.shape[1])
        return jnp.where(spot, entries, 0.0).reshape(4, -1, part)

    biases = jnp.concatenate(
        [spread(b_qv), spread(b_up), jnp.zeros((4, 5, part), f32)], axis=1
    )
    si = jnp.concatenate([jnp.concatenate([vectors, begins])[None], biases])
    in_q = w_qkv.reshape(part, 4, 3 * dim).transpose(1, 2, 0)
    in_o = w_out.reshape(4, dim, part)
    in_d = w_down.reshape(4, hidden, part)
    out, gtok, eq, eo, eu, ed, fs, fb = fused_layer(
        tokens_in, grad_out, in_q, in_o, w_up, in_d, si
    )
    grad_w_qkv = eq.transpose(2, 0, 1).reshape(part, 3 * 4 * dim).astype(f32)
    grad_w_out = eo.reshape(4 * dim, part).astype(f32)
    grad_w_up = eu.transpose(1, 0, 2).reshape(part, 4 * hidden).astype(f32)
    grad_w_down = ed.reshape(4 * hidden, part).astype(f32)
    take = lax.dynamic_slice_in_dim(fs, z * bit, bit, 1)

    def collect(rows, like):
        entries = rows.reshape(4, -1, 8, like.shape[1])
        return lax.dynamic_index_in_dim(entries, dp, 2, keepdims=False).reshape(like.shape)

    grad_b_qv = collect(fb[:, 0], b_qv)
    grad_b_up = collect(fb[:, 1:3], b_up)
    return (
        out, gtok, take[0], take[1], grad_w_qkv, grad_b_qv, grad_w_out, take[2],
        take[3], take[4], grad_w_up, grad_b_up, grad_w_down, take[5],
    )


def solution(mesh):
    sizes = (mesh.shape["dp"], mesh.shape["tensor"])

    def layer(tokens_in, starts, *others):
        fits = sizes == (8, 4) and tokens_in.shape[0] == PIECE and starts.shape == (1, 4)
        return (per_device_fused if fits else per_device)(tokens_in, starts, *others)

    return jax.shard_map(
        layer,
        mesh=mesh,
        in_specs=(
            P(("dp", "tensor"), None),
            P("dp", None),
            P(("dp", "tensor")),
            P(("dp", "tensor")),
            P("dp", "tensor"),
            P("tensor", "dp"),
            P("tensor", "dp"),
            P(("dp", "tensor")),
            P(("dp", "tensor")),
            P(("dp", "tensor")),
            P("dp", "tensor"),
            P("tensor", "dp"),
            P("tensor", "dp"),
            P(("dp", "tensor")),
            P(("dp", "tensor"), None),
        ),
        out_specs=(
            P(("dp", "tensor"), None),
            P(("dp", "tensor"), None),
            P(("dp", "tensor")),
            P(("dp", "tensor")),
            P("dp", "tensor"),
            P("tensor", "dp"),
            P("tensor", "dp"),
            P(("dp", "tensor")),
            P(("dp", "tensor")),
            P(("dp", "tensor")),
            P("dp", "tensor"),
            P("tensor", "dp"),
            P("tensor", "dp"),
            P(("dp", "tensor")),
        ),
        check_vma=False,
    )
```

```python
import functools

import jax
import jax.numpy as jnp
from jax import lax
from jax.experimental import pallas as pl
from jax.experimental.pallas import tpu as pltpu
from jax.sharding import PartitionSpec as P

HD = 64
PIECE = 256
QBLOCK = 512


EPS = 1e-05
ROOT = 0.7978845608028654


def gelu_tanh(values):
    return 0.5 * values * (1.0 + jnp.tanh(ROOT * (values + 0.044715 * values * values * values)))


def normalize(values):
    center = jnp.mean(values, axis=-1, keepdims=True)
    shifted = values - center
    inverse = lax.rsqrt(jnp.mean(shifted * shifted, axis=-1, keepdims=True) + EPS)
    return (shifted * inverse, inverse)


def norm_back(grad_normed, normed, inverse, gain):
    scaled = grad_normed * gain
    return inverse * (
        scaled
        - jnp.mean(scaled, axis=-1, keepdims=True)
        - normed * jnp.mean(scaled * normed, axis=-1, keepdims=True)
    )


def dot_last(left, right):
    return lax.dot_general(
        left, right, (((1,), (1,)), ((), ())), preferred_element_type=jnp.float32
    )


def dot_first(left, right):
    return lax.dot_general(
        left, right, (((0,), (0,)), ((), ())), preferred_element_type=jnp.float32
    )


def gather_rows(values):
    return lax.all_gather(values, "tensor", axis=0, tiled=True)


def gather_grads(values):
    return lax.all_gather(values, "tensor", axis=0, tiled=True)


def reduce_rows(left, weight, rows):

    def term(start, count):
        return jnp.dot(left, weight, preferred_element_type=jnp.float32)

    return lax.psum_scatter(
        term(jnp.int32(0), lax.axis_size("tensor") * rows).astype(jnp.bfloat16),
        "tensor",
        scatter_dimension=0,
        tiled=True,
    ).astype(jnp.float32)


def reduce_grads(left, weight, rows):

    def term(start, count):
        return dot_last(left, weight)

    return lax.psum_scatter(
        term(jnp.int32(0), lax.axis_size("tensor") * rows).astype(jnp.bfloat16),
        "tensor",
        scatter_dimension=0,
        tiled=True,
    ).astype(jnp.float32)


def piece_ids(start_row, length):
    places = jnp.arange(length, dtype=jnp.int32)
    inside = (places[:, None] >= start_row[None, :]) & (
        places[:, None] < start_row[None, :] + PIECE
    )
    labels = jnp.arange(1, start_row.shape[0] + 1, dtype=jnp.int32)
    return jnp.sum(jnp.where(inside, labels[None, :], 0), axis=1)


def allowed_block(row_ids, row_places, key_ids, key_places):
    causal = key_places[None, :] <= row_places[:, None]
    picture = (row_ids[:, None] == key_ids[None, :]) & (row_ids[:, None] > 0)
    return causal | picture


def block_scores(by_seq, start_rows, block_index):
    length = by_seq.shape[1]
    per_seq = length // QBLOCK
    seq_index = block_index // per_seq
    first_row = block_index % per_seq * QBLOCK
    sequence = lax.dynamic_index_in_dim(by_seq, seq_index, 0, keepdims=False)
    key_ids = piece_ids(lax.dynamic_index_in_dim(start_rows, seq_index, 0, keepdims=False), length)
    query_rows = lax.dynamic_slice_in_dim(sequence, first_row, QBLOCK, 0)[:, :, 0]
    key_rows = sequence[:, :, 1]
    value_rows = sequence[:, :, 2]
    row_ids = lax.dynamic_slice_in_dim(key_ids, first_row, QBLOCK, 0)
    row_places = first_row + jnp.arange(QBLOCK, dtype=jnp.int32)
    scores = (
        jnp.einsum("qhd,khd->hqk", query_rows, key_rows, preferred_element_type=jnp.float32) * 0.125
    )
    places = jnp.arange(length, dtype=jnp.int32)
    scores = jnp.where(allowed_block(row_ids, row_places, key_ids, places)[None], scores, -1e30)
    return (seq_index, first_row, query_rows, key_rows, value_rows, scores)


def attention_forward(by_seq, start_rows):
    total_blocks = by_seq.shape[0] * (by_seq.shape[1] // QBLOCK)

    def attend(block_index):
        _, _, query_rows, key_rows, value_rows, scores = block_scores(
            by_seq, start_rows, block_index
        )
        peak = jnp.max(scores, axis=-1, keepdims=True)
        log_total = peak + jnp.log(jnp.sum(jnp.exp(scores - peak), axis=-1, keepdims=True))
        probs = jnp.exp(scores - log_total)
        heads = jnp.einsum(
            "hqk,khd->qhd",
            probs.astype(jnp.bfloat16),
            value_rows,
            preferred_element_type=jnp.float32,
        )
        return (heads.astype(jnp.bfloat16), log_total)

    return lax.map(attend, jnp.arange(total_blocks, dtype=jnp.int32))


def attention_backward(by_seq, start_rows, log_totals, grad_heads):
    total_blocks = by_seq.shape[0] * (by_seq.shape[1] // QBLOCK)
    empty = jnp.zeros(by_seq.shape[:3] + (HD,), jnp.float32)

    def step(carry, item):
        grad_keys, grad_values = carry
        block_index, log_total = item
        seq_index, first_row, query_rows, key_rows, value_rows, scores = block_scores(
            by_seq, start_rows, block_index
        )
        grad_seq = lax.dynamic_index_in_dim(grad_heads, seq_index, 0, keepdims=False)
        grad_rows = lax.dynamic_slice_in_dim(grad_seq, first_row, QBLOCK, 0)
        probs = jnp.exp(scores - log_total)
        grad_probs = jnp.einsum(
            "qhd,khd->hqk", grad_rows, value_rows, preferred_element_type=jnp.float32
        )
        inner = jnp.sum(probs * grad_probs, axis=-1, keepdims=True)
        grad_scores = (probs * (grad_probs - inner)).astype(jnp.bfloat16)
        grad_query = (
            jnp.einsum("hqk,khd->qhd", grad_scores, key_rows, preferred_element_type=jnp.float32)
            * 0.125
        )
        key_term = (
            jnp.einsum("hqk,qhd->khd", grad_scores, query_rows, preferred_element_type=jnp.float32)
            * 0.125
        )
        value_term = jnp.einsum(
            "hqk,qhd->khd",
            probs.astype(jnp.bfloat16),
            grad_rows,
            preferred_element_type=jnp.float32,
        )
        grad_keys = lax.dynamic_update_index_in_dim(
            grad_keys,
            lax.dynamic_index_in_dim(grad_keys, seq_index, 0, keepdims=False) + key_term,
            seq_index,
            0,
        )
        grad_values = lax.dynamic_update_index_in_dim(
            grad_values,
            lax.dynamic_index_in_dim(grad_values, seq_index, 0, keepdims=False) + value_term,
            seq_index,
            0,
        )
        return ((grad_keys, grad_values), grad_query)

    (grad_keys, grad_values), grad_query = lax.scan(
        step, (empty, empty), (jnp.arange(total_blocks, dtype=jnp.int32), log_totals)
    )
    return (grad_query, grad_keys, grad_values)


def per_device(
    tokens_in,
    starts,
    ln1_gain,
    ln1_bias,
    w_qkv,
    b_qv,
    w_out,
    b_out,
    ln2_gain,
    ln2_bias,
    w_up,
    b_up,
    w_down,
    b_down,
    grad_out,
):
    rows = tokens_in.shape[0]
    gain_one, shift_one, bias_out, gain_two, shift_two, bias_down = (
        lax.all_gather(ln1_gain, ("dp", "tensor"), axis=0, tiled=True),
        lax.all_gather(ln1_bias, ("dp", "tensor"), axis=0, tiled=True),
        lax.all_gather(b_out, ("dp", "tensor"), axis=0, tiled=True),
        lax.all_gather(ln2_gain, ("dp", "tensor"), axis=0, tiled=True),
        lax.all_gather(ln2_bias, ("dp", "tensor"), axis=0, tiled=True),
        lax.all_gather(b_down, ("dp", "tensor"), axis=0, tiled=True),
    )
    weight_qkv, bias_qv, weight_out = (
        lax.all_gather(w_qkv, "dp", axis=0, tiled=True),
        lax.all_gather(b_qv, "dp", axis=1, tiled=True),
        lax.all_gather(w_out, "dp", axis=1, tiled=True),
    )
    weight_up, bias_up, weight_down = (
        lax.all_gather(w_up, "dp", axis=0, tiled=True),
        lax.all_gather(b_up, "dp", axis=1, tiled=True),
        lax.all_gather(w_down, "dp", axis=1, tiled=True),
    )
    local_heads = weight_qkv.shape[1] // (3 * HD)
    seq_count = starts.shape[0]
    inputs = tokens_in.astype(jnp.float32)
    normed_one, inverse_one = normalize(inputs)
    gathered_one = gather_rows((normed_one * gain_one + shift_one).astype(jnp.bfloat16))
    group = gathered_one.shape[0]
    length = group // seq_count
    bias_pair = bias_qv.astype(jnp.float32).reshape(local_heads, 2, HD)
    full_bias = jnp.stack(
        [bias_pair[:, 0], jnp.zeros_like(bias_pair[:, 0]), bias_pair[:, 1]], axis=1
    )
    projected = (
        jnp.dot(gathered_one, weight_qkv, preferred_element_type=jnp.float32).reshape(
            group, local_heads, 3, HD
        )
        + full_bias
    ).astype(jnp.bfloat16)
    by_seq = projected.reshape(seq_count, length, local_heads, 3, HD)
    heads_blocks, log_totals = attention_forward(by_seq, starts)
    heads_out = heads_blocks.reshape(group, local_heads * HD)
    middle = inputs + (reduce_rows(heads_out, weight_out, rows) + bias_out)
    normed_two, inverse_two = normalize(middle)
    rounded_two = (normed_two * gain_two + shift_two).astype(jnp.bfloat16)
    grad_final = grad_out.astype(jnp.float32)
    grad_bias_down = jnp.sum(grad_final, axis=0)
    gathered_two = gather_rows(rounded_two)
    up_proj = jnp.dot(gathered_two, weight_up, preferred_element_type=jnp.float32) + bias_up.astype(
        jnp.float32
    ).reshape(-1)
    hidden_act, gelu_pull = jax.vjp(gelu_tanh, up_proj)
    hidden_low = hidden_act.astype(jnp.bfloat16)
    output = (middle + reduce_rows(hidden_low, weight_down, rows) + bias_down).astype(jnp.bfloat16)
    grad_branch = gather_grads(grad_out)
    grad_w_down = dot_first(hidden_low, grad_branch)
    grad_up = gelu_pull(dot_last(grad_branch, weight_down))[0].astype(jnp.bfloat16)
    grad_b_up = jnp.sum(grad_up, axis=0, dtype=jnp.float32).reshape(bias_up.shape)
    grad_w_up = dot_first(gathered_two, grad_up)
    grad_two = reduce_grads(grad_up, weight_up, rows)
    grad_w_up, grad_b_up, grad_w_down = (
        lax.psum_scatter(
            grad_w_up.astype(jnp.bfloat16), "dp", scatter_dimension=0, tiled=True
        ).astype(jnp.float32),
        lax.psum_scatter(
            grad_b_up.astype(jnp.bfloat16), "dp", scatter_dimension=1, tiled=True
        ).astype(jnp.float32),
        lax.psum_scatter(
            grad_w_down.astype(jnp.bfloat16), "dp", scatter_dimension=1, tiled=True
        ).astype(jnp.float32),
    )
    grad_gain_two = jnp.sum(grad_two * normed_two, axis=0)
    grad_shift_two = jnp.sum(grad_two, axis=0)
    grad_middle = grad_final + norm_back(grad_two, normed_two, inverse_two, gain_two)
    grad_bias_out = jnp.sum(grad_middle, axis=0)
    grad_attn = gather_grads(grad_middle.astype(jnp.bfloat16))
    grad_w_out = dot_first(heads_out, grad_attn)
    grad_heads = (
        dot_last(grad_attn, weight_out)
        .astype(jnp.bfloat16)
        .reshape(seq_count, length, local_heads, HD)
    )
    grad_query, grad_keys, grad_values = attention_backward(by_seq, starts, log_totals, grad_heads)
    grad_proj = jnp.stack(
        [
            grad_query.reshape(group, local_heads, HD),
            grad_keys.reshape(group, local_heads, HD),
            grad_values.reshape(group, local_heads, HD),
        ],
        axis=2,
    ).astype(jnp.bfloat16)
    grad_b_qv = jnp.sum(grad_proj[:, :, 0::2], axis=0, dtype=jnp.float32).reshape(bias_qv.shape)
    grad_flat = grad_proj.reshape(group, 3 * local_heads * HD)
    grad_w_qkv = dot_first(gathered_one, grad_flat)
    grad_one = reduce_grads(grad_flat, weight_qkv, rows)
    grad_w_qkv, grad_b_qv, grad_w_out = (
        lax.psum_scatter(
            grad_w_qkv.astype(jnp.bfloat16), "dp", scatter_dimension=0, tiled=True
        ).astype(jnp.float32),
        lax.psum_scatter(
            grad_b_qv.astype(jnp.bfloat16), "dp", scatter_dimension=1, tiled=True
        ).astype(jnp.float32),
        lax.psum_scatter(
            grad_w_out.astype(jnp.bfloat16), "dp", scatter_dimension=1, tiled=True
        ).astype(jnp.float32),
    )
    grad_gain_one = jnp.sum(grad_one * normed_one, axis=0)
    grad_shift_one = jnp.sum(grad_one, axis=0)
    grad_tokens = (grad_middle + norm_back(grad_one, normed_one, inverse_one, gain_one)).astype(
        jnp.bfloat16
    )
    summed = (
        lax.psum_scatter(grad_gain_one, ("dp", "tensor"), scatter_dimension=0, tiled=True),
        lax.psum_scatter(grad_shift_one, ("dp", "tensor"), scatter_dimension=0, tiled=True),
        lax.psum_scatter(grad_bias_out, ("dp", "tensor"), scatter_dimension=0, tiled=True),
        lax.psum_scatter(grad_gain_two, ("dp", "tensor"), scatter_dimension=0, tiled=True),
        lax.psum_scatter(grad_shift_two, ("dp", "tensor"), scatter_dimension=0, tiled=True),
        lax.psum_scatter(grad_bias_down, ("dp", "tensor"), scatter_dimension=0, tiled=True),
    )
    return (
        output,
        grad_tokens,
        summed[0],
        summed[1],
        grad_w_qkv,
        grad_b_qv,
        grad_w_out,
        summed[2],
        summed[3],
        summed[4],
        grad_w_up,
        grad_b_up,
        grad_w_down,
        summed[5],
    )


MESH = pl.DeviceIdType.MESH
CH = 2
HOPS = 4


class Fused:
    def __init__(self, names, refs):
        for name, ref in zip(names, refs):
            setattr(self, name, ref)
        self.next_sem = 0
        self.unsent = []
        self.groups = {0: [], 1: []}
        self.unsent_later = []
        dp, self.z = lax.axis_index("dp"), lax.axis_index("tensor")
        self.y, self.x, self.c = dp // 4, (dp // 2) % 2, dp % 2
        self.j = self.member(self.x, self.c)
        self.q = self.quarter(self.j)
        self.sib = self.dev(self.y, self.x, 1 - self.c, self.z)
        self.across = self.dev(self.y, 1 - self.x, self.c, self.z)
        self.q_sib = self.quarter(self.member(self.x, 1 - self.c))
        self.q_x = self.quarter(self.member(1 - self.x, self.c))
        self.q_d = self.quarter(self.member(1 - self.x, 1 - self.c))
        self.rows = self.tok.shape[0]
        self.width = self.tok.shape[1]
        self.part = self.width // 8

    def dev(self, y, x, c, z):
        return ((y * 2 + x) * 2 + c, z)

    def member(self, x, c):
        return 2 * c + x

    def local(self, member):
        return 2 * (member % 2) + member // 2

    def mate(self, member):
        return self.dev(self.y, member % 2, member // 2, self.z)

    def quarter(self, member):
        return (member - self.z + 4) % 4

    def sem(self, count=1):
        index = self.next_sem
        self.next_sem += count
        return index

    def copy(self, src, dst, device, index, sent=None):
        return pltpu.make_async_remote_copy(
            src_ref=src,
            dst_ref=dst,
            send_sem=self.ssem.at[index if sent is None else sent],
            recv_sem=self.rsem.at[index],
            device_id=device,
            device_id_type=MESH,
        )

    def send(self, src, dst, device, index, group=None):
        copy = self.copy(src, dst, device, index)
        copy.start()
        (self.unsent if group is None else self.groups[group]).append(copy)

    def later(self, view, sent, when=None):
        self.unsent_later.append((view, sent, when))

    def arrived(self, dst, index):
        self.copy(dst, dst, self.sib, index).wait_recv()

    def drain(self):
        for copy in self.unsent + self.groups[0] + self.groups[1]:
            copy.wait_send()
        for view, sent, when in self.unsent_later:
            copy = self.copy(view(), view(), self.sib, sent)
            if when is None:
                copy.wait_send()
            else:
                pl.when(when())(copy.wait_send)

    def at_quarter(self, quarter, chunk=None):
        if chunk is None:
            return pl.ds(pl.multiple_of(quarter * self.rows, self.rows), self.rows)
        size = self.rows // CH
        return pl.ds(pl.multiple_of(quarter * self.rows + chunk * size, size), size)

    def at_chunk(self, chunk):
        size = self.rows // CH
        return pl.ds(chunk * size, size)

    def barrier(self):
        me = lax.axis_index("dp") * 4 + self.z
        bar = pltpu.get_barrier_semaphore()

        def greet(step, carry):
            other = (me + step) % 32
            pl.semaphore_signal(
                bar, inc=1, device_id=(other // 4, other % 4), device_id_type=MESH
            )
            return carry

        lax.fori_loop(1, 32, greet, 0)
        pl.semaphore_wait(bar, 31)

    def homes(self):
        plane = 2 * self.y + self.x
        member = (plane + self.z) % 4
        worker = (self.c, member % 2, member // 2, plane)
        owner = (self.z // 2, self.z % 2, self.y, self.q)
        same = (
            (worker[0] == self.y)
            & (worker[1] == self.x)
            & (worker[2] == self.c)
            & (worker[3] == self.z)
        )
        return self.dev(*worker), self.dev(*owner), same

    def move_start(self, src, dst, outward, index):
        worker, owner, same = self.homes()
        copy = self.copy(src, dst, worker if outward else owner, index)
        local = pltpu.make_async_copy(src, dst, self.lsem.at[index])

        @pl.when(jnp.logical_not(same))
        def _():
            copy.start()

        @pl.when(same)
        def _():
            local.start()

    def move_wait(self, src, dst, index):
        same = self.homes()[2]
        copy = self.copy(src, dst, self.sib, index)
        local = pltpu.make_async_copy(src, dst, self.lsem.at[index])

        @pl.when(jnp.logical_not(same))
        def _():
            copy.wait_send()
            copy.wait_recv()

        @pl.when(same)
        def _():
            local.wait()

    def hop_rows(self, chunk):
        size = self.rows // HOPS
        return pl.ds(chunk * size, size)

    def hop_one(self, src, mid, index):
        plane = 2 * self.y + self.x
        member = (plane + self.z) % 4
        first = self.dev(self.c, member % 2, member // 2, self.z)
        same = (self.c == self.y) & (member % 2 == self.x) & (member // 2 == self.c)
        for chunk in range(HOPS):
            view, there = src.at[self.hop_rows(chunk)], mid.at[self.hop_rows(chunk)]
            copy = self.copy(view, there, first, index + chunk)
            local = pltpu.make_async_copy(view, there, self.lsem.at[index + chunk])
            pl.when(jnp.logical_not(same))(copy.start)
            pl.when(same)(local.start)

    def hop_two(self, src, mid, dst, place, index, onward):
        plane = (self.j - self.z + 4) % 4
        member = (2 * self.y + self.x + self.z) % 4
        home = (self.c == self.y) & (member % 2 == self.x) & (member // 2 == self.c)
        stay = plane == self.z
        for chunk in range(HOPS):
            rows = self.hop_rows(chunk)
            size = self.rows // HOPS
            there = dst.at[pl.ds(pl.multiple_of(place + chunk * size, size), size)]
            first = self.copy(src.at[rows], mid.at[rows], self.sib, index + chunk)
            local = pltpu.make_async_copy(src.at[rows], mid.at[rows], self.lsem.at[index + chunk])
            pl.when(jnp.logical_not(home))(first.wait_send)
            pl.when(jnp.logical_not(home))(first.wait_recv)
            pl.when(home)(local.wait)
            copy = self.copy(
                mid.at[rows], there, self.dev(self.y, self.x, self.c, plane), onward + chunk
            )
            keep = pltpu.make_async_copy(mid.at[rows], there, self.lsem.at[onward + chunk])
            pl.when(jnp.logical_not(stay))(copy.start)
            pl.when(stay)(keep.start)

    def hop_wait(self, mid, dst, place, onward):
        plane = (self.j - self.z + 4) % 4
        stay = plane == self.z
        for chunk in range(HOPS):
            rows = self.hop_rows(chunk)
            size = self.rows // HOPS
            there = dst.at[pl.ds(pl.multiple_of(place + chunk * size, size), size)]
            copy = self.copy(mid.at[rows], there, self.sib, onward + chunk)
            keep = pltpu.make_async_copy(mid.at[rows], there, self.lsem.at[onward + chunk])
            pl.when(jnp.logical_not(stay))(copy.wait_send)
            pl.when(jnp.logical_not(stay))(copy.wait_recv)
            pl.when(stay)(keep.wait)

    def span(self, half):
        return pl.ds(pl.multiple_of(half * 4 * self.part, 4 * self.part), 4 * self.part)

    def place(self, source):
        return pl.ds(pl.multiple_of(source * self.part, self.part), self.part)

    def cut(self, kind, ref, zc, where):
        if kind == "u":
            return ref.at[zc, where, :]
        return ref.at[zc, :, where]

    def piece(self, kind, ref, member):
        if kind == "u":
            wide = self.wbuf["u"].shape[2]
            return ref.at[:, pl.ds(pl.multiple_of(member * wide, wide), wide)]
        return ref.at[member]

    def weights_one(self, kind):
        source = 4 * self.y + self.local(self.j)
        here = self.cut(kind, self.wbuf[kind], self.z, self.place(source))
        self.one[kind] = []
        for step in range(1, 4):
            member = (self.j + step) % 4
            index = self.sem()
            self.send(
                self.piece(kind, self.shard[kind], member), here, self.mate(member), index
            )
            sender = 4 * self.y + self.local((self.j - step + 4) % 4)
            self.one[kind].append(
                (self.cut(kind, self.wbuf[kind], self.z, self.place(sender)), index)
            )
        index = self.sem()
        local = pltpu.make_async_copy(
            self.piece(kind, self.shard[kind], self.j), here, self.lsem.at[index]
        )
        local.start()
        self.own[kind] = local
        self.two[kind] = self.sem(4)
        self.three[kind] = self.sem(4)
        self.pass_sem[kind] = self.sem()

    def mine(self, kind, plane):
        return self.cut(kind, self.wbuf[kind], plane, self.span(self.y))

    def weights_two(self, kind):
        self.own[kind].wait()
        for view, index in self.one[kind]:
            self.arrived(view, index)
        here = self.mine(kind, self.z)
        for step, when in ((2, None), (1, lambda: self.z != 3), (3, lambda: self.z != 0)):
            plane = (self.z + step) % 4
            index = self.two[kind] + step
            copy = self.copy(here, here, self.dev(self.y, self.x, self.c, plane), index)
            if when is None:
                copy.start()
            else:
                pl.when(when())(copy.start)
            self.later(lambda: self.mine(kind, self.z), index, when)

    def weights_relay(self, kind, guard=None):
        for here, plane, step in ((2, 3, 3), (1, 0, 1)):
            when = self.z == here
            block = self.mine(kind, (here + 2) % 4)
            copy = self.copy(
                block,
                block,
                self.dev(self.y, self.x, self.c, plane),
                self.two[kind] + step,
                self.pass_sem[kind],
            )
            pl.when(when if guard is None else when & guard)(copy.start)

    def relayed(self, kind):
        self.later(
            lambda: self.mine(kind, self.z),
            self.pass_sem[kind],
            lambda: (self.z == 1) | (self.z == 2),
        )
        for step in range(4):
            self.later(lambda: self.mine(kind, self.z), self.three[kind] + step)

    def weights_cross(self, kind, step):
        mine = self.mine(kind, (self.z - step + 4) % 4)
        self.copy(
            mine,
            mine,
            self.dev(1 - self.y, self.x, self.c, self.z),
            self.three[kind] + step,
        ).start()

    def weights_here(self, kind, step):
        self.arrived(self.mine(kind, (self.z - step + 4) % 4), self.two[kind] + step)

    def weights_three(self, kind, steps=(1, 3)):
        for step in steps:
            self.weights_here(kind, step)
            self.weights_cross(kind, step)

    def weights_start_three(self, kind):
        self.weights_cross(kind, 0)
        self.weights_here(kind, 2)
        self.weights_relay(kind)
        self.weights_cross(kind, 2)

    def weights_ready(self, kind, step):
        plane = (self.z - step + 4) % 4
        self.arrived(
            self.cut(kind, self.wbuf[kind], plane, self.span(1 - self.y)),
            self.three[kind] + step,
        )

    def weights_done(self, kind):
        for step in range(4):
            self.weights_ready(kind, step)

    def grads_one(self, kind):
        index = self.sem()
        self.back[kind] = index
        for plane in range(4):
            away = self.cut(kind, self.dbuf[kind], plane, self.span(1 - self.y))
            there = self.cut(kind, self.ybuf[kind], plane, slice(None))
            use = index if plane == 0 else self.sem()
            self.send(away, there, self.dev(1 - self.y, self.x, self.c, self.z), use)
            self.backs.setdefault(kind, []).append(use)

    def grads_two(self, kind):
        for plane in range(4):
            there = self.cut(kind, self.ybuf[kind], plane, slice(None))
            self.arrived(there, self.backs[kind][plane])
            mine = self.cut(kind, self.dbuf[kind], plane, self.span(self.y))
            mine[...] = (
                mine[...].astype(jnp.float32) + there[...].astype(jnp.float32)
            ).astype(jnp.bfloat16)
        self.swaps[kind] = []
        for step in range(1, 4):
            plane = (self.z + step) % 4
            index = self.sem()
            self.send(
                self.cut(kind, self.dbuf[kind], plane, self.span(self.y)),
                self.zbuf[kind].at[step - 1],
                self.dev(self.y, self.x, self.c, plane),
                index,
            )
            self.swaps[kind].append(index)

    def head_one(self, step, head):
        self.copy(
            self.cut("q", self.dq, head, self.span(1 - self.y)),
            self.cut("q", self.yq, head, slice(None)),
            self.dev(1 - self.y, self.x, self.c, self.z),
            self.head_y + step,
        ).start()

    def head_add(self, step, head):
        there = self.cut("q", self.yq, head, slice(None))
        self.arrived(there, self.head_y + step)
        mine = self.cut("q", self.dq, head, self.span(self.y))
        mine[...] = (mine[...].astype(jnp.float32) + there[...].astype(jnp.float32)).astype(
            jnp.bfloat16
        )

    def head_two(self, step, head):
        self.copy(
            self.cut("q", self.dq, head, self.span(self.y)),
            self.zq.at[step],
            self.dev(self.y, self.x, self.c, head),
            self.head_z + step,
        ).start()

    def grads_three(self, kind):
        mine = self.cut(kind, self.dbuf[kind], self.z, self.span(self.y))
        total = mine[...].astype(jnp.float32)
        for step in range(1, 4):
            there = self.zbuf[kind].at[step - 1]
            self.arrived(there, self.swaps[kind][step - 1])
            total = total + there[...].astype(jnp.float32)
        final = self.fbuf[kind]
        final[...] = total.astype(jnp.bfloat16)
        ends = self.ebuf[kind]
        self.last[kind] = []
        for step in range(1, 4):
            member = (self.j + step) % 4
            index = self.sem()
            self.send(
                self.slab(kind, final, self.local(member)),
                ends.at[self.j],
                self.mate(member),
                index,
            )
            self.last[kind].append(((self.j - step + 4) % 4, index))
        index = self.sem()
        local = pltpu.make_async_copy(
            self.slab(kind, final, self.local(self.j)), ends.at[self.j], self.lsem.at[index]
        )
        local.start()
        self.own[kind] = local

    def slab(self, kind, ref, member):
        where = pl.ds(pl.multiple_of(member * self.part, self.part), self.part)
        if kind == "u":
            return ref.at[where, :]
        return ref.at[:, where]

    def grads_done(self, kind):
        self.own[kind].wait()
        for member, index in self.last[kind]:
            self.arrived(self.ebuf[kind].at[member], index)

    def small_one(self):
        self.sma[self.z] = self.si[...]
        self.small_sem = [self.sem() for _ in range(3)]
        for step in range(1, 4):
            plane = (self.z + step) % 4
            self.send(
                self.si,
                self.sma.at[self.z],
                self.dev(self.y, self.x, self.c, plane),
                self.small_sem[step - 1],
            )

    def around(self, step):
        return (lax.axis_index("dp") + step + 8) % 8

    def small_two(self):
        for step in range(1, 4):
            self.arrived(self.sma.at[(self.z - step + 4) % 4], self.small_sem[step - 1])
        me = self.around(0)
        self.lb[me] = sum(self.sma[plane, 0] for plane in range(4))
        self.bb[me] = self.sma[:, 1 + self.j]
        self.plane_sem = [(self.sem(), self.sem()) for _ in range(7)]
        for step in range(1, 8):
            other = self.around(step)
            member = self.member((other // 2) % 2, other % 2)
            first, second = self.plane_sem[step - 1]
            self.send(self.lb.at[me], self.lb.at[me], (other, self.z), first)
            self.send(self.sma.at[:, 1 + member], self.bb.at[me], (other, self.z), second)

    def small_three(self):
        for step in range(1, 8):
            other = self.around(-step)
            first, second = self.plane_sem[step - 1]
            self.arrived(self.lb.at[other], first)
            self.arrived(self.bb.at[other], second)
        part, dim = self.part, self.qh.shape[2]
        for source in range(8):
            self.small[:, source * part : (source + 1) * part] = self.lb[source]
        bias = sum(self.bb[source] for source in range(8))
        for head in range(4):
            row = bias[head, 0:1]
            self.bq[head, :, 0:dim] = row[:, 0:dim]
            self.bq[head, :, dim : 2 * dim] = jnp.zeros((1, dim), jnp.float32)
            self.bq[head, :, 2 * dim :] = row[:, dim:]
            for half in range(2):
                place = (2 * head + half) * part
                self.bu[:, place : place + part] = bias[head, 1 + half : 2 + half]

    def back_one(self):
        part, me = self.part, self.around(0)
        for target in range(8):
            self.cs[target] = self.sums[:, target * part : (target + 1) * part]
        self.cr[me] = self.cs[me]
        self.cd[me] = self.cb[...]
        self.back_sem = [(self.sem(), self.sem()) for _ in range(7)]
        for step in range(1, 8):
            other = self.around(step)
            first, second = self.back_sem[step - 1]
            self.send(self.cs.at[other], self.cr.at[me], (other, self.z), first)
            self.send(self.cb, self.cd.at[me], (other, self.z), second)

    def back_two(self):
        for step in range(1, 8):
            other = self.around(-step)
            first, second = self.back_sem[step - 1]
            self.arrived(self.cr.at[other], first)
            self.arrived(self.cd.at[other], second)
        self.es[self.z] = sum(self.cr[source] for source in range(8))
        for member in range(4):
            pair = [2 * (member % 2) + member // 2, 4 + 2 * (member % 2) + member // 2]
            self.ed_small[:, member] = self.cd[pair[0]] + self.cd[pair[1]]
        self.eb[self.z] = self.ed_small[self.z]
        self.line_sem = [(self.sem(), self.sem()) for _ in range(3)]
        for step in range(1, 4):
            plane = (self.z + step) % 4
            device = self.dev(self.y, self.x, self.c, plane)
            first, second = self.line_sem[step - 1]
            self.send(self.es.at[self.z], self.es.at[self.z], device, first)
            self.send(self.ed_small.at[plane], self.eb.at[self.z], device, second)

    def back_three(self):
        for step in range(1, 4):
            plane = (self.z - step + 4) % 4
            first, second = self.line_sem[step - 1]
            self.arrived(self.es.at[plane], first)
            self.arrived(self.eb.at[plane], second)
        self.fs[...] = sum(self.es[plane] for plane in range(4))
        self.fb[...] = sum(self.eb[plane] for plane in range(4))

    def gather_plan(self):
        return {kind: [self.sem() for _ in range(CH)] for kind in ("across", "sib", "pass")}

    def gather_send(self, buf, plan, chunk):
        rows = self.at_quarter(self.q, chunk)
        self.send(buf.at[rows], buf.at[rows], self.across, plan["across"][chunk])
        self.send(buf.at[rows], buf.at[rows], self.sib, plan["sib"][chunk])

    def gather_pass(self, buf, plan):
        for chunk in range(CH):
            rows = self.at_quarter(self.q_x, chunk)
            self.arrived(buf.at[rows], plan["across"][chunk])
            self.send(buf.at[rows], buf.at[rows], self.sib, plan["pass"][chunk])

    def gather_sib(self, buf, plan):
        for chunk in range(CH):
            self.arrived(buf.at[self.at_quarter(self.q_sib, chunk)], plan["sib"][chunk])

    def gather_last(self, buf, plan):
        for chunk in range(CH):
            self.arrived(buf.at[self.at_quarter(self.q_d, chunk)], plan["pass"][chunk])

    def gathered(self, buf, plan, use):
        use(self.q)
        self.gather_sib(buf, plan)
        use(self.q_sib)
        self.gather_pass(buf, plan)
        use(self.q_x)
        self.gather_last(buf, plan)
        use(self.q_d)

    def scatter_start(self, partial, own, which, rx):
        sa, ra, sb, sc, rb = (self.rs.at[which, slot] for slot in range(5))
        plan = [[self.sem() for _ in range(CH)] for _ in range(3)]
        low = jnp.bfloat16
        for copy in self.groups[which]:
            copy.wait_send()
        self.groups[which] = []
        sa[...] = partial(self.q_d).astype(low)
        for chunk in range(CH):
            rows = self.at_chunk(chunk)
            self.send(sa.at[rows], ra.at[rows], self.sib, plan[0][chunk], which)
        held = partial(self.q_x)
        for chunk in range(CH):
            self.arrived(ra.at[self.at_chunk(chunk)], plan[0][chunk])
        sb[...] = (held + ra[...].astype(jnp.float32)).astype(low)
        for chunk in range(CH):
            rows = self.at_chunk(chunk)
            self.send(sb.at[rows], rx.at[rows], self.across, plan[1][chunk], which)
        sc[...] = partial(self.q_sib).astype(low)
        for chunk in range(CH):
            rows = self.at_chunk(chunk)
            self.send(sc.at[rows], rb.at[rows], self.sib, plan[2][chunk], which)
        own[...] = partial(self.q)
        return plan, which, rx

    def scatter_chunk(self, started, own, chunk):
        plan, which, rx = started
        rows = self.at_chunk(chunk)
        rb = self.rs.at[which, 4]
        self.arrived(rb.at[rows], plan[2][chunk])
        self.arrived(rx.at[rows], plan[1][chunk])
        return (
            own[rows, :] + rb[rows, :].astype(jnp.float32) + rx[rows, :].astype(jnp.float32)
        )

    def run(self):
        f32, low = jnp.float32, jnp.bfloat16
        rows, width = self.rows, self.width
        quarters = range(4)
        self.wbuf = dict(q=self.wq, o=self.wo, u=self.wu, d=self.wd)
        self.shard = dict(q=self.in_q, o=self.in_o, u=self.in_u, d=self.in_d)
        self.dbuf = dict(q=self.dq, o=self.do, u=self.du, d=self.dd)
        self.ybuf = dict(q=self.yq, o=self.yo, u=self.yu, d=self.yd)
        self.zbuf = dict(q=self.zq, o=self.zo, u=self.zu, d=self.zd)
        self.fbuf = dict(q=self.fq, o=self.fo, u=self.fu, d=self.fd)
        self.ebuf = dict(q=self.eq, o=self.eo, u=self.eu, d=self.ed)
        self.one, self.two, self.three, self.own = {}, {}, {}, {}
        self.back, self.backs, self.swaps, self.last = {}, {}, {}, {}
        self.pass_sem = {}
        heads, dim = self.qh.shape[0], self.qh.shape[2]
        hidden = self.wu.shape[2]

        self.barrier()
        move = [self.sem() for _ in range(4)]
        self.small_one()
        hop = [self.sem(HOPS) for _ in range(4)]
        self.hop_one(self.tok, self.mid_x, hop[0])
        self.weights_one("q")
        plan_one, plan_two, plan_go, plan_mid = (self.gather_plan() for _ in range(4))
        self.hop_two(self.tok, self.mid_x, self.xs, 0, hop[0], hop[1])
        self.small_two()
        own_rows = self.at_quarter(self.q)
        self.small_three()
        gain_one, shift_one = self.small[0:1, :], self.small[1:2, :]
        bias_out = self.small[2:3, :]
        gain_two, shift_two = self.small[3:4, :], self.small[4:5, :]
        bias_down = self.small[5:6, :]
        self.hop_wait(self.mid_x, self.xs, 0, hop[1])

        for chunk in range(CH):
            part = self.at_chunk(chunk)
            normed, inverse = normalize(self.xs[part, :].astype(f32))
            self.n1[part, :] = normed
            self.i1[part, :] = inverse
            self.h1[self.at_quarter(self.q, chunk), :] = (normed * gain_one + shift_one).astype(low)
            self.gather_send(self.h1, plan_one, chunk)
        self.weights_two("q")
        self.weights_cross("q", 0)
        self.mask_blocks()
        self.gather_sib(self.h1, plan_one)
        self.gather_pass(self.h1, plan_one)
        for kind in "oud":
            self.weights_one(kind)
        self.gather_last(self.h1, plan_one)

        def parts_of(block):
            return ([(0, block * rows)] if block else []) + [(block * rows, rows)]

        near = 1 + 2 * ((3 - self.z) // 3)

        def turn(step):
            late, odd = step // 2, step % 2
            return (1 - late) * 2 * odd + late * (near + odd * (4 - 2 * near))

        def attend(step, carry):
            back = turn(step)
            head = (self.z - back + 4) % 4
            self.weights_ready("q", back)

            def project(block, carry):
                place = pl.ds(pl.multiple_of(block * rows, rows), rows)
                both = dot_last(self.h1[place, :], self.wq[head]) + self.bq[head]
                for slot, ref in enumerate((self.qh, self.kh, self.vh)):
                    value = both[:, slot * dim : (slot + 1) * dim].astype(low)
                    if slot == 0:
                        value = (value.astype(f32) * 0.125).astype(low)
                    ref[head, place, :] = value
                return carry

            lax.fori_loop(0, 4, project, 0)

            @pl.when(step < 3)
            def _():
                coming = turn(step + 1)
                self.weights_here("q", coming)
                self.weights_relay("q", step == 0)
                self.weights_cross("q", coming)

            @pl.when(step == 1)
            def _():
                self.weights_two("o")
                self.weights_two("u")
                self.hop_one(self.go, self.ox, hop[2])

            @pl.when(step == 3)
            def _():
                self.weights_start_three("o")
                self.weights_three("o")

            for block in quarters:
                place = pl.ds(block * rows, rows)
                query = self.qh[head, place, :]
                scores = []
                for first, count in parts_of(block):
                    value = dot_last(query, self.kh[head, pl.ds(first, count), :])
                    if first == block * rows:
                        value = value + self.mk[block].astype(f32)
                    scores.append(value)
                peak = functools.reduce(
                    jnp.maximum, [jnp.max(value, axis=1, keepdims=True) for value in scores]
                )
                powers = [jnp.exp(value - peak) for value in scores]
                total = sum(jnp.sum(value, axis=1, keepdims=True) for value in powers)
                scale = 1.0 / total
                result = 0.0
                for (first, count), value in zip(parts_of(block), powers):
                    probs = (value * scale).astype(low)
                    self.pb[block][head, :, pl.ds(first, count)] = probs
                    result = result + jnp.dot(
                        probs,
                        self.vh[head, pl.ds(first, count), :],
                        preferred_element_type=f32,
                    )
                self.hh[head, place, :] = result.astype(low)
            return carry

        lax.fori_loop(0, heads, attend, 0)
        for kind in "qou":
            self.relayed(kind)

        def assemble(target, refs, count):
            def one(block, carry):
                place = pl.ds(pl.multiple_of(block * rows, rows), rows)
                pieces = [ref[head, place, :] for ref in refs for head in range(count)]
                target[place, :] = jnp.concatenate(pieces, axis=1)
                return carry

            lax.fori_loop(0, 4, one, 0)

        assemble(self.ho, (self.hh,), heads)
        self.weights_done("o")

        flat_out = lambda: self.wo[...].reshape(heads * dim, width)
        started = self.scatter_start(
            lambda quarter: jnp.dot(
                self.ho[self.at_quarter(quarter), :], flat_out(), preferred_element_type=f32
            ),
            self.own_a,
            0,
            self.rx.at[0],
        )
        self.weights_start_three("u")
        self.hop_two(self.go, self.ox, self.gg, self.z * rows, hop[2], hop[3])
        self.weights_three("u")
        for chunk in range(CH):
            part = self.at_chunk(chunk)
            summed = self.scatter_chunk(started, self.own_a, chunk)
            middle = self.xs[part, :].astype(f32) + (summed + bias_out)
            self.mid[part, :] = middle
            normed, inverse = normalize(middle)
            self.n2[part, :] = normed
            self.i2[part, :] = inverse
            self.h2[self.at_quarter(self.q, chunk), :] = (normed * gain_two + shift_two).astype(low)
            self.gather_send(self.h2, plan_two, chunk)
        self.weights_two("d")
        self.weights_done("u")

        def up(quarter):
            place = self.at_quarter(quarter)

            for block in range(4):
                lanes = pl.ds(block * hidden, hidden)
                value = (
                    jnp.dot(self.h2[place, :], self.wu[block], preferred_element_type=f32)
                    + self.bu[:, lanes]
                )
                square = value * value
                bend = jnp.tanh(ROOT * (value + 0.044715 * value * square))
                self.hid[place, lanes] = (0.5 * value * (1.0 + bend)).astype(low)
                slope = 0.5 * (1.0 + bend) + 0.5 * value * (1.0 - bend * bend) * ROOT * (
                    1.0 + 3.0 * 0.044715 * square
                )
                self.gu[place, lanes] = slope.astype(low)

        self.gathered(self.h2, plan_two, up)

        self.hop_wait(self.ox, self.gg, self.q * rows, hop[3])
        for chunk in range(CH):
            self.gather_send(self.gg, plan_go, chunk)
        flat_down = lambda: self.wd[...].reshape(4 * hidden, width)
        self.weights_start_three("d")
        self.relayed("d")
        self.weights_three("d")
        self.gather_sib(self.gg, plan_go)
        self.gather_pass(self.gg, plan_go)
        grad_out = self.gg[own_rows, :].astype(f32)
        self.sums[5:6, :] = jnp.sum(grad_out, axis=0, keepdims=True)
        self.gather_last(self.gg, plan_go)

        def down_grad(block, carry):
            lanes = pl.ds(pl.multiple_of(block * hidden, hidden), hidden)
            self.dd[block] = dot_first(self.hid[:, lanes], self.gg[...]).astype(low)
            return carry

        lax.fori_loop(0, 4, down_grad, 0)
        self.grads_one("d")
        self.weights_done("d")

        def to_up(quarter):
            place = self.at_quarter(quarter)
            value = dot_last(self.gg[place, :], flat_down())
            self.gu[place, :] = (self.gu[place, :].astype(f32) * value).astype(low)

        for quarter in (self.q_d, self.q_x, self.q_sib, self.q):
            to_up(quarter)

        def two_part(quarter):
            place = self.at_quarter(quarter)
            return sum(
                dot_last(self.gu[place, pl.ds(block * hidden, hidden)], self.wu[block])
                for block in range(4)
            )

        started = self.scatter_start(two_part, self.own_a, 0, self.rx.at[0])

        step = width // 4

        def up_grad(block, carry):
            lanes = pl.ds(pl.multiple_of(block * step, step), step)
            value = dot_first(self.h2[:, lanes], self.gu[...]).astype(low)
            for plane in range(4):
                self.du[plane, lanes, :] = value[:, plane * hidden : (plane + 1) * hidden]
            return carry

        lax.fori_loop(0, 4, up_grad, 0)
        self.grads_one("u")
        totals = [0.0] * 3
        for chunk in range(CH):
            part = self.at_chunk(chunk)
            grad_two = self.scatter_chunk(started, self.own_a, chunk)
            normed = self.n2[part, :]
            middle = self.gg[self.at_quarter(self.q, chunk), :].astype(f32) + norm_back(
                grad_two, normed, self.i2[part, :], gain_two
            )
            self.gm[part, :] = middle
            self.ga[self.at_quarter(self.q, chunk), :] = middle.astype(low)
            self.gather_send(self.ga, plan_mid, chunk)
            for place, value in enumerate((grad_two * normed, grad_two, middle)):
                totals[place] = totals[place] + jnp.sum(value, axis=0, keepdims=True)
        self.sums[3:4, :] = totals[0]
        self.sums[4:5, :] = totals[1]
        self.sums[2:3, :] = totals[2]
        up_sum = jnp.sum(self.gu[...].astype(f32), axis=0, keepdims=True)
        lanes = self.part
        for place in range(8):
            self.cb[place // 2, 1 + place % 2 : 2 + place % 2, :] = up_sum[
                :, place * lanes : (place + 1) * lanes
            ]
        def to_heads(quarter):
            place = self.at_quarter(quarter)
            value = dot_last(self.ga[place, :], flat_out()).astype(low)
            for head in range(heads):
                self.hh[head, place, :] = value[:, head * dim : (head + 1) * dim]

        self.gathered(self.ga, plan_mid, to_heads)
        self.grads_two("d")
        started_down = self.scatter_start(
            lambda quarter: jnp.dot(
                self.hid[self.at_quarter(quarter), :], flat_down(), preferred_element_type=f32
            ),
            self.own_b,
            1,
            self.rx.at[1],
        )
        self.do[...] = dot_first(self.ho[...], self.ga[...]).astype(low).reshape(self.do.shape)
        self.grads_one("o")

        self.head_y, self.head_z = self.sem(4), self.sem(3)

        def attend_back(step, carry):
            head = (self.z + 1 + step) % 4
            self.ka[...] = jnp.zeros_like(self.ka)
            self.va[...] = jnp.zeros_like(self.va)
            for block in quarters:
                place = pl.ds(block * rows, rows)
                query = self.qh[head, place, :]
                grads = self.hh[head, place, :]
                probs, values = [], []
                inner = 0.0
                for first, count in parts_of(block):
                    span = pl.ds(first, count)
                    prob = self.pb[block][head, :, span]
                    value = dot_last(grads, self.vh[head, span, :])
                    self.va[span, :] += dot_first(prob, grads)
                    prob = prob.astype(f32)
                    inner = inner + jnp.sum(prob * value, axis=1, keepdims=True)
                    probs.append(prob)
                    values.append(value)
                result = 0.0
                for (first, count), prob, value in zip(parts_of(block), probs, values):
                    span = pl.ds(first, count)
                    score = (prob * (value - inner)).astype(low)
                    result = result + jnp.dot(
                        score, self.kh[head, span, :], preferred_element_type=f32
                    )
                    self.ka[span, :] += dot_first(score, query)
                self.qh[head, place, :] = (result * 0.125).astype(low)
            self.gp[head, :, 0:dim] = self.qh[head]
            self.gp[head, :, dim : 2 * dim] = self.ka[...].astype(low)
            self.gp[head, :, 2 * dim :] = self.va[...].astype(low)
            self.dq[head] = dot_first(self.gp[head], self.h1[...]).astype(low)
            self.head_one(step, head)

            @pl.when(step > 0)
            def _():
                before = (self.z + step) % 4
                self.head_add(step - 1, before)
                self.head_two(step - 1, before)

            @pl.when(step == 1)
            def _():
                for chunk in range(CH):
                    part = self.at_chunk(chunk)
                    summed = self.scatter_chunk(started_down, self.own_b, chunk)
                    self.ox[part, :] = (self.mid[part, :] + summed + bias_down).astype(low)
                self.move_start(self.ox, self.out, False, move[2])

            return carry

        lax.fori_loop(0, heads, attend_back, 0)
        self.swaps["q"] = [self.head_z + step for step in range(3)]
        for step in range(4):
            self.later(lambda: self.cut("q", self.dq, 0, self.span(0)), self.head_y + step)
        for step in range(3):
            self.later(lambda: self.zq.at[0], self.head_z + step)
        started = self.scatter_start(
            lambda quarter: sum(
                jnp.dot(
                    self.gp[head, self.at_quarter(quarter), :],
                    self.wq[head],
                    preferred_element_type=f32,
                )
                for head in range(heads)
            ),
            self.own_a,
            0,
            self.rx.at[0],
        )
        self.grads_two("u")
        self.grads_two("o")
        for head in range(heads):
            total = jnp.sum(self.gp[head].astype(f32), axis=0, keepdims=True)
            self.cb[head, 0:1, 0:dim] = total[:, 0:dim]
            self.cb[head, 0:1, dim:] = total[:, 2 * dim :]
            self.cb[head, 3:, :] = jnp.zeros((5, self.part), f32)
        self.head_add(3, self.z)
        self.grads_three("d")
        totals = [0.0] * 2
        for chunk in range(CH):
            part = self.at_chunk(chunk)
            grad_one = self.scatter_chunk(started, self.own_a, chunk)
            normed = self.n1[part, :]
            self.xs[part, :] = (
                self.gm[part, :] + norm_back(grad_one, normed, self.i1[part, :], gain_one)
            ).astype(low)
            for place, value in enumerate((grad_one * normed, grad_one)):
                totals[place] = totals[place] + jnp.sum(value, axis=0, keepdims=True)
        self.sums[0:1, :] = totals[0]
        self.sums[1:2, :] = totals[1]
        self.sums[6:8, :] = jnp.zeros((2, width), f32)
        self.back_one()
        self.move_start(self.xs, self.gtok, False, move[3])
        self.grads_three("u")
        self.grads_three("o")
        self.back_two()
        self.grads_three("q")
        for kind in "duoq":
            self.grads_done(kind)
        self.move_wait(self.ox, self.out, move[2])
        self.back_three()
        self.move_wait(self.xs, self.gtok, move[3])
        self.drain()

    def mask_blocks(self):
        rows = self.rows
        begins = self.lb[2 * self.z + self.y, 6:7, 0:4].astype(jnp.int32)
        for block in range(4):
            down = block * rows + lax.broadcasted_iota(jnp.int32, (rows, 1), 0)
            side = block * rows + lax.broadcasted_iota(jnp.int32, (1, rows), 1)

            def ids(places):
                total = jnp.zeros_like(places)
                for piece in range(4):
                    first = begins[:, piece : piece + 1]
                    inside = (places >= first) & (places < first + PIECE)
                    total = jnp.where(inside, piece + 1, total)
                return total

            mine, theirs = ids(down), ids(side)
            seen = (side <= down) | ((mine == theirs) & (mine > 0))
            self.mk[block] = jnp.where(seen, 0.0, -1e30).astype(jnp.bfloat16)


IN_NAMES = ("tok", "go", "in_q", "in_o", "in_u", "in_d", "si")
OUT_NAMES = ("out", "gtok", "eq", "eo", "eu", "ed", "fs", "fb")


def fused_layer(tok, go, in_q, in_o, in_u, in_d, si):
    rows, width = tok.shape
    heads, dim = 4, width // 16
    hidden = in_u.shape[1] // 4
    part = width // 8
    n = 4 * rows
    low, f32 = jnp.bfloat16, jnp.float32
    scratch = dict(
        xs=((rows, width), low),
        mid_x=((rows, width), low),
        wq=((4, 3 * dim, width), low),
        wo=((4, dim, width), low),
        wu=((4, width, hidden), low),
        wd=((4, hidden, width), low),
        h1=((n, width), low),
        h2=((n, width), low),
        gg=((n, width), low),
        ga=((n, width), low),
        qh=((heads, n, dim), low),
        kh=((heads, n, dim), low),
        vh=((heads, n, dim), low),
        hh=((heads, n, dim), low),
        ho=((n, heads * dim), low),
        gp=((heads, n, 3 * dim), low),
        ka=((n, dim), f32),
        va=((n, dim), f32),
        mk=((4, rows, rows), low),
        n1=((rows, width), f32),
        n2=((rows, width), f32),
        mid=((rows, width), f32),
        gm=((rows, width), f32),
        i1=((rows, 1), f32),
        i2=((rows, 1), f32),
        own_a=((rows, width), f32),
        own_b=((rows, width), f32),
        hid=((n, 4 * hidden), low),
        gu=((n, 4 * hidden), low),
        ox=((rows, width), low),
        rs=((2, 5, rows, width), low),
        rx=((2, rows, width), low),
        dq=((4, 3 * dim, width), low),
        do=((4, dim, width), low),
        du=((4, width, hidden), low),
        dd=((4, hidden, width), low),
        yq=((4, 3 * dim, 4 * part), low),
        yo=((4, dim, 4 * part), low),
        yu=((4, 4 * part, hidden), low),
        yd=((4, hidden, 4 * part), low),
        zq=((3, 3 * dim, 4 * part), low),
        zo=((3, dim, 4 * part), low),
        zu=((3, 4 * part, hidden), low),
        zd=((3, hidden, 4 * part), low),
        fq=((3 * dim, 4 * part), low),
        fo=((dim, 4 * part), low),
        fu=((4 * part, hidden), low),
        fd=((hidden, 4 * part), low),
        small=((8, width), f32),
        sums=((8, width), f32),
        bq=((4, 1, 3 * dim), f32),
        bu=((1, 4 * hidden), f32),
        sma=((4, 5, 8, part), f32),
        lb=((8, 8, part), f32),
        bb=((8, 4, 8, part), f32),
        cs=((8, 8, part), f32),
        cr=((8, 8, part), f32),
        cb=((4, 8, part), f32),
        cd=((8, 4, 8, part), f32),
        es=((4, 8, part), f32),
        ed_small=((4, 4, 8, part), f32),
        eb=((4, 4, 8, part), f32),
    )
    probs = [((heads, rows, (block + 1) * rows), low) for block in range(4)]
    names = IN_NAMES + OUT_NAMES + tuple(scratch)

    def kernel(*refs):
        count = len(names)
        state = Fused(names, refs[:count])
        state.pb = refs[count : count + 4]
        state.ssem, state.rsem, state.lsem = refs[count + 4 :]
        state.run()

    hbm = pl.BlockSpec(memory_space=pl.ANY)
    vmem = pl.BlockSpec(memory_space=pltpu.VMEM)
    return pl.pallas_call(
        kernel,
        out_shape=(
            jax.ShapeDtypeStruct((rows, width), low),
            jax.ShapeDtypeStruct((rows, width), low),
            jax.ShapeDtypeStruct((4, 3 * dim, part), low),
            jax.ShapeDtypeStruct((4, dim, part), low),
            jax.ShapeDtypeStruct((4, part, hidden), low),
            jax.ShapeDtypeStruct((4, hidden, part), low),
            jax.ShapeDtypeStruct((8, part), f32),
            jax.ShapeDtypeStruct((4, 8, part), f32),
        ),
        in_specs=[hbm] * 6 + [vmem],
        out_specs=(hbm,) * 6 + (vmem,) * 2,
        scratch_shapes=[pltpu.VMEM(*spec) for spec in scratch.values()]
        + [pltpu.VMEM(*spec) for spec in probs]
        + [pltpu.SemaphoreType.DMA((SEMS,))] * 3,
        name="fused_layer",
        compiler_params=pltpu.CompilerParams(
            collective_id=0, has_side_effects=True, vmem_limit_bytes=VMEM_LIMIT
        ),
    )(tok, go, in_q, in_o, in_u, in_d, si)


SEMS = 256
VMEM_LIMIT = 67043328


def per_device_fused(
    tokens_in, starts, ln1_gain, ln1_bias, w_qkv, b_qv, w_out, b_out,
    ln2_gain, ln2_bias, w_up, b_up, w_down, b_down, grad_out,
):
    rows, width = tokens_in.shape
    f32 = jnp.float32
    dp, z = lax.axis_index("dp"), lax.axis_index("tensor")
    part = width // 8
    dim = width // 16
    hidden = w_up.shape[1] // 4
    bit = ln1_gain.shape[0]
    here = jnp.arange(part) // bit == z
    vectors = jnp.stack([ln1_gain, ln1_bias, b_out, ln2_gain, ln2_bias, b_down])
    vectors = jnp.where(here, jnp.tile(vectors, (1, part // bit)), 0.0)
    begins = jnp.where(z == 0, starts.astype(f32), 0.0)
    begins = jnp.pad(begins, ((0, 1), (0, part - 4)))
    spot = (jnp.arange(8) == dp)[:, None]

    def spread(bias):
        entries = bias.astype(f32).reshape(4, -1, 1, bias.shape[1])
        return jnp.where(spot, entries, 0.0).reshape(4, -1, part)

    biases = jnp.concatenate(
        [spread(b_qv), spread(b_up), jnp.zeros((4, 5, part), f32)], axis=1
    )
    si = jnp.concatenate([jnp.concatenate([vectors, begins])[None], biases])
    in_q = w_qkv.reshape(part, 4, 3 * dim).transpose(1, 2, 0)
    in_o = w_out.reshape(4, dim, part)
    in_d = w_down.reshape(4, hidden, part)
    out, gtok, eq, eo, eu, ed, fs, fb = fused_layer(
        tokens_in, grad_out, in_q, in_o, w_up, in_d, si
    )
    grad_w_qkv = eq.transpose(2, 0, 1).reshape(part, 3 * 4 * dim).astype(f32)
    grad_w_out = eo.reshape(4 * dim, part).astype(f32)
    grad_w_up = eu.transpose(1, 0, 2).reshape(part, 4 * hidden).astype(f32)
    grad_w_down = ed.reshape(4 * hidden, part).astype(f32)
    take = lax.dynamic_slice_in_dim(fs, z * bit, bit, 1)

    def collect(rows, like):
        entries = rows.reshape(4, -1, 8, like.shape[1])
        return lax.dynamic_index_in_dim(entries, dp, 2, keepdims=False).reshape(like.shape)

    grad_b_qv = collect(fb[:, 0], b_qv)
    grad_b_up = collect(fb[:, 1:3], b_up)
    return (
        out, gtok, take[0], take[1], grad_w_qkv, grad_b_qv, grad_w_out, take[2],
        take[3], take[4], grad_w_up, grad_b_up, grad_w_down, take[5],
    )


def solution(mesh):
    sizes = (mesh.shape["dp"], mesh.shape["tensor"])

    def layer(tokens_in, starts, *others):
        fits = sizes == (8, 4) and tokens_in.shape[0] == PIECE and starts.shape == (1, 4)
        return (per_device_fused if fits else per_device)(tokens_in, starts, *others)

    return jax.shard_map(
        layer,
        mesh=mesh,
        in_specs=(
            P(("dp", "tensor"), None),
            P("dp", None),
            P(("dp", "tensor")),
            P(("dp", "tensor")),
            P("dp", "tensor"),
            P("tensor", "dp"),
            P("tensor", "dp"),
            P(("dp", "tensor")),
            P(("dp", "tensor")),
            P(("dp", "tensor")),
            P("dp", "tensor"),
            P("tensor", "dp"),
            P("tensor", "dp"),
            P(("dp", "tensor")),
            P(("dp", "tensor"), None),
        ),
        out_specs=(
            P(("dp", "tensor"), None),
            P(("dp", "tensor"), None),
            P(("dp", "tensor")),
            P(("dp", "tensor")),
            P("dp", "tensor"),
            P("tensor", "dp"),
            P("tensor", "dp"),
            P(("dp", "tensor")),
            P(("dp", "tensor")),
            P(("dp", "tensor")),
            P("dp", "tensor"),
            P("tensor", "dp"),
            P("tensor", "dp"),
            P(("dp", "tensor")),
        ),
        check_vma=False,
    )
```

```python
import functools

import jax
import jax.numpy as jnp
from jax import lax
from jax.experimental import pallas as pl
from jax.experimental.pallas import tpu as pltpu
from jax.sharding import PartitionSpec as P

HD = 64
PIECE = 256
QBLOCK = 512


EPS = 1e-05
ROOT = 0.7978845608028654


def gelu_tanh(values):
    return 0.5 * values * (1.0 + jnp.tanh(ROOT * (values + 0.044715 * values * values * values)))


def normalize(values):
    center = jnp.mean(values, axis=-1, keepdims=True)
    shifted = values - center
    inverse = lax.rsqrt(jnp.mean(shifted * shifted, axis=-1, keepdims=True) + EPS)
    return (shifted * inverse, inverse)


def norm_back(grad_normed, normed, inverse, gain):
    scaled = grad_normed * gain
    return inverse * (
        scaled
        - jnp.mean(scaled, axis=-1, keepdims=True)
        - normed * jnp.mean(scaled * normed, axis=-1, keepdims=True)
    )


def dot_last(left, right):
    return lax.dot_general(
        left, right, (((1,), (1,)), ((), ())), preferred_element_type=jnp.float32
    )


def dot_first(left, right):
    return lax.dot_general(
        left, right, (((0,), (0,)), ((), ())), preferred_element_type=jnp.float32
    )


def gather_rows(values):
    return lax.all_gather(values, "tensor", axis=0, tiled=True)


def gather_grads(values):
    return lax.all_gather(values, "tensor", axis=0, tiled=True)


def reduce_rows(left, weight, rows):

    def term(start, count):
        return jnp.dot(left, weight, preferred_element_type=jnp.float32)

    return lax.psum_scatter(
        term(jnp.int32(0), lax.axis_size("tensor") * rows).astype(jnp.bfloat16),
        "tensor",
        scatter_dimension=0,
        tiled=True,
    ).astype(jnp.float32)


def reduce_grads(left, weight, rows):

    def term(start, count):
        return dot_last(left, weight)

    return lax.psum_scatter(
        term(jnp.int32(0), lax.axis_size("tensor") * rows).astype(jnp.bfloat16),
        "tensor",
        scatter_dimension=0,
        tiled=True,
    ).astype(jnp.float32)


def piece_ids(start_row, length):
    places = jnp.arange(length, dtype=jnp.int32)
    inside = (places[:, None] >= start_row[None, :]) & (
        places[:, None] < start_row[None, :] + PIECE
    )
    labels = jnp.arange(1, start_row.shape[0] + 1, dtype=jnp.int32)
    return jnp.sum(jnp.where(inside, labels[None, :], 0), axis=1)


def allowed_block(row_ids, row_places, key_ids, key_places):
    causal = key_places[None, :] <= row_places[:, None]
    picture = (row_ids[:, None] == key_ids[None, :]) & (row_ids[:, None] > 0)
    return causal | picture


def block_scores(by_seq, start_rows, block_index):
    length = by_seq.shape[1]
    per_seq = length // QBLOCK
    seq_index = block_index // per_seq
    first_row = block_index % per_seq * QBLOCK
    sequence = lax.dynamic_index_in_dim(by_seq, seq_index, 0, keepdims=False)
    key_ids = piece_ids(lax.dynamic_index_in_dim(start_rows, seq_index, 0, keepdims=False), length)
    query_rows = lax.dynamic_slice_in_dim(sequence, first_row, QBLOCK, 0)[:, :, 0]
    key_rows = sequence[:, :, 1]
    value_rows = sequence[:, :, 2]
    row_ids = lax.dynamic_slice_in_dim(key_ids, first_row, QBLOCK, 0)
    row_places = first_row + jnp.arange(QBLOCK, dtype=jnp.int32)
    scores = (
        jnp.einsum("qhd,khd->hqk", query_rows, key_rows, preferred_element_type=jnp.float32) * 0.125
    )
    places = jnp.arange(length, dtype=jnp.int32)
    scores = jnp.where(allowed_block(row_ids, row_places, key_ids, places)[None], scores, -1e30)
    return (seq_index, first_row, query_rows, key_rows, value_rows, scores)


def attention_forward(by_seq, start_rows):
    total_blocks = by_seq.shape[0] * (by_seq.shape[1] // QBLOCK)

    def attend(block_index):
        _, _, query_rows, key_rows, value_rows, scores = block_scores(
            by_seq, start_rows, block_index
        )
        peak = jnp.max(scores, axis=-1, keepdims=True)
        log_total = peak + jnp.log(jnp.sum(jnp.exp(scores - peak), axis=-1, keepdims=True))
        probs = jnp.exp(scores - log_total)
        heads = jnp.einsum(
            "hqk,khd->qhd",
            probs.astype(jnp.bfloat16),
            value_rows,
            preferred_element_type=jnp.float32,
        )
        return (heads.astype(jnp.bfloat16), log_total)

    return lax.map(attend, jnp.arange(total_blocks, dtype=jnp.int32))


def attention_backward(by_seq, start_rows, log_totals, grad_heads):
    total_blocks = by_seq.shape[0] * (by_seq.shape[1] // QBLOCK)
    empty = jnp.zeros(by_seq.shape[:3] + (HD,), jnp.float32)

    def step(carry, item):
        grad_keys, grad_values = carry
        block_index, log_total = item
        seq_index, first_row, query_rows, key_rows, value_rows, scores = block_scores(
            by_seq, start_rows, block_index
        )
        grad_seq = lax.dynamic_index_in_dim(grad_heads, seq_index, 0, keepdims=False)
        grad_rows = lax.dynamic_slice_in_dim(grad_seq, first_row, QBLOCK, 0)
        probs = jnp.exp(scores - log_total)
        grad_probs = jnp.einsum(
            "qhd,khd->hqk", grad_rows, value_rows, preferred_element_type=jnp.float32
        )
        inner = jnp.sum(probs * grad_probs, axis=-1, keepdims=True)
        grad_scores = (probs * (grad_probs - inner)).astype(jnp.bfloat16)
        grad_query = (
            jnp.einsum("hqk,khd->qhd", grad_scores, key_rows, preferred_element_type=jnp.float32)
            * 0.125
        )
        key_term = (
            jnp.einsum("hqk,qhd->khd", grad_scores, query_rows, preferred_element_type=jnp.float32)
            * 0.125
        )
        value_term = jnp.einsum(
            "hqk,qhd->khd",
            probs.astype(jnp.bfloat16),
            grad_rows,
            preferred_element_type=jnp.float32,
        )
        grad_keys = lax.dynamic_update_index_in_dim(
            grad_keys,
            lax.dynamic_index_in_dim(grad_keys, seq_index, 0, keepdims=False) + key_term,
            seq_index,
            0,
        )
        grad_values = lax.dynamic_update_index_in_dim(
            grad_values,
            lax.dynamic_index_in_dim(grad_values, seq_index, 0, keepdims=False) + value_term,
            seq_index,
            0,
        )
        return ((grad_keys, grad_values), grad_query)

    (grad_keys, grad_values), grad_query = lax.scan(
        step, (empty, empty), (jnp.arange(total_blocks, dtype=jnp.int32), log_totals)
    )
    return (grad_query, grad_keys, grad_values)


def per_device(
    tokens_in,
    starts,
    ln1_gain,
    ln1_bias,
    w_qkv,
    b_qv,
    w_out,
    b_out,
    ln2_gain,
    ln2_bias,
    w_up,
    b_up,
    w_down,
    b_down,
    grad_out,
):
    rows = tokens_in.shape[0]
    gain_one, shift_one, bias_out, gain_two, shift_two, bias_down = (
        lax.all_gather(ln1_gain, ("dp", "tensor"), axis=0, tiled=True),
        lax.all_gather(ln1_bias, ("dp", "tensor"), axis=0, tiled=True),
        lax.all_gather(b_out, ("dp", "tensor"), axis=0, tiled=True),
        lax.all_gather(ln2_gain, ("dp", "tensor"), axis=0, tiled=True),
        lax.all_gather(ln2_bias, ("dp", "tensor"), axis=0, tiled=True),
        lax.all_gather(b_down, ("dp", "tensor"), axis=0, tiled=True),
    )
    weight_qkv, bias_qv, weight_out = (
        lax.all_gather(w_qkv, "dp", axis=0, tiled=True),
        lax.all_gather(b_qv, "dp", axis=1, tiled=True),
        lax.all_gather(w_out, "dp", axis=1, tiled=True),
    )
    weight_up, bias_up, weight_down = (
        lax.all_gather(w_up, "dp", axis=0, tiled=True),
        lax.all_gather(b_up, "dp", axis=1, tiled=True),
        lax.all_gather(w_down, "dp", axis=1, tiled=True),
    )
    local_heads = weight_qkv.shape[1] // (3 * HD)
    seq_count = starts.shape[0]
    inputs = tokens_in.astype(jnp.float32)
    normed_one, inverse_one = normalize(inputs)
    gathered_one = gather_rows((normed_one * gain_one + shift_one).astype(jnp.bfloat16))
    group = gathered_one.shape[0]
    length = group // seq_count
    bias_pair = bias_qv.astype(jnp.float32).reshape(local_heads, 2, HD)
    full_bias = jnp.stack(
        [bias_pair[:, 0], jnp.zeros_like(bias_pair[:, 0]), bias_pair[:, 1]], axis=1
    )
    projected = (
        jnp.dot(gathered_one, weight_qkv, preferred_element_type=jnp.float32).reshape(
            group, local_heads, 3, HD
        )
        + full_bias
    ).astype(jnp.bfloat16)
    by_seq = projected.reshape(seq_count, length, local_heads, 3, HD)
    heads_blocks, log_totals = attention_forward(by_seq, starts)
    heads_out = heads_blocks.reshape(group, local_heads * HD)
    middle = inputs + (reduce_rows(heads_out, weight_out, rows) + bias_out)
    normed_two, inverse_two = normalize(middle)
    rounded_two = (normed_two * gain_two + shift_two).astype(jnp.bfloat16)
    grad_final = grad_out.astype(jnp.float32)
    grad_bias_down = jnp.sum(grad_final, axis=0)
    gathered_two = gather_rows(rounded_two)
    up_proj = jnp.dot(gathered_two, weight_up, preferred_element_type=jnp.float32) + bias_up.astype(
        jnp.float32
    ).reshape(-1)
    hidden_act, gelu_pull = jax.vjp(gelu_tanh, up_proj)
    hidden_low = hidden_act.astype(jnp.bfloat16)
    output = (middle + reduce_rows(hidden_low, weight_down, rows) + bias_down).astype(jnp.bfloat16)
    grad_branch = gather_grads(grad_out)
    grad_w_down = dot_first(hidden_low, grad_branch)
    grad_up = gelu_pull(dot_last(grad_branch, weight_down))[0].astype(jnp.bfloat16)
    grad_b_up = jnp.sum(grad_up, axis=0, dtype=jnp.float32).reshape(bias_up.shape)
    grad_w_up = dot_first(gathered_two, grad_up)
    grad_two = reduce_grads(grad_up, weight_up, rows)
    grad_w_up, grad_b_up, grad_w_down = (
        lax.psum_scatter(
            grad_w_up.astype(jnp.bfloat16), "dp", scatter_dimension=0, tiled=True
        ).astype(jnp.float32),
        lax.psum_scatter(
            grad_b_up.astype(jnp.bfloat16), "dp", scatter_dimension=1, tiled=True
        ).astype(jnp.float32),
        lax.psum_scatter(
            grad_w_down.astype(jnp.bfloat16), "dp", scatter_dimension=1, tiled=True
        ).astype(jnp.float32),
    )
    grad_gain_two = jnp.sum(grad_two * normed_two, axis=0)
    grad_shift_two = jnp.sum(grad_two, axis=0)
    grad_middle = grad_final + norm_back(grad_two, normed_two, inverse_two, gain_two)
    grad_bias_out = jnp.sum(grad_middle, axis=0)
    grad_attn = gather_grads(grad_middle.astype(jnp.bfloat16))
    grad_w_out = dot_first(heads_out, grad_attn)
    grad_heads = (
        dot_last(grad_attn, weight_out)
        .astype(jnp.bfloat16)
        .reshape(seq_count, length, local_heads, HD)
    )
    grad_query, grad_keys, grad_values = attention_backward(by_seq, starts, log_totals, grad_heads)
    grad_proj = jnp.stack(
        [
            grad_query.reshape(group, local_heads, HD),
            grad_keys.reshape(group, local_heads, HD),
            grad_values.reshape(group, local_heads, HD),
        ],
        axis=2,
    ).astype(jnp.bfloat16)
    grad_b_qv = jnp.sum(grad_proj[:, :, 0::2], axis=0, dtype=jnp.float32).reshape(bias_qv.shape)
    grad_flat = grad_proj.reshape(group, 3 * local_heads * HD)
    grad_w_qkv = dot_first(gathered_one, grad_flat)
    grad_one = reduce_grads(grad_flat, weight_qkv, rows)
    grad_w_qkv, grad_b_qv, grad_w_out = (
        lax.psum_scatter(
            grad_w_qkv.astype(jnp.bfloat16), "dp", scatter_dimension=0, tiled=True
        ).astype(jnp.float32),
        lax.psum_scatter(
            grad_b_qv.astype(jnp.bfloat16), "dp", scatter_dimension=1, tiled=True
        ).astype(jnp.float32),
        lax.psum_scatter(
            grad_w_out.astype(jnp.bfloat16), "dp", scatter_dimension=1, tiled=True
        ).astype(jnp.float32),
    )
    grad_gain_one = jnp.sum(grad_one * normed_one, axis=0)
    grad_shift_one = jnp.sum(grad_one, axis=0)
    grad_tokens = (grad_middle + norm_back(grad_one, normed_one, inverse_one, gain_one)).astype(
        jnp.bfloat16
    )
    summed = (
        lax.psum_scatter(grad_gain_one, ("dp", "tensor"), scatter_dimension=0, tiled=True),
        lax.psum_scatter(grad_shift_one, ("dp", "tensor"), scatter_dimension=0, tiled=True),
        lax.psum_scatter(grad_bias_out, ("dp", "tensor"), scatter_dimension=0, tiled=True),
        lax.psum_scatter(grad_gain_two, ("dp", "tensor"), scatter_dimension=0, tiled=True),
        lax.psum_scatter(grad_shift_two, ("dp", "tensor"), scatter_dimension=0, tiled=True),
        lax.psum_scatter(grad_bias_down, ("dp", "tensor"), scatter_dimension=0, tiled=True),
    )
    return (
        output,
        grad_tokens,
        summed[0],
        summed[1],
        grad_w_qkv,
        grad_b_qv,
        grad_w_out,
        summed[2],
        summed[3],
        summed[4],
        grad_w_up,
        grad_b_up,
        grad_w_down,
        summed[5],
    )


MESH = pl.DeviceIdType.MESH
CH = 2
HOPS = 4
RELAYED = "ud"


class Fused:
    def __init__(self, names, refs):
        for name, ref in zip(names, refs):
            setattr(self, name, ref)
        self.next_sem = 0
        self.unsent = []
        self.groups = {0: [], 1: []}
        self.unsent_later = []
        dp, self.z = lax.axis_index("dp"), lax.axis_index("tensor")
        self.y, self.x, self.c = dp // 4, (dp // 2) % 2, dp % 2
        self.j = self.member(self.x, self.c)
        self.q = self.quarter(self.j)
        self.sib = self.dev(self.y, self.x, 1 - self.c, self.z)
        self.across = self.dev(self.y, 1 - self.x, self.c, self.z)
        self.q_sib = self.quarter(self.member(self.x, 1 - self.c))
        self.q_x = self.quarter(self.member(1 - self.x, self.c))
        self.q_d = self.quarter(self.member(1 - self.x, 1 - self.c))
        self.rows = self.tok.shape[0]
        self.width = self.tok.shape[1]
        self.part = self.width // 8

    def dev(self, y, x, c, z):
        return ((y * 2 + x) * 2 + c, z)

    def member(self, x, c):
        return 2 * c + x

    def local(self, member):
        return 2 * (member % 2) + member // 2

    def mate(self, member):
        return self.dev(self.y, member % 2, member // 2, self.z)

    def quarter(self, member):
        return (member - self.z + 4) % 4

    def sem(self, count=1):
        index = self.next_sem
        self.next_sem += count
        return index

    def copy(self, src, dst, device, index, sent=None):
        return pltpu.make_async_remote_copy(
            src_ref=src,
            dst_ref=dst,
            send_sem=self.ssem.at[index if sent is None else sent],
            recv_sem=self.rsem.at[index],
            device_id=device,
            device_id_type=MESH,
        )

    def send(self, src, dst, device, index, group=None):
        copy = self.copy(src, dst, device, index)
        copy.start()
        (self.unsent if group is None else self.groups[group]).append(copy)

    def later(self, view, sent, when=None):
        self.unsent_later.append((view, sent, when))

    def arrived(self, dst, index):
        self.copy(dst, dst, self.sib, index).wait_recv()

    def drain(self):
        for copy in self.unsent + self.groups[0] + self.groups[1]:
            copy.wait_send()
        for view, sent, when in self.unsent_later:
            copy = self.copy(view(), view(), self.sib, sent)
            if when is None:
                copy.wait_send()
            else:
                pl.when(when())(copy.wait_send)

    def at_quarter(self, quarter, chunk=None):
        if chunk is None:
            return pl.ds(pl.multiple_of(quarter * self.rows, self.rows), self.rows)
        size = self.rows // CH
        return pl.ds(pl.multiple_of(quarter * self.rows + chunk * size, size), size)

    def at_chunk(self, chunk):
        size = self.rows // CH
        return pl.ds(chunk * size, size)

    def barrier(self):
        me = lax.axis_index("dp") * 4 + self.z
        bar = pltpu.get_barrier_semaphore()

        def greet(step, carry):
            other = (me + step) % 32
            pl.semaphore_signal(
                bar, inc=1, device_id=(other // 4, other % 4), device_id_type=MESH
            )
            return carry

        lax.fori_loop(1, 32, greet, 0)
        pl.semaphore_wait(bar, 31)

    def homes(self):
        plane = 2 * self.y + self.x
        member = (plane + self.z) % 4
        worker = (self.c, member % 2, member // 2, plane)
        owner = (self.z // 2, self.z % 2, self.y, self.q)
        same = (
            (worker[0] == self.y)
            & (worker[1] == self.x)
            & (worker[2] == self.c)
            & (worker[3] == self.z)
        )
        return self.dev(*worker), self.dev(*owner), same

    def move_start(self, src, dst, outward, index):
        worker, owner, same = self.homes()
        copy = self.copy(src, dst, worker if outward else owner, index)
        local = pltpu.make_async_copy(src, dst, self.lsem.at[index])

        @pl.when(jnp.logical_not(same))
        def _():
            copy.start()

        @pl.when(same)
        def _():
            local.start()

    def move_wait(self, src, dst, index):
        same = self.homes()[2]
        copy = self.copy(src, dst, self.sib, index)
        local = pltpu.make_async_copy(src, dst, self.lsem.at[index])

        @pl.when(jnp.logical_not(same))
        def _():
            copy.wait_send()
            copy.wait_recv()

        @pl.when(same)
        def _():
            local.wait()

    def hop_rows(self, chunk):
        size = self.rows // HOPS
        return pl.ds(chunk * size, size)

    def hop_one(self, src, mid, index):
        plane = 2 * self.y + self.x
        member = (plane + self.z) % 4
        first = self.dev(self.c, member % 2, member // 2, self.z)
        same = (self.c == self.y) & (member % 2 == self.x) & (member // 2 == self.c)
        for chunk in range(HOPS):
            view, there = src.at[self.hop_rows(chunk)], mid.at[self.hop_rows(chunk)]
            copy = self.copy(view, there, first, index + chunk)
            local = pltpu.make_async_copy(view, there, self.lsem.at[index + chunk])
            pl.when(jnp.logical_not(same))(copy.start)
            pl.when(same)(local.start)

    def hop_two(self, src, mid, dst, place, index, onward):
        plane = (self.j - self.z + 4) % 4
        member = (2 * self.y + self.x + self.z) % 4
        home = (self.c == self.y) & (member % 2 == self.x) & (member // 2 == self.c)
        stay = plane == self.z
        for chunk in range(HOPS):
            rows = self.hop_rows(chunk)
            size = self.rows // HOPS
            there = dst.at[pl.ds(pl.multiple_of(place + chunk * size, size), size)]
            first = self.copy(src.at[rows], mid.at[rows], self.sib, index + chunk)
            local = pltpu.make_async_copy(src.at[rows], mid.at[rows], self.lsem.at[index + chunk])
            pl.when(jnp.logical_not(home))(first.wait_send)
            pl.when(jnp.logical_not(home))(first.wait_recv)
            pl.when(home)(local.wait)
            copy = self.copy(
                mid.at[rows], there, self.dev(self.y, self.x, self.c, plane), onward + chunk
            )
            keep = pltpu.make_async_copy(mid.at[rows], there, self.lsem.at[onward + chunk])
            pl.when(jnp.logical_not(stay))(copy.start)
            pl.when(stay)(keep.start)

    def hop_wait(self, mid, dst, place, onward, half):
        plane = (self.j - self.z + 4) % 4
        stay = plane == self.z
        for chunk in range(half * HOPS // CH, (half + 1) * HOPS // CH):
            rows = self.hop_rows(chunk)
            size = self.rows // HOPS
            there = dst.at[pl.ds(pl.multiple_of(place + chunk * size, size), size)]
            copy = self.copy(mid.at[rows], there, self.sib, onward + chunk)
            keep = pltpu.make_async_copy(mid.at[rows], there, self.lsem.at[onward + chunk])
            pl.when(jnp.logical_not(stay))(copy.wait_send)
            pl.when(jnp.logical_not(stay))(copy.wait_recv)
            pl.when(stay)(keep.wait)

    def span(self, half):
        return pl.ds(pl.multiple_of(half * 4 * self.part, 4 * self.part), 4 * self.part)

    def place(self, source):
        return pl.ds(pl.multiple_of(source * self.part, self.part), self.part)

    def cut(self, kind, ref, zc, where):
        if kind == "u":
            return ref.at[zc, where, :]
        return ref.at[zc, :, where]

    def piece(self, kind, ref, member):
        if kind == "u":
            wide = self.wbuf["u"].shape[2]
            return ref.at[:, pl.ds(pl.multiple_of(member * wide, wide), wide)]
        return ref.at[member]

    def weights_one(self, kind):
        source = 4 * self.y + self.local(self.j)
        here = self.cut(kind, self.wbuf[kind], self.z, self.place(source))
        self.one[kind] = []
        for step in range(1, 4):
            member = (self.j + step) % 4
            index = self.sem()
            self.send(
                self.piece(kind, self.shard[kind], member), here, self.mate(member), index
            )
            sender = 4 * self.y + self.local((self.j - step + 4) % 4)
            self.one[kind].append(
                (self.cut(kind, self.wbuf[kind], self.z, self.place(sender)), index)
            )
        index = self.sem()
        local = pltpu.make_async_copy(
            self.piece(kind, self.shard[kind], self.j), here, self.lsem.at[index]
        )
        local.start()
        self.own[kind] = local
        self.two[kind] = self.sem(4)
        self.three[kind] = self.sem(4)
        self.pass_sem[kind] = self.sem()

    def weights_in(self, kind):
        self.own[kind].wait()
        for view, index in self.one[kind]:
            self.arrived(view, index)
        self.weights_cross(kind, 0)

    def mine(self, kind, plane):
        return self.cut(kind, self.wbuf[kind], plane, self.span(self.y))

    def weights_two(self, kind):
        here = self.mine(kind, self.z)
        near, far = (lambda: self.z != 3), (lambda: self.z != 0)
        if kind not in RELAYED:
            near = far = None
        for step, when in ((2, None), (1, near), (3, far)):
            plane = (self.z + step) % 4
            index = self.two[kind] + step
            copy = self.copy(here, here, self.dev(self.y, self.x, self.c, plane), index)
            if when is None:
                copy.start()
            else:
                pl.when(when())(copy.start)
            self.later(lambda: self.mine(kind, self.z), index, when)

    def weights_relay(self, kind, guard=None):
        if kind not in RELAYED:
            return
        for here, plane, step in ((2, 3, 3), (1, 0, 1)):
            when = self.z == here
            block = self.mine(kind, (here + 2) % 4)
            copy = self.copy(
                block,
                block,
                self.dev(self.y, self.x, self.c, plane),
                self.two[kind] + step,
                self.pass_sem[kind],
            )
            pl.when(when if guard is None else when & guard)(copy.start)

    def relayed(self, kind):
        if kind in RELAYED:
            self.later(
                lambda: self.mine(kind, self.z),
                self.pass_sem[kind],
                lambda: (self.z == 1) | (self.z == 2),
            )
        for step in range(4):
            self.later(lambda: self.mine(kind, self.z), self.three[kind] + step)

    def weights_cross(self, kind, step):
        mine = self.mine(kind, (self.z - step + 4) % 4)
        self.copy(
            mine,
            mine,
            self.dev(1 - self.y, self.x, self.c, self.z),
            self.three[kind] + step,
        ).start()

    def weights_here(self, kind, step):
        self.arrived(self.mine(kind, (self.z - step + 4) % 4), self.two[kind] + step)

    def weights_three(self, kind, steps=(1, 3)):
        for step in steps:
            self.weights_here(kind, step)
            self.weights_cross(kind, step)

    def weights_start_three(self, kind):
        self.weights_here(kind, 2)
        self.weights_relay(kind)
        self.weights_cross(kind, 2)

    def weights_ready(self, kind, step):
        plane = (self.z - step + 4) % 4
        self.arrived(
            self.cut(kind, self.wbuf[kind], plane, self.span(1 - self.y)),
            self.three[kind] + step,
        )

    def weights_done(self, kind):
        for step in range(4):
            self.weights_ready(kind, step)

    def grads_one(self, kind):
        self.swaps[kind] = [self.sem() for _ in range(3)]
        for swap in self.swaps[kind]:
            self.later(lambda: self.zbuf[kind].at[0], swap)
        for turn in (2, 1, 3, 0):
            plane = (self.z + turn) % 4
            away = self.cut(kind, self.dbuf[kind], plane, self.span(1 - self.y))
            there = self.cut(kind, self.ybuf[kind], plane, slice(None))
            use = self.sem()
            self.send(away, there, self.dev(1 - self.y, self.x, self.c, self.z), use)
            self.backs.setdefault(kind, {})[turn] = use

    def grads_two(self, kind, turns=(2, 1, 3, 0)):
        for turn in turns:
            plane = (self.z + turn) % 4
            there = self.cut(kind, self.ybuf[kind], plane, slice(None))
            self.arrived(there, self.backs[kind][turn])
            mine = self.cut(kind, self.dbuf[kind], plane, self.span(self.y))
            mine[...] = (
                mine[...].astype(jnp.float32) + there[...].astype(jnp.float32)
            ).astype(jnp.bfloat16)
            if turn:
                self.copy(
                    mine,
                    self.zbuf[kind].at[turn - 1],
                    self.dev(self.y, self.x, self.c, plane),
                    self.swaps[kind][turn - 1],
                ).start()

    def head_one(self, step, head):
        self.copy(
            self.cut("q", self.dq, head, self.span(1 - self.y)),
            self.cut("q", self.yq, head, slice(None)),
            self.dev(1 - self.y, self.x, self.c, self.z),
            self.head_y + step,
        ).start()

    def head_add(self, step, head):
        there = self.cut("q", self.yq, head, slice(None))
        self.arrived(there, self.head_y + step)
        mine = self.cut("q", self.dq, head, self.span(self.y))
        mine[...] = (mine[...].astype(jnp.float32) + there[...].astype(jnp.float32)).astype(
            jnp.bfloat16
        )

    def head_two(self, step, head):
        self.copy(
            self.cut("q", self.dq, head, self.span(self.y)),
            self.zq.at[step],
            self.dev(self.y, self.x, self.c, head),
            self.head_z + step,
        ).start()

    def grads_three(self, kind):
        mine = self.cut(kind, self.dbuf[kind], self.z, self.span(self.y))
        total = mine[...].astype(jnp.float32)
        for step in range(1, 4):
            there = self.zbuf[kind].at[step - 1]
            self.arrived(there, self.swaps[kind][step - 1])
            total = total + there[...].astype(jnp.float32)
        final = self.fbuf[kind]
        final[...] = total.astype(jnp.bfloat16)
        ends = self.ebuf[kind]
        self.last[kind] = []
        for step in range(1, 4):
            member = (self.j + step) % 4
            index = self.sem()
            self.send(
                self.slab(kind, final, self.local(member)),
                ends.at[self.j],
                self.mate(member),
                index,
            )
            self.last[kind].append(((self.j - step + 4) % 4, index))
        index = self.sem()
        local = pltpu.make_async_copy(
            self.slab(kind, final, self.local(self.j)), ends.at[self.j], self.lsem.at[index]
        )
        local.start()
        self.own[kind] = local

    def slab(self, kind, ref, member):
        where = pl.ds(pl.multiple_of(member * self.part, self.part), self.part)
        if kind == "u":
            return ref.at[where, :]
        return ref.at[:, where]

    def grads_done(self, kind):
        self.own[kind].wait()
        for member, index in self.last[kind]:
            self.arrived(self.ebuf[kind].at[member], index)

    def small_one(self):
        self.sma[self.z] = self.si[...]
        self.small_sem = [self.sem() for _ in range(3)]
        for step in range(1, 4):
            plane = (self.z + step) % 4
            self.send(
                self.si,
                self.sma.at[self.z],
                self.dev(self.y, self.x, self.c, plane),
                self.small_sem[step - 1],
            )

    def around(self, step):
        return (lax.axis_index("dp") + step + 8) % 8

    def small_two(self):
        for step in range(1, 4):
            self.arrived(self.sma.at[(self.z - step + 4) % 4], self.small_sem[step - 1])
        me = self.around(0)
        self.lb[me] = sum(self.sma[plane, 0] for plane in range(4))
        self.bb[me] = self.sma[:, 1 + self.j]
        self.plane_sem = [(self.sem(), self.sem()) for _ in range(7)]
        for step in range(1, 8):
            other = self.around(step)
            member = self.member((other // 2) % 2, other % 2)
            first, second = self.plane_sem[step - 1]
            self.send(self.lb.at[me], self.lb.at[me], (other, self.z), first)
            self.send(self.sma.at[:, 1 + member], self.bb.at[me], (other, self.z), second)

    def small_three(self):
        for step in range(1, 8):
            other = self.around(-step)
            first, second = self.plane_sem[step - 1]
            self.arrived(self.lb.at[other], first)
            self.arrived(self.bb.at[other], second)
        part, dim = self.part, self.qh.shape[2]
        for source in range(8):
            self.small[:, source * part : (source + 1) * part] = self.lb[source]
        bias = sum(self.bb[source] for source in range(8))
        for head in range(4):
            row = bias[head, 0:1]
            self.bq[head, :, 0:dim] = row[:, 0:dim]
            self.bq[head, :, dim : 2 * dim] = jnp.zeros((1, dim), jnp.float32)
            self.bq[head, :, 2 * dim :] = row[:, dim:]
            for half in range(2):
                place = (2 * head + half) * part
                self.bu[:, place : place + part] = bias[head, 1 + half : 2 + half]

    def back_one(self):
        part, me = self.part, self.around(0)
        for target in range(8):
            self.cs[target] = self.sums[:, target * part : (target + 1) * part]
        self.cr[me] = self.cs[me]
        self.cd[me] = self.cb[...]
        self.back_sem = [(self.sem(), self.sem()) for _ in range(7)]
        for step in range(1, 8):
            other = self.around(step)
            first, second = self.back_sem[step - 1]
            self.send(self.cs.at[other], self.cr.at[me], (other, self.z), first)
            self.send(self.cb, self.cd.at[me], (other, self.z), second)

    def back_two(self):
        for step in range(1, 8):
            other = self.around(-step)
            first, second = self.back_sem[step - 1]
            self.arrived(self.cr.at[other], first)
            self.arrived(self.cd.at[other], second)
        self.es[self.z] = sum(self.cr[source] for source in range(8))
        for member in range(4):
            pair = [2 * (member % 2) + member // 2, 4 + 2 * (member % 2) + member // 2]
            self.ed_small[:, member] = self.cd[pair[0]] + self.cd[pair[1]]
        self.eb[self.z] = self.ed_small[self.z]
        self.line_sem = [(self.sem(), self.sem()) for _ in range(3)]
        for step in range(1, 4):
            plane = (self.z + step) % 4
            device = self.dev(self.y, self.x, self.c, plane)
            first, second = self.line_sem[step - 1]
            self.send(self.es.at[self.z], self.es.at[self.z], device, first)
            self.send(self.ed_small.at[plane], self.eb.at[self.z], device, second)

    def back_three(self):
        for step in range(1, 4):
            plane = (self.z - step + 4) % 4
            first, second = self.line_sem[step - 1]
            self.arrived(self.es.at[plane], first)
            self.arrived(self.eb.at[plane], second)
        self.fs[...] = sum(self.es[plane] for plane in range(4))
        self.fb[...] = sum(self.eb[plane] for plane in range(4))

    def gather_plan(self):
        return {kind: [self.sem() for _ in range(CH)] for kind in ("across", "sib", "pass")}

    def gather_send(self, buf, plan, chunk):
        rows = self.at_quarter(self.q, chunk)
        self.send(buf.at[rows], buf.at[rows], self.across, plan["across"][chunk])
        self.send(buf.at[rows], buf.at[rows], self.sib, plan["sib"][chunk])

    def gather_pass(self, buf, plan):
        for chunk in range(CH):
            rows = self.at_quarter(self.q_x, chunk)
            self.arrived(buf.at[rows], plan["across"][chunk])
            self.send(buf.at[rows], buf.at[rows], self.sib, plan["pass"][chunk])

    def gather_sib(self, buf, plan):
        for chunk in range(CH):
            self.arrived(buf.at[self.at_quarter(self.q_sib, chunk)], plan["sib"][chunk])

    def gather_last(self, buf, plan):
        for chunk in range(CH):
            self.arrived(buf.at[self.at_quarter(self.q_d, chunk)], plan["pass"][chunk])

    def gathered(self, buf, plan, use):
        use(self.q)
        self.gather_sib(buf, plan)
        use(self.q_sib)
        self.gather_pass(buf, plan)
        use(self.q_x)
        self.gather_last(buf, plan)
        use(self.q_d)

    def scatter_start(self, partial, own, which, rx, hold=False):
        sa, ra, sb, sc, rb = (self.rs.at[which, slot] for slot in range(5))
        plan = [[self.sem() for _ in range(CH)] for _ in range(3)]
        low = jnp.bfloat16
        for copy in self.groups[which]:
            copy.wait_send()
        self.groups[which] = []
        sa[...] = partial(self.q_d).astype(low)
        for chunk in range(CH):
            rows = self.at_chunk(chunk)
            self.send(sa.at[rows], ra.at[rows], self.sib, plan[0][chunk], which)
        held = partial(self.q_x)
        for chunk in range(CH):
            self.arrived(ra.at[self.at_chunk(chunk)], plan[0][chunk])
        sb[...] = (held + ra[...].astype(jnp.float32)).astype(low)
        if not hold:
            self.scatter_send((plan, which, rx))
        sc[...] = partial(self.q_sib).astype(low)
        for chunk in range(CH):
            rows = self.at_chunk(chunk)
            self.send(sc.at[rows], rb.at[rows], self.sib, plan[2][chunk], which)
        own[...] = partial(self.q)
        return plan, which, rx

    def scatter_send(self, started):
        plan, which, rx = started
        sb = self.rs.at[which, 2]
        for chunk in range(CH):
            rows = self.at_chunk(chunk)
            self.send(sb.at[rows], rx.at[rows], self.across, plan[1][chunk], which)

    def scatter_chunk(self, started, own, chunk):
        plan, which, rx = started
        rows = self.at_chunk(chunk)
        rb = self.rs.at[which, 4]
        self.arrived(rb.at[rows], plan[2][chunk])
        self.arrived(rx.at[rows], plan[1][chunk])
        return (
            own[rows, :] + rb[rows, :].astype(jnp.float32) + rx[rows, :].astype(jnp.float32)
        )

    def run(self):
        f32, low = jnp.float32, jnp.bfloat16
        rows, width = self.rows, self.width
        quarters = range(4)
        self.wbuf = dict(q=self.wq, o=self.wo, u=self.wu, d=self.wd)
        self.shard = dict(q=self.in_q, o=self.in_o, u=self.in_u, d=self.in_d)
        self.dbuf = dict(q=self.dq, o=self.do, u=self.du, d=self.dd)
        self.ybuf = dict(q=self.yq, o=self.yo, u=self.yu, d=self.yd)
        self.zbuf = dict(q=self.zq, o=self.zo, u=self.zu, d=self.zd)
        self.fbuf = dict(q=self.fq, o=self.fo, u=self.fu, d=self.fd)
        self.ebuf = dict(q=self.eq, o=self.eo, u=self.eu, d=self.ed)
        self.one, self.two, self.three, self.own = {}, {}, {}, {}
        self.back, self.backs, self.swaps, self.last = {}, {}, {}, {}
        self.pass_sem = {}
        heads, dim = self.qh.shape[0], self.qh.shape[2]
        hidden = self.wu.shape[2]

        self.barrier()
        move = [self.sem() for _ in range(4)]
        self.small_one()
        hop = [self.sem(HOPS) for _ in range(4)]
        self.hop_one(self.tok, self.mid_x, hop[0])
        self.weights_one("q")
        plan_one, plan_two, plan_go, plan_mid = (self.gather_plan() for _ in range(4))
        self.hop_two(self.tok, self.mid_x, self.xs, 0, hop[0], hop[1])
        self.small_two()
        own_rows = self.at_quarter(self.q)
        self.weights_in("q")
        self.weights_two("q")
        for kind in "ou":
            self.weights_one(kind)
        self.small_three()
        gain_one, shift_one = self.small[0:1, :], self.small[1:2, :]
        bias_out = self.small[2:3, :]
        gain_two, shift_two = self.small[3:4, :], self.small[4:5, :]
        bias_down = self.small[5:6, :]

        for chunk in range(CH):
            part = self.at_chunk(chunk)
            self.hop_wait(self.mid_x, self.xs, 0, hop[1], chunk)
            normed, inverse = normalize(self.xs[part, :].astype(f32))
            self.n1[part, :] = normed
            self.i1[part, :] = inverse
            self.h1[self.at_quarter(self.q, chunk), :] = (normed * gain_one + shift_one).astype(low)
            self.gather_send(self.h1, plan_one, chunk)
        self.mask_blocks()
        near = 1 + 2 * ((3 - self.z) // 3)
        self.gather_sib(self.h1, plan_one)
        self.weights_start_three("q")
        self.gather_pass(self.h1, plan_one)
        self.weights_one("d")
        self.weights_three("q", (near,))
        self.weights_in("o")
        self.weights_two("o")
        self.gather_last(self.h1, plan_one)

        def parts_of(block):
            return ([(0, block * rows)] if block else []) + [(block * rows, rows)]

        def turn(step):
            late, odd = step // 2, step % 2
            return (1 - late) * 2 * odd + late * (near + odd * (4 - 2 * near))

        def attend(step, carry):
            back = turn(step)
            head = (self.z - back + 4) % 4
            self.weights_ready("q", back)

            def project(block, carry):
                place = pl.ds(pl.multiple_of(block * rows, rows), rows)
                both = dot_last(self.h1[place, :], self.wq[head]) + self.bq[head]
                for slot, ref in enumerate((self.qh, self.kh, self.vh)):
                    value = both[:, slot * dim : (slot + 1) * dim].astype(low)
                    if slot == 0:
                        value = (value.astype(f32) * 0.125).astype(low)
                    ref[head, place, :] = value
                return carry

            lax.fori_loop(0, 4, project, 0)

            @pl.when(step == 0)
            def _():
                self.weights_three("q", (4 - near,))
                self.weights_in("u")

            @pl.when(step == 1)
            def _():
                self.weights_start_three("o")
                self.weights_two("u")
                self.hop_one(self.go, self.ox, hop[2])

            @pl.when(step == 2)
            def _():
                self.weights_three("o")

            @pl.when(step == 3)
            def _():
                self.weights_start_three("u")

            for block in quarters:
                place = pl.ds(block * rows, rows)
                query = self.qh[head, place, :]
                scores = []
                for first, count in parts_of(block):
                    value = dot_last(query, self.kh[head, pl.ds(first, count), :])
                    if first == block * rows:
                        value = value + self.mk[block].astype(f32)
                    scores.append(value)
                peak = functools.reduce(
                    jnp.maximum, [jnp.max(value, axis=1, keepdims=True) for value in scores]
                )
                powers = [jnp.exp(value - peak) for value in scores]
                total = sum(jnp.sum(value, axis=1, keepdims=True) for value in powers)
                scale = 1.0 / total
                result = 0.0
                for (first, count), value in zip(parts_of(block), powers):
                    probs = (value * scale).astype(low)
                    self.pb[block][head, :, pl.ds(first, count)] = probs
                    result = result + jnp.dot(
                        probs,
                        self.vh[head, pl.ds(first, count), :],
                        preferred_element_type=f32,
                    )
                self.hh[head, place, :] = result.astype(low)
            return carry

        lax.fori_loop(0, heads, attend, 0)
        for kind in "qou":
            self.relayed(kind)

        def assemble(target, refs, count):
            def one(block, carry):
                place = pl.ds(pl.multiple_of(block * rows, rows), rows)
                pieces = [ref[head, place, :] for ref in refs for head in range(count)]
                target[place, :] = jnp.concatenate(pieces, axis=1)
                return carry

            lax.fori_loop(0, 4, one, 0)

        assemble(self.ho, (self.hh,), heads)
        self.weights_done("o")

        flat_out = lambda: self.wo[...].reshape(heads * dim, width)
        started = self.scatter_start(
            lambda quarter: jnp.dot(
                self.ho[self.at_quarter(quarter), :], flat_out(), preferred_element_type=f32
            ),
            self.own_a,
            0,
            self.rx.at[0],
        )
        self.hop_two(self.go, self.ox, self.gg, self.z * rows, hop[2], hop[3])
        self.weights_in("d")
        self.weights_two("d")
        self.weights_three("u")
        for chunk in range(CH):
            part = self.at_chunk(chunk)
            summed = self.scatter_chunk(started, self.own_a, chunk)
            middle = self.xs[part, :].astype(f32) + (summed + bias_out)
            self.mid[part, :] = middle
            normed, inverse = normalize(middle)
            self.n2[part, :] = normed
            self.i2[part, :] = inverse
            self.h2[self.at_quarter(self.q, chunk), :] = (normed * gain_two + shift_two).astype(low)
            self.gather_send(self.h2, plan_two, chunk)
        for chunk in range(CH):
            self.hop_wait(self.ox, self.gg, self.q * rows, hop[3], chunk)
            self.gather_send(self.gg, plan_go, chunk)
        self.weights_start_three("d")
        self.relayed("d")
        self.weights_done("u")

        def up(quarter):
            place = self.at_quarter(quarter)

            for block in range(4):
                lanes = pl.ds(block * hidden, hidden)
                value = (
                    jnp.dot(self.h2[place, :], self.wu[block], preferred_element_type=f32)
                    + self.bu[:, lanes]
                )
                square = value * value
                bend = jnp.tanh(ROOT * (value + 0.044715 * value * square))
                self.hid[place, lanes] = (0.5 * value * (1.0 + bend)).astype(low)
                slope = 0.5 * (1.0 + bend) + 0.5 * value * (1.0 - bend * bend) * ROOT * (
                    1.0 + 3.0 * 0.044715 * square
                )
                self.gu[place, lanes] = slope.astype(low)

        up(self.q)
        self.gather_sib(self.h2, plan_two)
        up(self.q_sib)
        self.weights_three("d", (near,))
        self.gather_pass(self.h2, plan_two)
        up(self.q_x)
        self.weights_three("d", (4 - near,))
        self.gather_last(self.h2, plan_two)
        up(self.q_d)
        flat_down = lambda: self.wd[...].reshape(4 * hidden, width)
        self.gather_sib(self.gg, plan_go)
        self.gather_pass(self.gg, plan_go)
        grad_out = self.gg[own_rows, :].astype(f32)
        self.sums[5:6, :] = jnp.sum(grad_out, axis=0, keepdims=True)
        self.gather_last(self.gg, plan_go)

        def down_grad(block, carry):
            lanes = pl.ds(pl.multiple_of(block * hidden, hidden), hidden)
            self.dd[block] = dot_first(self.hid[:, lanes], self.gg[...]).astype(low)
            return carry

        lax.fori_loop(0, 4, down_grad, 0)
        self.grads_one("d")
        self.weights_done("d")

        def to_up(quarter):
            place = self.at_quarter(quarter)
            value = dot_last(self.gg[place, :], flat_down())
            self.gu[place, :] = (self.gu[place, :].astype(f32) * value).astype(low)

        for quarter in (self.q_d, self.q_x, self.q_sib, self.q):
            to_up(quarter)
        self.grads_two("d", (2,))

        def two_part(quarter):
            place = self.at_quarter(quarter)
            return sum(
                dot_last(self.gu[place, pl.ds(block * hidden, hidden)], self.wu[block])
                for block in range(4)
            )

        started = self.scatter_start(two_part, self.own_a, 0, self.rx.at[0])

        self.grads_two("d", (1,))
        step = width // 4

        def up_grad(block, carry):
            lanes = pl.ds(pl.multiple_of(block * step, step), step)
            value = dot_first(self.h2[:, lanes], self.gu[...]).astype(low)
            for plane in range(4):
                self.du[plane, lanes, :] = value[:, plane * hidden : (plane + 1) * hidden]
            return carry

        lax.fori_loop(0, 4, up_grad, 0)
        self.grads_one("u")
        started_down = self.scatter_start(
            lambda quarter: jnp.dot(
                self.hid[self.at_quarter(quarter), :], flat_down(), preferred_element_type=f32
            ),
            self.own_b,
            1,
            self.rx.at[1],
            hold=True,
        )
        self.grads_two("d", (3, 0))
        totals = [0.0] * 3
        for chunk in range(CH):
            part = self.at_chunk(chunk)
            grad_two = self.scatter_chunk(started, self.own_a, chunk)
            normed = self.n2[part, :]
            middle = self.gg[self.at_quarter(self.q, chunk), :].astype(f32) + norm_back(
                grad_two, normed, self.i2[part, :], gain_two
            )
            self.gm[part, :] = middle
            self.ga[self.at_quarter(self.q, chunk), :] = middle.astype(low)
            self.gather_send(self.ga, plan_mid, chunk)
            for place, value in enumerate((grad_two * normed, grad_two, middle)):
                totals[place] = totals[place] + jnp.sum(value, axis=0, keepdims=True)
        self.sums[3:4, :] = totals[0]
        self.sums[4:5, :] = totals[1]
        self.sums[2:3, :] = totals[2]
        self.scatter_send(started_down)
        up_sum = jnp.sum(self.gu[...].astype(f32), axis=0, keepdims=True)
        lanes = self.part
        for place in range(8):
            self.cb[place // 2, 1 + place % 2 : 2 + place % 2, :] = up_sum[
                :, place * lanes : (place + 1) * lanes
            ]
        def to_heads(quarter):
            place = self.at_quarter(quarter)
            value = dot_last(self.ga[place, :], flat_out()).astype(low)
            for head in range(heads):
                self.hh[head, place, :] = value[:, head * dim : (head + 1) * dim]

        to_heads(self.q)
        self.gather_sib(self.ga, plan_mid)
        to_heads(self.q_sib)
        self.grads_two("u", (2,))
        self.gather_pass(self.ga, plan_mid)
        to_heads(self.q_x)
        self.grads_two("u", (1,))
        self.gather_last(self.ga, plan_mid)
        to_heads(self.q_d)
        self.do[...] = dot_first(self.ho[...], self.ga[...]).astype(low).reshape(self.do.shape)
        self.grads_one("o")
        self.grads_two("u", (3, 0))

        self.head_y, self.head_z = self.sem(4), self.sem(3)

        def attend_back(step, carry):
            head = (self.z + 1 + step) % 4
            self.ka[...] = jnp.zeros_like(self.ka)
            self.va[...] = jnp.zeros_like(self.va)
            for block in quarters:
                place = pl.ds(block * rows, rows)
                query = self.qh[head, place, :]
                grads = self.hh[head, place, :]
                probs, values = [], []
                inner = 0.0
                for first, count in parts_of(block):
                    span = pl.ds(first, count)
                    prob = self.pb[block][head, :, span]
                    value = dot_last(grads, self.vh[head, span, :])
                    self.va[span, :] += dot_first(prob, grads)
                    prob = prob.astype(f32)
                    inner = inner + jnp.sum(prob * value, axis=1, keepdims=True)
                    probs.append(prob)
                    values.append(value)
                result = 0.0
                for (first, count), prob, value in zip(parts_of(block), probs, values):
                    span = pl.ds(first, count)
                    score = (prob * (value - inner)).astype(low)
                    result = result + jnp.dot(
                        score, self.kh[head, span, :], preferred_element_type=f32
                    )
                    self.ka[span, :] += dot_first(score, query)
                self.qh[head, place, :] = (result * 0.125).astype(low)
            self.gp[head, :, 0:dim] = self.qh[head]
            self.gp[head, :, dim : 2 * dim] = self.ka[...].astype(low)
            self.gp[head, :, 2 * dim :] = self.va[...].astype(low)
            self.dq[head] = dot_first(self.gp[head], self.h1[...]).astype(low)
            self.head_one(step, head)

            @pl.when(step == 2)
            def _():
                self.grads_two("o")

            @pl.when(step == 1)
            def _():
                for chunk in range(CH):
                    part = self.at_chunk(chunk)
                    summed = self.scatter_chunk(started_down, self.own_b, chunk)
                    self.ox[part, :] = (self.mid[part, :] + summed + bias_down).astype(low)
                self.move_start(self.ox, self.out, False, move[2])

            return carry

        lax.fori_loop(0, heads, attend_back, 0)
        self.swaps["q"] = [self.head_z + step for step in range(3)]
        for step in range(4):
            self.later(lambda: self.cut("q", self.dq, 0, self.span(0)), self.head_y + step)
        for step in range(3):
            self.later(lambda: self.zq.at[0], self.head_z + step)
        started = self.scatter_start(
            lambda quarter: sum(
                jnp.dot(
                    self.gp[head, self.at_quarter(quarter), :],
                    self.wq[head],
                    preferred_element_type=f32,
                )
                for head in range(heads)
            ),
            self.own_a,
            0,
            self.rx.at[0],
        )
        for step in range(3):
            head = (self.z + 1 + step) % 4
            self.head_add(step, head)
            self.head_two(step, head)
        for head in range(heads):
            total = jnp.sum(self.gp[head].astype(f32), axis=0, keepdims=True)
            self.cb[head, 0:1, 0:dim] = total[:, 0:dim]
            self.cb[head, 0:1, dim:] = total[:, 2 * dim :]
            self.cb[head, 3:, :] = jnp.zeros((5, self.part), f32)
        self.grads_three("d")
        self.head_add(3, self.z)
        totals = [0.0] * 2
        for chunk in range(CH):
            part = self.at_chunk(chunk)
            grad_one = self.scatter_chunk(started, self.own_a, chunk)
            normed = self.n1[part, :]
            self.xs[part, :] = (
                self.gm[part, :] + norm_back(grad_one, normed, self.i1[part, :], gain_one)
            ).astype(low)
            for place, value in enumerate((grad_one * normed, grad_one)):
                totals[place] = totals[place] + jnp.sum(value, axis=0, keepdims=True)
        self.sums[0:1, :] = totals[0]
        self.sums[1:2, :] = totals[1]
        self.sums[6:8, :] = jnp.zeros((2, width), f32)
        self.back_one()
        self.move_start(self.xs, self.gtok, False, move[3])
        self.grads_three("u")
        self.grads_three("o")
        self.back_two()
        self.grads_three("q")
        for kind in "duoq":
            self.grads_done(kind)
        self.move_wait(self.ox, self.out, move[2])
        self.back_three()
        self.move_wait(self.xs, self.gtok, move[3])
        self.drain()

    def mask_blocks(self):
        rows = self.rows
        begins = self.lb[2 * self.z + self.y, 6:7, 0:4].astype(jnp.int32)
        for block in range(4):
            down = block * rows + lax.broadcasted_iota(jnp.int32, (rows, 1), 0)
            side = block * rows + lax.broadcasted_iota(jnp.int32, (1, rows), 1)

            def ids(places):
                total = jnp.zeros_like(places)
                for piece in range(4):
                    first = begins[:, piece : piece + 1]
                    inside = (places >= first) & (places < first + PIECE)
                    total = jnp.where(inside, piece + 1, total)
                return total

            mine, theirs = ids(down), ids(side)
            seen = (side <= down) | ((mine == theirs) & (mine > 0))
            self.mk[block] = jnp.where(seen, 0.0, -1e30).astype(jnp.bfloat16)


IN_NAMES = ("tok", "go", "in_q", "in_o", "in_u", "in_d", "si")
OUT_NAMES = ("out", "gtok", "eq", "eo", "eu", "ed", "fs", "fb")


def fused_layer(tok, go, in_q, in_o, in_u, in_d, si):
    rows, width = tok.shape
    heads, dim = 4, width // 16
    hidden = in_u.shape[1] // 4
    part = width // 8
    n = 4 * rows
    low, f32 = jnp.bfloat16, jnp.float32
    scratch = dict(
        xs=((rows, width), low),
        mid_x=((rows, width), low),
        wq=((4, 3 * dim, width), low),
        wo=((4, dim, width), low),
        wu=((4, width, hidden), low),
        wd=((4, hidden, width), low),
        h1=((n, width), low),
        h2=((n, width), low),
        gg=((n, width), low),
        ga=((n, width), low),
        qh=((heads, n, dim), low),
        kh=((heads, n, dim), low),
        vh=((heads, n, dim), low),
        hh=((heads, n, dim), low),
        ho=((n, heads * dim), low),
        gp=((heads, n, 3 * dim), low),
        ka=((n, dim), f32),
        va=((n, dim), f32),
        mk=((4, rows, rows), low),
        n1=((rows, width), f32),
        n2=((rows, width), f32),
        mid=((rows, width), f32),
        gm=((rows, width), f32),
        i1=((rows, 1), f32),
        i2=((rows, 1), f32),
        own_a=((rows, width), f32),
        own_b=((rows, width), f32),
        hid=((n, 4 * hidden), low),
        gu=((n, 4 * hidden), low),
        ox=((rows, width), low),
        rs=((2, 5, rows, width), low),
        rx=((2, rows, width), low),
        dq=((4, 3 * dim, width), low),
        do=((4, dim, width), low),
        du=((4, width, hidden), low),
        dd=((4, hidden, width), low),
        yq=((4, 3 * dim, 4 * part), low),
        yo=((4, dim, 4 * part), low),
        yu=((4, 4 * part, hidden), low),
        yd=((4, hidden, 4 * part), low),
        zq=((3, 3 * dim, 4 * part), low),
        zo=((3, dim, 4 * part), low),
        zu=((3, 4 * part, hidden), low),
        zd=((3, hidden, 4 * part), low),
        fq=((3 * dim, 4 * part), low),
        fo=((dim, 4 * part), low),
        fu=((4 * part, hidden), low),
        fd=((hidden, 4 * part), low),
        small=((8, width), f32),
        sums=((8, width), f32),
        bq=((4, 1, 3 * dim), f32),
        bu=((1, 4 * hidden), f32),
        sma=((4, 5, 8, part), f32),
        lb=((8, 8, part), f32),
        bb=((8, 4, 8, part), f32),
        cs=((8, 8, part), f32),
        cr=((8, 8, part), f32),
        cb=((4, 8, part), f32),
        cd=((8, 4, 8, part), f32),
        es=((4, 8, part), f32),
        ed_small=((4, 4, 8, part), f32),
        eb=((4, 4, 8, part), f32),
    )
    probs = [((heads, rows, (block + 1) * rows), low) for block in range(4)]
    names = IN_NAMES + OUT_NAMES + tuple(scratch)

    def kernel(*refs):
        count = len(names)
        state = Fused(names, refs[:count])
        state.pb = refs[count : count + 4]
        state.ssem, state.rsem, state.lsem = refs[count + 4 :]
        state.run()

    hbm = pl.BlockSpec(memory_space=pl.ANY)
    vmem = pl.BlockSpec(memory_space=pltpu.VMEM)
    return pl.pallas_call(
        kernel,
        out_shape=(
            jax.ShapeDtypeStruct((rows, width), low),
            jax.ShapeDtypeStruct((rows, width), low),
            jax.ShapeDtypeStruct((4, 3 * dim, part), low),
            jax.ShapeDtypeStruct((4, dim, part), low),
            jax.ShapeDtypeStruct((4, part, hidden), low),
            jax.ShapeDtypeStruct((4, hidden, part), low),
            jax.ShapeDtypeStruct((8, part), f32),
            jax.ShapeDtypeStruct((4, 8, part), f32),
        ),
        in_specs=[hbm] * 6 + [vmem],
        out_specs=(hbm,) * 6 + (vmem,) * 2,
        scratch_shapes=[pltpu.VMEM(*spec) for spec in scratch.values()]
        + [pltpu.VMEM(*spec) for spec in probs]
        + [pltpu.SemaphoreType.DMA((SEMS,))] * 3,
        name="fused_layer",
        compiler_params=pltpu.CompilerParams(
            collective_id=0, has_side_effects=True, vmem_limit_bytes=VMEM_LIMIT
        ),
    )(tok, go, in_q, in_o, in_u, in_d, si)


SEMS = 256
VMEM_LIMIT = 67043328


def per_device_fused(
    tokens_in, starts, ln1_gain, ln1_bias, w_qkv, b_qv, w_out, b_out,
    ln2_gain, ln2_bias, w_up, b_up, w_down, b_down, grad_out,
):
    rows, width = tokens_in.shape
    f32 = jnp.float32
    dp, z = lax.axis_index("dp"), lax.axis_index("tensor")
    part = width // 8
    dim = width // 16
    hidden = w_up.shape[1] // 4
    bit = ln1_gain.shape[0]
    here = jnp.arange(part) // bit == z
    vectors = jnp.stack([ln1_gain, ln1_bias, b_out, ln2_gain, ln2_bias, b_down])
    vectors = jnp.where(here, jnp.tile(vectors, (1, part // bit)), 0.0)
    begins = jnp.where(z == 0, starts.astype(f32), 0.0)
    begins = jnp.pad(begins, ((0, 1), (0, part - 4)))
    spot = (jnp.arange(8) == dp)[:, None]

    def spread(bias):
        entries = bias.astype(f32).reshape(4, -1, 1, bias.shape[1])
        return jnp.where(spot, entries, 0.0).reshape(4, -1, part)

    biases = jnp.concatenate(
        [spread(b_qv), spread(b_up), jnp.zeros((4, 5, part), f32)], axis=1
    )
    si = jnp.concatenate([jnp.concatenate([vectors, begins])[None], biases])
    in_q = w_qkv.reshape(part, 4, 3 * dim).transpose(1, 2, 0)
    in_o = w_out.reshape(4, dim, part)
    in_d = w_down.reshape(4, hidden, part)
    out, gtok, eq, eo, eu, ed, fs, fb = fused_layer(
        tokens_in, grad_out, in_q, in_o, w_up, in_d, si
    )
    grad_w_qkv = eq.transpose(2, 0, 1).reshape(part, 3 * 4 * dim).astype(f32)
    grad_w_out = eo.reshape(4 * dim, part).astype(f32)
    grad_w_up = eu.transpose(1, 0, 2).reshape(part, 4 * hidden).astype(f32)
    grad_w_down = ed.reshape(4 * hidden, part).astype(f32)
    take = lax.dynamic_slice_in_dim(fs, z * bit, bit, 1)

    def collect(rows, like):
        entries = rows.reshape(4, -1, 8, like.shape[1])
        return lax.dynamic_index_in_dim(entries, dp, 2, keepdims=False).reshape(like.shape)

    grad_b_qv = collect(fb[:, 0], b_qv)
    grad_b_up = collect(fb[:, 1:3], b_up)
    return (
        out, gtok, take[0], take[1], grad_w_qkv, grad_b_qv, grad_w_out, take[2],
        take[3], take[4], grad_w_up, grad_b_up, grad_w_down, take[5],
    )


def solution(mesh):
    sizes = (mesh.shape["dp"], mesh.shape["tensor"])

    def layer(tokens_in, starts, *others):
        fits = sizes == (8, 4) and tokens_in.shape[0] == PIECE and starts.shape == (1, 4)
        return (per_device_fused if fits else per_device)(tokens_in, starts, *others)

    return jax.shard_map(
        layer,
        mesh=mesh,
        in_specs=(
            P(("dp", "tensor"), None),
            P("dp", None),
            P(("dp", "tensor")),
            P(("dp", "tensor")),
            P("dp", "tensor"),
            P("tensor", "dp"),
            P("tensor", "dp"),
            P(("dp", "tensor")),
            P(("dp", "tensor")),
            P(("dp", "tensor")),
            P("dp", "tensor"),
            P("tensor", "dp"),
            P("tensor", "dp"),
            P(("dp", "tensor")),
            P(("dp", "tensor"), None),
        ),
        out_specs=(
            P(("dp", "tensor"), None),
            P(("dp", "tensor"), None),
            P(("dp", "tensor")),
            P(("dp", "tensor")),
            P("dp", "tensor"),
            P("tensor", "dp"),
            P("tensor", "dp"),
            P(("dp", "tensor")),
            P(("dp", "tensor")),
            P(("dp", "tensor")),
            P("dp", "tensor"),
            P("tensor", "dp"),
            P("tensor", "dp"),
            P(("dp", "tensor")),
        ),
        check_vma=False,
    )
```

```python
import functools

import jax
import jax.numpy as jnp
from jax import lax
from jax.experimental import pallas as pl
from jax.experimental.pallas import tpu as pltpu
from jax.sharding import PartitionSpec as P

HD = 64
PIECE = 256
QBLOCK = 512


EPS = 1e-05
ROOT = 0.7978845608028654


def gelu_tanh(values):
    return 0.5 * values * (1.0 + jnp.tanh(ROOT * (values + 0.044715 * values * values * values)))


def normalize(values):
    center = jnp.mean(values, axis=-1, keepdims=True)
    shifted = values - center
    inverse = lax.rsqrt(jnp.mean(shifted * shifted, axis=-1, keepdims=True) + EPS)
    return (shifted * inverse, inverse)


def norm_back(grad_normed, normed, inverse, gain):
    scaled = grad_normed * gain
    return inverse * (
        scaled
        - jnp.mean(scaled, axis=-1, keepdims=True)
        - normed * jnp.mean(scaled * normed, axis=-1, keepdims=True)
    )


def dot_last(left, right):
    return lax.dot_general(
        left, right, (((1,), (1,)), ((), ())), preferred_element_type=jnp.float32
    )


def dot_first(left, right):
    return lax.dot_general(
        left, right, (((0,), (0,)), ((), ())), preferred_element_type=jnp.float32
    )


def gather_rows(values):
    return lax.all_gather(values, "tensor", axis=0, tiled=True)


def gather_grads(values):
    return lax.all_gather(values, "tensor", axis=0, tiled=True)


def reduce_rows(left, weight, rows):

    def term(start, count):
        return jnp.dot(left, weight, preferred_element_type=jnp.float32)

    return lax.psum_scatter(
        term(jnp.int32(0), lax.axis_size("tensor") * rows).astype(jnp.bfloat16),
        "tensor",
        scatter_dimension=0,
        tiled=True,
    ).astype(jnp.float32)


def reduce_grads(left, weight, rows):

    def term(start, count):
        return dot_last(left, weight)

    return lax.psum_scatter(
        term(jnp.int32(0), lax.axis_size("tensor") * rows).astype(jnp.bfloat16),
        "tensor",
        scatter_dimension=0,
        tiled=True,
    ).astype(jnp.float32)


def piece_ids(start_row, length):
    places = jnp.arange(length, dtype=jnp.int32)
    inside = (places[:, None] >= start_row[None, :]) & (
        places[:, None] < start_row[None, :] + PIECE
    )
    labels = jnp.arange(1, start_row.shape[0] + 1, dtype=jnp.int32)
    return jnp.sum(jnp.where(inside, labels[None, :], 0), axis=1)


def allowed_block(row_ids, row_places, key_ids, key_places):
    causal = key_places[None, :] <= row_places[:, None]
    picture = (row_ids[:, None] == key_ids[None, :]) & (row_ids[:, None] > 0)
    return causal | picture


def block_scores(by_seq, start_rows, block_index):
    length = by_seq.shape[1]
    per_seq = length // QBLOCK
    seq_index = block_index // per_seq
    first_row = block_index % per_seq * QBLOCK
    sequence = lax.dynamic_index_in_dim(by_seq, seq_index, 0, keepdims=False)
    key_ids = piece_ids(lax.dynamic_index_in_dim(start_rows, seq_index, 0, keepdims=False), length)
    query_rows = lax.dynamic_slice_in_dim(sequence, first_row, QBLOCK, 0)[:, :, 0]
    key_rows = sequence[:, :, 1]
    value_rows = sequence[:, :, 2]
    row_ids = lax.dynamic_slice_in_dim(key_ids, first_row, QBLOCK, 0)
    row_places = first_row + jnp.arange(QBLOCK, dtype=jnp.int32)
    scores = (
        jnp.einsum("qhd,khd->hqk", query_rows, key_rows, preferred_element_type=jnp.float32) * 0.125
    )
    places = jnp.arange(length, dtype=jnp.int32)
    scores = jnp.where(allowed_block(row_ids, row_places, key_ids, places)[None], scores, -1e30)
    return (seq_index, first_row, query_rows, key_rows, value_rows, scores)


def attention_forward(by_seq, start_rows):
    total_blocks = by_seq.shape[0] * (by_seq.shape[1] // QBLOCK)

    def attend(block_index):
        _, _, query_rows, key_rows, value_rows, scores = block_scores(
            by_seq, start_rows, block_index
        )
        peak = jnp.max(scores, axis=-1, keepdims=True)
        log_total = peak + jnp.log(jnp.sum(jnp.exp(scores - peak), axis=-1, keepdims=True))
        probs = jnp.exp(scores - log_total)
        heads = jnp.einsum(
            "hqk,khd->qhd",
            probs.astype(jnp.bfloat16),
            value_rows,
            preferred_element_type=jnp.float32,
        )
        return (heads.astype(jnp.bfloat16), log_total)

    return lax.map(attend, jnp.arange(total_blocks, dtype=jnp.int32))


def attention_backward(by_seq, start_rows, log_totals, grad_heads):
    total_blocks = by_seq.shape[0] * (by_seq.shape[1] // QBLOCK)
    empty = jnp.zeros(by_seq.shape[:3] + (HD,), jnp.float32)

    def step(carry, item):
        grad_keys, grad_values = carry
        block_index, log_total = item
        seq_index, first_row, query_rows, key_rows, value_rows, scores = block_scores(
            by_seq, start_rows, block_index
        )
        grad_seq = lax.dynamic_index_in_dim(grad_heads, seq_index, 0, keepdims=False)
        grad_rows = lax.dynamic_slice_in_dim(grad_seq, first_row, QBLOCK, 0)
        probs = jnp.exp(scores - log_total)
        grad_probs = jnp.einsum(
            "qhd,khd->hqk", grad_rows, value_rows, preferred_element_type=jnp.float32
        )
        inner = jnp.sum(probs * grad_probs, axis=-1, keepdims=True)
        grad_scores = (probs * (grad_probs - inner)).astype(jnp.bfloat16)
        grad_query = (
            jnp.einsum("hqk,khd->qhd", grad_scores, key_rows, preferred_element_type=jnp.float32)
            * 0.125
        )
        key_term = (
            jnp.einsum("hqk,qhd->khd", grad_scores, query_rows, preferred_element_type=jnp.float32)
            * 0.125
        )
        value_term = jnp.einsum(
            "hqk,qhd->khd",
            probs.astype(jnp.bfloat16),
            grad_rows,
            preferred_element_type=jnp.float32,
        )
        grad_keys = lax.dynamic_update_index_in_dim(
            grad_keys,
            lax.dynamic_index_in_dim(grad_keys, seq_index, 0, keepdims=False) + key_term,
            seq_index,
            0,
        )
        grad_values = lax.dynamic_update_index_in_dim(
            grad_values,
            lax.dynamic_index_in_dim(grad_values, seq_index, 0, keepdims=False) + value_term,
            seq_index,
            0,
        )
        return ((grad_keys, grad_values), grad_query)

    (grad_keys, grad_values), grad_query = lax.scan(
        step, (empty, empty), (jnp.arange(total_blocks, dtype=jnp.int32), log_totals)
    )
    return (grad_query, grad_keys, grad_values)


def per_device(
    tokens_in,
    starts,
    ln1_gain,
    ln1_bias,
    w_qkv,
    b_qv,
    w_out,
    b_out,
    ln2_gain,
    ln2_bias,
    w_up,
    b_up,
    w_down,
    b_down,
    grad_out,
):
    rows = tokens_in.shape[0]
    gain_one, shift_one, bias_out, gain_two, shift_two, bias_down = (
        lax.all_gather(ln1_gain, ("dp", "tensor"), axis=0, tiled=True),
        lax.all_gather(ln1_bias, ("dp", "tensor"), axis=0, tiled=True),
        lax.all_gather(b_out, ("dp", "tensor"), axis=0, tiled=True),
        lax.all_gather(ln2_gain, ("dp", "tensor"), axis=0, tiled=True),
        lax.all_gather(ln2_bias, ("dp", "tensor"), axis=0, tiled=True),
        lax.all_gather(b_down, ("dp", "tensor"), axis=0, tiled=True),
    )
    weight_qkv, bias_qv, weight_out = (
        lax.all_gather(w_qkv, "dp", axis=0, tiled=True),
        lax.all_gather(b_qv, "dp", axis=1, tiled=True),
        lax.all_gather(w_out, "dp", axis=1, tiled=True),
    )
    weight_up, bias_up, weight_down = (
        lax.all_gather(w_up, "dp", axis=0, tiled=True),
        lax.all_gather(b_up, "dp", axis=1, tiled=True),
        lax.all_gather(w_down, "dp", axis=1, tiled=True),
    )
    local_heads = weight_qkv.shape[1] // (3 * HD)
    seq_count = starts.shape[0]
    inputs = tokens_in.astype(jnp.float32)
    normed_one, inverse_one = normalize(inputs)
    gathered_one = gather_rows((normed_one * gain_one + shift_one).astype(jnp.bfloat16))
    group = gathered_one.shape[0]
    length = group // seq_count
    bias_pair = bias_qv.astype(jnp.float32).reshape(local_heads, 2, HD)
    full_bias = jnp.stack(
        [bias_pair[:, 0], jnp.zeros_like(bias_pair[:, 0]), bias_pair[:, 1]], axis=1
    )
    projected = (
        jnp.dot(gathered_one, weight_qkv, preferred_element_type=jnp.float32).reshape(
            group, local_heads, 3, HD
        )
        + full_bias
    ).astype(jnp.bfloat16)
    by_seq = projected.reshape(seq_count, length, local_heads, 3, HD)
    heads_blocks, log_totals = attention_forward(by_seq, starts)
    heads_out = heads_blocks.reshape(group, local_heads * HD)
    middle = inputs + (reduce_rows(heads_out, weight_out, rows) + bias_out)
    normed_two, inverse_two = normalize(middle)
    rounded_two = (normed_two * gain_two + shift_two).astype(jnp.bfloat16)
    grad_final = grad_out.astype(jnp.float32)
    grad_bias_down = jnp.sum(grad_final, axis=0)
    gathered_two = gather_rows(rounded_two)
    up_proj = jnp.dot(gathered_two, weight_up, preferred_element_type=jnp.float32) + bias_up.astype(
        jnp.float32
    ).reshape(-1)
    hidden_act, gelu_pull = jax.vjp(gelu_tanh, up_proj)
    hidden_low = hidden_act.astype(jnp.bfloat16)
    output = (middle + reduce_rows(hidden_low, weight_down, rows) + bias_down).astype(jnp.bfloat16)
    grad_branch = gather_grads(grad_out)
    grad_w_down = dot_first(hidden_low, grad_branch)
    grad_up = gelu_pull(dot_last(grad_branch, weight_down))[0].astype(jnp.bfloat16)
    grad_b_up = jnp.sum(grad_up, axis=0, dtype=jnp.float32).reshape(bias_up.shape)
    grad_w_up = dot_first(gathered_two, grad_up)
    grad_two = reduce_grads(grad_up, weight_up, rows)
    grad_w_up, grad_b_up, grad_w_down = (
        lax.psum_scatter(
            grad_w_up.astype(jnp.bfloat16), "dp", scatter_dimension=0, tiled=True
        ).astype(jnp.float32),
        lax.psum_scatter(
            grad_b_up.astype(jnp.bfloat16), "dp", scatter_dimension=1, tiled=True
        ).astype(jnp.float32),
        lax.psum_scatter(
            grad_w_down.astype(jnp.bfloat16), "dp", scatter_dimension=1, tiled=True
        ).astype(jnp.float32),
    )
    grad_gain_two = jnp.sum(grad_two * normed_two, axis=0)
    grad_shift_two = jnp.sum(grad_two, axis=0)
    grad_middle = grad_final + norm_back(grad_two, normed_two, inverse_two, gain_two)
    grad_bias_out = jnp.sum(grad_middle, axis=0)
    grad_attn = gather_grads(grad_middle.astype(jnp.bfloat16))
    grad_w_out = dot_first(heads_out, grad_attn)
    grad_heads = (
        dot_last(grad_attn, weight_out)
        .astype(jnp.bfloat16)
        .reshape(seq_count, length, local_heads, HD)
    )
    grad_query, grad_keys, grad_values = attention_backward(by_seq, starts, log_totals, grad_heads)
    grad_proj = jnp.stack(
        [
            grad_query.reshape(group, local_heads, HD),
            grad_keys.reshape(group, local_heads, HD),
            grad_values.reshape(group, local_heads, HD),
        ],
        axis=2,
    ).astype(jnp.bfloat16)
    grad_b_qv = jnp.sum(grad_proj[:, :, 0::2], axis=0, dtype=jnp.float32).reshape(bias_qv.shape)
    grad_flat = grad_proj.reshape(group, 3 * local_heads * HD)
    grad_w_qkv = dot_first(gathered_one, grad_flat)
    grad_one = reduce_grads(grad_flat, weight_qkv, rows)
    grad_w_qkv, grad_b_qv, grad_w_out = (
        lax.psum_scatter(
            grad_w_qkv.astype(jnp.bfloat16), "dp", scatter_dimension=0, tiled=True
        ).astype(jnp.float32),
        lax.psum_scatter(
            grad_b_qv.astype(jnp.bfloat16), "dp", scatter_dimension=1, tiled=True
        ).astype(jnp.float32),
        lax.psum_scatter(
            grad_w_out.astype(jnp.bfloat16), "dp", scatter_dimension=1, tiled=True
        ).astype(jnp.float32),
    )
    grad_gain_one = jnp.sum(grad_one * normed_one, axis=0)
    grad_shift_one = jnp.sum(grad_one, axis=0)
    grad_tokens = (grad_middle + norm_back(grad_one, normed_one, inverse_one, gain_one)).astype(
        jnp.bfloat16
    )
    summed = (
        lax.psum_scatter(grad_gain_one, ("dp", "tensor"), scatter_dimension=0, tiled=True),
        lax.psum_scatter(grad_shift_one, ("dp", "tensor"), scatter_dimension=0, tiled=True),
        lax.psum_scatter(grad_bias_out, ("dp", "tensor"), scatter_dimension=0, tiled=True),
        lax.psum_scatter(grad_gain_two, ("dp", "tensor"), scatter_dimension=0, tiled=True),
        lax.psum_scatter(grad_shift_two, ("dp", "tensor"), scatter_dimension=0, tiled=True),
        lax.psum_scatter(grad_bias_down, ("dp", "tensor"), scatter_dimension=0, tiled=True),
    )
    return (
        output,
        grad_tokens,
        summed[0],
        summed[1],
        grad_w_qkv,
        grad_b_qv,
        grad_w_out,
        summed[2],
        summed[3],
        summed[4],
        grad_w_up,
        grad_b_up,
        grad_w_down,
        summed[5],
    )


MESH = pl.DeviceIdType.MESH
CH = 2
HOPS = 4
RELAYED = "ud"


class Fused:
    def __init__(self, names, refs):
        for name, ref in zip(names, refs):
            setattr(self, name, ref)
        self.next_sem = 0
        self.unsent = []
        self.groups = {0: [], 1: []}
        self.unsent_later = []
        dp, self.z = lax.axis_index("dp"), lax.axis_index("tensor")
        self.y, self.x, self.c = dp // 4, (dp // 2) % 2, dp % 2
        self.j = self.member(self.x, self.c)
        self.q = self.quarter(self.j)
        self.sib = self.dev(self.y, self.x, 1 - self.c, self.z)
        self.across = self.dev(self.y, 1 - self.x, self.c, self.z)
        self.q_sib = self.quarter(self.member(self.x, 1 - self.c))
        self.q_x = self.quarter(self.member(1 - self.x, self.c))
        self.q_d = self.quarter(self.member(1 - self.x, 1 - self.c))
        self.rows = self.tok.shape[0]
        self.width = self.tok.shape[1]
        self.part = self.width // 8

    def dev(self, y, x, c, z):
        return ((y * 2 + x) * 2 + c, z)

    def member(self, x, c):
        return 2 * c + x

    def local(self, member):
        return 2 * (member % 2) + member // 2

    def mate(self, member):
        return self.dev(self.y, member % 2, member // 2, self.z)

    def quarter(self, member):
        return (member - self.z - self.y + 8) % 4

    def sem(self, count=1):
        index = self.next_sem
        self.next_sem += count
        return index

    def copy(self, src, dst, device, index, sent=None):
        return pltpu.make_async_remote_copy(
            src_ref=src,
            dst_ref=dst,
            send_sem=self.ssem.at[index if sent is None else sent],
            recv_sem=self.rsem.at[index],
            device_id=device,
            device_id_type=MESH,
        )

    def send(self, src, dst, device, index, group=None):
        copy = self.copy(src, dst, device, index)
        copy.start()
        (self.unsent if group is None else self.groups[group]).append(copy)

    def later(self, view, sent, when=None):
        self.unsent_later.append((view, sent, when))

    def arrived(self, dst, index):
        self.copy(dst, dst, self.sib, index).wait_recv()

    def drain(self):
        for copy in self.unsent + self.groups[0] + self.groups[1]:
            copy.wait_send()
        for view, sent, when in self.unsent_later:
            copy = self.copy(view(), view(), self.sib, sent)
            if when is None:
                copy.wait_send()
            else:
                pl.when(when())(copy.wait_send)

    def at_quarter(self, quarter, chunk=None):
        if chunk is None:
            return pl.ds(pl.multiple_of(quarter * self.rows, self.rows), self.rows)
        size = self.rows // CH
        return pl.ds(pl.multiple_of(quarter * self.rows + chunk * size, size), size)

    def at_chunk(self, chunk):
        size = self.rows // CH
        return pl.ds(chunk * size, size)

    def barrier(self):
        me = lax.axis_index("dp") * 4 + self.z
        bar = pltpu.get_barrier_semaphore()

        def greet(step, carry):
            other = (me + step) % 32
            pl.semaphore_signal(
                bar, inc=1, device_id=(other // 4, other % 4), device_id_type=MESH
            )
            return carry

        lax.fori_loop(1, 32, greet, 0)
        pl.semaphore_wait(bar, 31)

    def homes(self):
        plane = 2 * self.y + self.x
        member = (plane + self.z + self.c) % 4
        worker = (self.c, member % 2, member // 2, plane)
        owner = (self.z // 2, self.z % 2, self.y, self.q)
        same = (
            (worker[0] == self.y)
            & (worker[1] == self.x)
            & (worker[2] == self.c)
            & (worker[3] == self.z)
        )
        return self.dev(*worker), self.dev(*owner), same

    def move_start(self, src, dst, outward, index):
        worker, owner, same = self.homes()
        copy = self.copy(src, dst, worker if outward else owner, index)
        local = pltpu.make_async_copy(src, dst, self.lsem.at[index])

        @pl.when(jnp.logical_not(same))
        def _():
            copy.start()

        @pl.when(same)
        def _():
            local.start()

    def move_wait(self, src, dst, index):
        same = self.homes()[2]
        copy = self.copy(src, dst, self.sib, index)
        local = pltpu.make_async_copy(src, dst, self.lsem.at[index])

        @pl.when(jnp.logical_not(same))
        def _():
            copy.wait_send()
            copy.wait_recv()

        @pl.when(same)
        def _():
            local.wait()

    def hop_rows(self, chunk):
        size = self.rows // HOPS
        return pl.ds(chunk * size, size)

    def hop_one(self, src, mid, index):
        plane = 2 * self.y + self.x
        member = (plane + self.z + self.c) % 4
        first = self.dev(self.c, member % 2, member // 2, self.z)
        same = (self.c == self.y) & (member % 2 == self.x) & (member // 2 == self.c)
        for chunk in range(HOPS):
            view, there = src.at[self.hop_rows(chunk)], mid.at[self.hop_rows(chunk)]
            copy = self.copy(view, there, first, index + chunk)
            local = pltpu.make_async_copy(view, there, self.lsem.at[index + chunk])
            pl.when(jnp.logical_not(same))(copy.start)
            pl.when(same)(local.start)

    def hop_two(self, src, mid, dst, place, index, onward):
        plane = self.q
        member = (2 * self.y + self.x + self.z + self.c) % 4
        home = (self.c == self.y) & (member % 2 == self.x) & (member // 2 == self.c)
        stay = plane == self.z
        for chunk in range(HOPS):
            rows = self.hop_rows(chunk)
            size = self.rows // HOPS
            there = dst.at[pl.ds(pl.multiple_of(place + chunk * size, size), size)]
            first = self.copy(src.at[rows], mid.at[rows], self.sib, index + chunk)
            local = pltpu.make_async_copy(src.at[rows], mid.at[rows], self.lsem.at[index + chunk])
            pl.when(jnp.logical_not(home))(first.wait_send)
            pl.when(jnp.logical_not(home))(first.wait_recv)
            pl.when(home)(local.wait)
            copy = self.copy(
                mid.at[rows], there, self.dev(self.y, self.x, self.c, plane), onward + chunk
            )
            keep = pltpu.make_async_copy(mid.at[rows], there, self.lsem.at[onward + chunk])
            pl.when(jnp.logical_not(stay))(copy.start)
            pl.when(stay)(keep.start)

    def hop_wait(self, mid, dst, place, onward, half):
        plane = self.q
        stay = plane == self.z
        for chunk in range(half * HOPS // CH, (half + 1) * HOPS // CH):
            rows = self.hop_rows(chunk)
            size = self.rows // HOPS
            there = dst.at[pl.ds(pl.multiple_of(place + chunk * size, size), size)]
            copy = self.copy(mid.at[rows], there, self.sib, onward + chunk)
            keep = pltpu.make_async_copy(mid.at[rows], there, self.lsem.at[onward + chunk])
            pl.when(jnp.logical_not(stay))(copy.wait_send)
            pl.when(jnp.logical_not(stay))(copy.wait_recv)
            pl.when(stay)(keep.wait)

    def span(self, half):
        return pl.ds(pl.multiple_of(half * 4 * self.part, 4 * self.part), 4 * self.part)

    def place(self, source):
        return pl.ds(pl.multiple_of(source * self.part, self.part), self.part)

    def cut(self, kind, ref, zc, where):
        if kind == "u":
            return ref.at[zc, where, :]
        return ref.at[zc, :, where]

    def piece(self, kind, ref, member):
        if kind == "u":
            wide = self.wbuf["u"].shape[2]
            return ref.at[:, pl.ds(pl.multiple_of(member * wide, wide), wide)]
        return ref.at[member]

    def weights_one(self, kind):
        source = 4 * self.y + self.local(self.j)
        here = self.cut(kind, self.wbuf[kind], self.z, self.place(source))
        self.one[kind] = []
        for step in range(1, 4):
            member = (self.j + step) % 4
            index = self.sem()
            self.send(
                self.piece(kind, self.shard[kind], member), here, self.mate(member), index
            )
            sender = 4 * self.y + self.local((self.j - step + 4) % 4)
            self.one[kind].append(
                (self.cut(kind, self.wbuf[kind], self.z, self.place(sender)), index)
            )
        index = self.sem()
        local = pltpu.make_async_copy(
            self.piece(kind, self.shard[kind], self.j), here, self.lsem.at[index]
        )
        local.start()
        self.own[kind] = local
        self.two[kind] = self.sem(4)
        self.three[kind] = self.sem(4)
        self.pass_sem[kind] = self.sem()

    def weights_in(self, kind):
        self.own[kind].wait()
        for view, index in self.one[kind]:
            self.arrived(view, index)
        self.weights_cross(kind, 0)

    def mine(self, kind, plane):
        return self.cut(kind, self.wbuf[kind], plane, self.span(self.y))

    def weights_two(self, kind):
        here = self.mine(kind, self.z)
        near, far = (lambda: self.z != 3), (lambda: self.z != 0)
        if kind not in RELAYED:
            near = far = None
        for step, when in ((2, None), (1, near), (3, far)):
            plane = (self.z + step) % 4
            index = self.two[kind] + step
            copy = self.copy(here, here, self.dev(self.y, self.x, self.c, plane), index)
            if when is None:
                copy.start()
            else:
                pl.when(when())(copy.start)
            self.later(lambda: self.mine(kind, self.z), index, when)

    def weights_relay(self, kind, guard=None):
        if kind not in RELAYED:
            return
        for here, plane, step in ((2, 3, 3), (1, 0, 1)):
            when = self.z == here
            block = self.mine(kind, (here + 2) % 4)
            copy = self.copy(
                block,
                block,
                self.dev(self.y, self.x, self.c, plane),
                self.two[kind] + step,
                self.pass_sem[kind],
            )
            pl.when(when if guard is None else when & guard)(copy.start)

    def relayed(self, kind):
        if kind in RELAYED:
            self.later(
                lambda: self.mine(kind, self.z),
                self.pass_sem[kind],
                lambda: (self.z == 1) | (self.z == 2),
            )
        for step in range(4):
            self.later(lambda: self.mine(kind, self.z), self.three[kind] + step)

    def weights_cross(self, kind, step):
        mine = self.mine(kind, (self.z - step + 4) % 4)
        self.copy(
            mine,
            mine,
            self.dev(1 - self.y, self.x, self.c, self.z),
            self.three[kind] + step,
        ).start()

    def weights_here(self, kind, step):
        self.arrived(self.mine(kind, (self.z - step + 4) % 4), self.two[kind] + step)

    def weights_three(self, kind, steps=(1, 3)):
        for step in steps:
            self.weights_here(kind, step)
            self.weights_cross(kind, step)

    def weights_start_three(self, kind):
        self.weights_here(kind, 2)
        self.weights_relay(kind)
        self.weights_cross(kind, 2)

    def weights_ready(self, kind, step):
        plane = (self.z - step + 4) % 4
        self.arrived(
            self.cut(kind, self.wbuf[kind], plane, self.span(1 - self.y)),
            self.three[kind] + step,
        )

    def weights_done(self, kind):
        for step in range(4):
            self.weights_ready(kind, step)

    def grads_one(self, kind):
        self.swaps[kind] = [self.sem() for _ in range(3)]
        for swap in self.swaps[kind]:
            self.later(lambda: self.zbuf[kind].at[0], swap)
        for turn in (2, 1, 3, 0):
            plane = (self.z + turn) % 4
            away = self.cut(kind, self.dbuf[kind], plane, self.span(1 - self.y))
            there = self.cut(kind, self.ybuf[kind], plane, slice(None))
            use = self.sem()
            self.send(away, there, self.dev(1 - self.y, self.x, self.c, self.z), use)
            self.backs.setdefault(kind, {})[turn] = use

    def grads_two(self, kind, turns=(2, 1, 3, 0)):
        for turn in turns:
            plane = (self.z + turn) % 4
            there = self.cut(kind, self.ybuf[kind], plane, slice(None))
            self.arrived(there, self.backs[kind][turn])
            mine = self.cut(kind, self.dbuf[kind], plane, self.span(self.y))
            mine[...] = (
                mine[...].astype(jnp.float32) + there[...].astype(jnp.float32)
            ).astype(jnp.bfloat16)
            if turn:
                self.copy(
                    mine,
                    self.zbuf[kind].at[turn - 1],
                    self.dev(self.y, self.x, self.c, plane),
                    self.swaps[kind][turn - 1],
                ).start()

    def head_one(self, step, head):
        self.copy(
            self.cut("q", self.dq, head, self.span(1 - self.y)),
            self.cut("q", self.yq, head, slice(None)),
            self.dev(1 - self.y, self.x, self.c, self.z),
            self.head_y + step,
        ).start()

    def head_add(self, step, head):
        there = self.cut("q", self.yq, head, slice(None))
        self.arrived(there, self.head_y + step)
        mine = self.cut("q", self.dq, head, self.span(self.y))
        mine[...] = (mine[...].astype(jnp.float32) + there[...].astype(jnp.float32)).astype(
            jnp.bfloat16
        )

    def head_two(self, step, head):
        self.copy(
            self.cut("q", self.dq, head, self.span(self.y)),
            self.zq.at[step],
            self.dev(self.y, self.x, self.c, head),
            self.head_z + step,
        ).start()

    def grads_three(self, kind):
        mine = self.cut(kind, self.dbuf[kind], self.z, self.span(self.y))
        total = mine[...].astype(jnp.float32)
        for step in range(1, 4):
            there = self.zbuf[kind].at[step - 1]
            self.arrived(there, self.swaps[kind][step - 1])
            total = total + there[...].astype(jnp.float32)
        final = self.fbuf[kind]
        final[...] = total.astype(jnp.bfloat16)
        ends = self.ebuf[kind]
        self.last[kind] = []
        for step in range(1, 4):
            member = (self.j + step) % 4
            index = self.sem()
            self.send(
                self.slab(kind, final, self.local(member)),
                ends.at[self.j],
                self.mate(member),
                index,
            )
            self.last[kind].append(((self.j - step + 4) % 4, index))
        index = self.sem()
        local = pltpu.make_async_copy(
            self.slab(kind, final, self.local(self.j)), ends.at[self.j], self.lsem.at[index]
        )
        local.start()
        self.own[kind] = local

    def slab(self, kind, ref, member):
        where = pl.ds(pl.multiple_of(member * self.part, self.part), self.part)
        if kind == "u":
            return ref.at[where, :]
        return ref.at[:, where]

    def grads_done(self, kind):
        self.own[kind].wait()
        for member, index in self.last[kind]:
            self.arrived(self.ebuf[kind].at[member], index)

    def small_one(self):
        self.sma[self.z] = self.si[...]
        self.small_sem = [self.sem() for _ in range(3)]
        for step in range(1, 4):
            plane = (self.z + step) % 4
            self.send(
                self.si,
                self.sma.at[self.z],
                self.dev(self.y, self.x, self.c, plane),
                self.small_sem[step - 1],
            )

    def around(self, step):
        return (lax.axis_index("dp") + step + 8) % 8

    def small_two(self):
        for step in range(1, 4):
            self.arrived(self.sma.at[(self.z - step + 4) % 4], self.small_sem[step - 1])
        me = self.around(0)
        self.lb[me] = sum(self.sma[plane, 0] for plane in range(4))
        self.bb[me] = self.sma[:, 1 + self.j]
        self.plane_sem = [(self.sem(), self.sem()) for _ in range(7)]
        for step in range(1, 8):
            other = self.around(step)
            member = self.member((other // 2) % 2, other % 2)
            first, second = self.plane_sem[step - 1]
            self.send(self.lb.at[me], self.lb.at[me], (other, self.z), first)
            self.send(self.sma.at[:, 1 + member], self.bb.at[me], (other, self.z), second)

    def small_three(self):
        for step in range(1, 8):
            other = self.around(-step)
            first, second = self.plane_sem[step - 1]
            self.arrived(self.lb.at[other], first)
            self.arrived(self.bb.at[other], second)
        part, dim = self.part, self.qh.shape[2]
        for source in range(8):
            self.small[:, source * part : (source + 1) * part] = self.lb[source]
        bias = sum(self.bb[source] for source in range(8))
        for head in range(4):
            row = bias[head, 0:1]
            self.bq[head, :, 0:dim] = row[:, 0:dim]
            self.bq[head, :, dim : 2 * dim] = jnp.zeros((1, dim), jnp.float32)
            self.bq[head, :, 2 * dim :] = row[:, dim:]
            for half in range(2):
                place = (2 * head + half) * part
                self.bu[:, place : place + part] = bias[head, 1 + half : 2 + half]

    def back_one(self):
        part, me = self.part, self.around(0)
        for target in range(8):
            self.cs[target] = self.sums[:, target * part : (target + 1) * part]
        self.cr[me] = self.cs[me]
        self.cd[me] = self.cb[...]
        self.back_sem = [(self.sem(), self.sem()) for _ in range(7)]
        for step in range(1, 8):
            other = self.around(step)
            first, second = self.back_sem[step - 1]
            self.send(self.cs.at[other], self.cr.at[me], (other, self.z), first)
            self.send(self.cb, self.cd.at[me], (other, self.z), second)

    def back_two(self):
        for step in range(1, 8):
            other = self.around(-step)
            first, second = self.back_sem[step - 1]
            self.arrived(self.cr.at[other], first)
            self.arrived(self.cd.at[other], second)
        self.es[self.z] = sum(self.cr[source] for source in range(8))
        for member in range(4):
            pair = [2 * (member % 2) + member // 2, 4 + 2 * (member % 2) + member // 2]
            self.ed_small[:, member] = self.cd[pair[0]] + self.cd[pair[1]]
        self.eb[self.z] = self.ed_small[self.z]
        self.line_sem = [(self.sem(), self.sem()) for _ in range(3)]
        for step in range(1, 4):
            plane = (self.z + step) % 4
            device = self.dev(self.y, self.x, self.c, plane)
            first, second = self.line_sem[step - 1]
            self.send(self.es.at[self.z], self.es.at[self.z], device, first)
            self.send(self.ed_small.at[plane], self.eb.at[self.z], device, second)

    def back_three(self):
        for step in range(1, 4):
            plane = (self.z - step + 4) % 4
            first, second = self.line_sem[step - 1]
            self.arrived(self.es.at[plane], first)
            self.arrived(self.eb.at[plane], second)
        self.fs[...] = sum(self.es[plane] for plane in range(4))
        self.fb[...] = sum(self.eb[plane] for plane in range(4))

    def gather_plan(self):
        return {kind: [self.sem() for _ in range(CH)] for kind in ("across", "sib", "pass")}

    def gather_send(self, buf, plan, chunk):
        rows = self.at_quarter(self.q, chunk)
        for device, kind in ((self.across, "across"), (self.sib, "sib")):
            self.copy(buf.at[rows], buf.at[rows], device, plan[kind][chunk]).start()
            self.later(lambda: buf.at[self.at_quarter(self.q, 0)], plan[kind][chunk])

    def gather_pass(self, buf, plan):
        for chunk in range(CH):
            rows = self.at_quarter(self.q_x, chunk)
            self.arrived(buf.at[rows], plan["across"][chunk])
            self.send(buf.at[rows], buf.at[rows], self.sib, plan["pass"][chunk])

    def gather_sib(self, buf, plan):
        for chunk in range(CH):
            self.arrived(buf.at[self.at_quarter(self.q_sib, chunk)], plan["sib"][chunk])

    def gather_last(self, buf, plan):
        for chunk in range(CH):
            self.arrived(buf.at[self.at_quarter(self.q_d, chunk)], plan["pass"][chunk])

    def gathered(self, buf, plan, use):
        use(self.q)
        self.gather_sib(buf, plan)
        use(self.q_sib)
        self.gather_pass(buf, plan)
        use(self.q_x)
        self.gather_last(buf, plan)
        use(self.q_d)

    def scatter_start(self, partial, own, which, rx, hold=False):
        sa, ra, sb, sc, rb = (self.rs.at[which, slot] for slot in range(5))
        plan = [[self.sem() for _ in range(CH)] for _ in range(3)]
        low = jnp.bfloat16
        for copy in self.groups[which]:
            copy.wait_send()
        self.groups[which] = []
        sa[...] = partial(self.q_d).astype(low)
        for chunk in range(CH):
            rows = self.at_chunk(chunk)
            self.send(sa.at[rows], ra.at[rows], self.sib, plan[0][chunk], which)
        held = partial(self.q_x)
        for chunk in range(CH):
            self.arrived(ra.at[self.at_chunk(chunk)], plan[0][chunk])
        sb[...] = (held + ra[...].astype(jnp.float32)).astype(low)
        if not hold:
            self.scatter_send((plan, which, rx))
        sc[...] = partial(self.q_sib).astype(low)
        for chunk in range(CH):
            rows = self.at_chunk(chunk)
            self.send(sc.at[rows], rb.at[rows], self.sib, plan[2][chunk], which)
        own[...] = partial(self.q)
        return plan, which, rx

    def scatter_send(self, started):
        plan, which, rx = started
        sb = self.rs.at[which, 2]
        for chunk in range(CH):
            rows = self.at_chunk(chunk)
            self.send(sb.at[rows], rx.at[rows], self.across, plan[1][chunk], which)

    def scatter_chunk(self, started, own, chunk):
        plan, which, rx = started
        rows = self.at_chunk(chunk)
        rb = self.rs.at[which, 4]
        self.arrived(rb.at[rows], plan[2][chunk])
        self.arrived(rx.at[rows], plan[1][chunk])
        return (
            own[rows, :] + rb[rows, :].astype(jnp.float32) + rx[rows, :].astype(jnp.float32)
        )

    def run(self):
        f32, low = jnp.float32, jnp.bfloat16
        rows, width = self.rows, self.width
        quarters = range(4)
        self.wbuf = dict(q=self.wq, o=self.wo, u=self.wu, d=self.wd)
        self.shard = dict(q=self.in_q, o=self.in_o, u=self.in_u, d=self.in_d)
        self.dbuf = dict(q=self.dq, o=self.do, u=self.du, d=self.dd)
        self.ybuf = dict(q=self.yq, o=self.yo, u=self.yu, d=self.yd)
        self.zbuf = dict(q=self.zq, o=self.zo, u=self.zu, d=self.zd)
        self.fbuf = dict(q=self.fq, o=self.fo, u=self.fu, d=self.fd)
        self.ebuf = dict(q=self.eq, o=self.eo, u=self.eu, d=self.ed)
        self.one, self.two, self.three, self.own = {}, {}, {}, {}
        self.back, self.backs, self.swaps, self.last = {}, {}, {}, {}
        self.pass_sem = {}
        heads, dim = self.qh.shape[0], self.qh.shape[2]
        hidden = self.wu.shape[2]

        self.barrier()
        move = [self.sem() for _ in range(4)]
        self.small_one()
        hop = [self.sem(HOPS) for _ in range(4)]
        self.hop_one(self.tok, self.mid_x, hop[0])
        self.hop_one(self.go, self.ox, hop[2])
        self.weights_one("q")
        plan_one, plan_two, plan_go, plan_mid = (self.gather_plan() for _ in range(4))
        self.hop_two(self.tok, self.mid_x, self.xs, 0, hop[0], hop[1])
        self.small_two()
        own_rows = self.at_quarter(self.q)
        self.weights_in("q")
        self.weights_two("q")
        for kind in "ou":
            self.weights_one(kind)
        self.small_three()
        gain_one, shift_one = self.small[0:1, :], self.small[1:2, :]
        bias_out = self.small[2:3, :]
        gain_two, shift_two = self.small[3:4, :], self.small[4:5, :]
        bias_down = self.small[5:6, :]

        for chunk in range(CH):
            part = self.at_chunk(chunk)
            self.hop_wait(self.mid_x, self.xs, 0, hop[1], chunk)
            normed, inverse = normalize(self.xs[part, :].astype(f32))
            self.n1[part, :] = normed
            self.i1[part, :] = inverse
            self.h1[self.at_quarter(self.q, chunk), :] = (normed * gain_one + shift_one).astype(low)
            self.gather_send(self.h1, plan_one, chunk)
        self.mask_blocks()
        near = 1 + 2 * ((3 - self.z) // 3)
        self.gather_sib(self.h1, plan_one)
        self.weights_start_three("q")
        self.weights_in("o")
        self.weights_two("o")
        self.hop_two(self.go, self.ox, self.gg, self.z * rows, hop[2], hop[3])
        self.gather_pass(self.h1, plan_one)
        self.weights_one("d")
        self.weights_three("q", (near,))
        self.gather_last(self.h1, plan_one)

        def parts_of(block):
            return ([(0, block * rows)] if block else []) + [(block * rows, rows)]

        def turn(step):
            late, odd = step // 2, step % 2
            return (1 - late) * 2 * odd + late * (near + odd * (4 - 2 * near))

        def attend(step, carry):
            back = turn(step)
            head = (self.z - back + 4) % 4
            self.weights_ready("q", back)

            def project(block, carry):
                place = pl.ds(pl.multiple_of(block * rows, rows), rows)
                both = dot_last(self.h1[place, :], self.wq[head]) + self.bq[head]
                for slot, ref in enumerate((self.qh, self.kh, self.vh)):
                    value = both[:, slot * dim : (slot + 1) * dim].astype(low)
                    if slot == 0:
                        value = (value.astype(f32) * 0.125).astype(low)
                    ref[head, place, :] = value
                return carry

            lax.fori_loop(0, 4, project, 0)

            @pl.when(step == 0)
            def _():
                self.weights_three("q", (4 - near,))
                self.weights_in("u")
                self.weights_two("u")

            @pl.when(step == 1)
            def _():
                self.weights_start_three("o")

            @pl.when(step == 2)
            def _():
                self.weights_three("o")
                for chunk in range(CH):
                    self.hop_wait(self.ox, self.gg, self.q * rows, hop[3], chunk)
                    self.gather_send(self.gg, plan_go, chunk)

            @pl.when(step == 3)
            def _():
                self.weights_start_three("u")

            for block in quarters:
                place = pl.ds(block * rows, rows)
                query = self.qh[head, place, :]
                scores = []
                for first, count in parts_of(block):
                    value = dot_last(query, self.kh[head, pl.ds(first, count), :])
                    if first == block * rows:
                        value = value + self.mk[block].astype(f32)
                    scores.append(value)
                peak = functools.reduce(
                    jnp.maximum, [jnp.max(value, axis=1, keepdims=True) for value in scores]
                )
                powers = [jnp.exp(value - peak) for value in scores]
                total = sum(jnp.sum(value, axis=1, keepdims=True) for value in powers)
                scale = 1.0 / total
                result = 0.0
                for (first, count), value in zip(parts_of(block), powers):
                    probs = (value * scale).astype(low)
                    self.pb[block][head, :, pl.ds(first, count)] = probs
                    result = result + jnp.dot(
                        probs,
                        self.vh[head, pl.ds(first, count), :],
                        preferred_element_type=f32,
                    )
                self.hh[head, place, :] = result.astype(low)
            return carry

        lax.fori_loop(0, heads, attend, 0)
        for kind in "qou":
            self.relayed(kind)

        def assemble(target, refs, count):
            def one(block, carry):
                place = pl.ds(pl.multiple_of(block * rows, rows), rows)
                pieces = [ref[head, place, :] for ref in refs for head in range(count)]
                target[place, :] = jnp.concatenate(pieces, axis=1)
                return carry

            lax.fori_loop(0, 4, one, 0)

        assemble(self.ho, (self.hh,), heads)
        self.weights_done("o")

        flat_out = lambda: self.wo[...].reshape(heads * dim, width)
        started = self.scatter_start(
            lambda quarter: jnp.dot(
                self.ho[self.at_quarter(quarter), :], flat_out(), preferred_element_type=f32
            ),
            self.own_a,
            0,
            self.rx.at[0],
        )
        self.weights_in("d")
        self.weights_two("d")
        self.weights_three("u")
        for chunk in range(CH):
            part = self.at_chunk(chunk)
            summed = self.scatter_chunk(started, self.own_a, chunk)
            middle = self.xs[part, :].astype(f32) + (summed + bias_out)
            self.mid[part, :] = middle
            normed, inverse = normalize(middle)
            self.n2[part, :] = normed
            self.i2[part, :] = inverse
            self.h2[self.at_quarter(self.q, chunk), :] = (normed * gain_two + shift_two).astype(low)
            self.gather_send(self.h2, plan_two, chunk)
        self.gather_sib(self.gg, plan_go)
        self.gather_pass(self.gg, plan_go)
        self.weights_start_three("d")
        self.relayed("d")
        self.weights_done("u")

        def up(quarter):
            place = self.at_quarter(quarter)

            for block in range(4):
                lanes = pl.ds(block * hidden, hidden)
                value = (
                    jnp.dot(self.h2[place, :], self.wu[block], preferred_element_type=f32)
                    + self.bu[:, lanes]
                )
                square = value * value
                bend = jnp.tanh(ROOT * (value + 0.044715 * value * square))
                self.hid[place, lanes] = (0.5 * value * (1.0 + bend)).astype(low)
                slope = 0.5 * (1.0 + bend) + 0.5 * value * (1.0 - bend * bend) * ROOT * (
                    1.0 + 3.0 * 0.044715 * square
                )
                self.gu[place, lanes] = slope.astype(low)

        up(self.q)
        self.gather_sib(self.h2, plan_two)
        up(self.q_sib)
        self.weights_three("d", (near,))
        self.gather_pass(self.h2, plan_two)
        up(self.q_x)
        self.weights_three("d", (4 - near,))
        self.gather_last(self.h2, plan_two)
        up(self.q_d)
        flat_down = lambda: self.wd[...].reshape(4 * hidden, width)
        grad_out = self.gg[own_rows, :].astype(f32)
        self.sums[5:6, :] = jnp.sum(grad_out, axis=0, keepdims=True)
        self.gather_last(self.gg, plan_go)

        def down_grad(block, carry):
            lanes = pl.ds(pl.multiple_of(block * hidden, hidden), hidden)
            self.dd[block] = dot_first(self.hid[:, lanes], self.gg[...]).astype(low)
            return carry

        lax.fori_loop(0, 4, down_grad, 0)
        self.grads_one("d")
        self.weights_done("d")

        def to_up(quarter):
            place = self.at_quarter(quarter)
            value = dot_last(self.gg[place, :], flat_down())
            self.gu[place, :] = (self.gu[place, :].astype(f32) * value).astype(low)

        for quarter in (self.q_d, self.q_x, self.q_sib, self.q):
            to_up(quarter)
        self.grads_two("d", (2,))

        def two_part(quarter):
            place = self.at_quarter(quarter)
            return sum(
                dot_last(self.gu[place, pl.ds(block * hidden, hidden)], self.wu[block])
                for block in range(4)
            )

        started = self.scatter_start(two_part, self.own_a, 0, self.rx.at[0])

        self.grads_two("d", (1,))
        step = width // 4

        def up_grad(block, carry):
            lanes = pl.ds(pl.multiple_of(block * step, step), step)
            value = dot_first(self.h2[:, lanes], self.gu[...]).astype(low)
            for plane in range(4):
                self.du[plane, lanes, :] = value[:, plane * hidden : (plane + 1) * hidden]
            return carry

        lax.fori_loop(0, 4, up_grad, 0)
        self.grads_one("u")
        started_down = self.scatter_start(
            lambda quarter: jnp.dot(
                self.hid[self.at_quarter(quarter), :], flat_down(), preferred_element_type=f32
            ),
            self.own_b,
            1,
            self.rx.at[1],
            hold=True,
        )
        self.grads_two("d", (3, 0))
        totals = [0.0] * 3
        for chunk in range(CH):
            part = self.at_chunk(chunk)
            grad_two = self.scatter_chunk(started, self.own_a, chunk)
            normed = self.n2[part, :]
            middle = self.gg[self.at_quarter(self.q, chunk), :].astype(f32) + norm_back(
                grad_two, normed, self.i2[part, :], gain_two
            )
            self.gm[part, :] = middle
            self.ga[self.at_quarter(self.q, chunk), :] = middle.astype(low)
            self.gather_send(self.ga, plan_mid, chunk)
            for place, value in enumerate((grad_two * normed, grad_two, middle)):
                totals[place] = totals[place] + jnp.sum(value, axis=0, keepdims=True)
        self.sums[3:4, :] = totals[0]
        self.sums[4:5, :] = totals[1]
        self.sums[2:3, :] = totals[2]
        self.scatter_send(started_down)
        up_sum = jnp.sum(self.gu[...].astype(f32), axis=0, keepdims=True)
        lanes = self.part
        for place in range(8):
            self.cb[place // 2, 1 + place % 2 : 2 + place % 2, :] = up_sum[
                :, place * lanes : (place + 1) * lanes
            ]
        def to_heads(quarter):
            place = self.at_quarter(quarter)
            value = dot_last(self.ga[place, :], flat_out()).astype(low)
            for head in range(heads):
                self.hh[head, place, :] = value[:, head * dim : (head + 1) * dim]

        to_heads(self.q)
        self.gather_sib(self.ga, plan_mid)
        to_heads(self.q_sib)
        self.grads_two("u", (2,))
        self.gather_pass(self.ga, plan_mid)
        to_heads(self.q_x)
        self.grads_two("u", (1,))
        self.gather_last(self.ga, plan_mid)
        to_heads(self.q_d)
        self.do[...] = dot_first(self.ho[...], self.ga[...]).astype(low).reshape(self.do.shape)
        self.grads_one("o")

        self.head_y, self.head_z = self.sem(4), self.sem(3)

        def attend_back(step, carry):
            head = (self.z + 1 + step) % 4
            self.ka[...] = jnp.zeros_like(self.ka)
            self.va[...] = jnp.zeros_like(self.va)
            for block in quarters:
                place = pl.ds(block * rows, rows)
                query = self.qh[head, place, :]
                grads = self.hh[head, place, :]
                probs, values = [], []
                inner = 0.0
                for first, count in parts_of(block):
                    span = pl.ds(first, count)
                    prob = self.pb[block][head, :, span]
                    value = dot_last(grads, self.vh[head, span, :])
                    self.va[span, :] += dot_first(prob, grads)
                    prob = prob.astype(f32)
                    inner = inner + jnp.sum(prob * value, axis=1, keepdims=True)
                    probs.append(prob)
                    values.append(value)
                result = 0.0
                for (first, count), prob, value in zip(parts_of(block), probs, values):
                    span = pl.ds(first, count)
                    score = (prob * (value - inner)).astype(low)
                    result = result + jnp.dot(
                        score, self.kh[head, span, :], preferred_element_type=f32
                    )
                    self.ka[span, :] += dot_first(score, query)
                self.qh[head, place, :] = (result * 0.125).astype(low)
            self.gp[head, :, 0:dim] = self.qh[head]
            self.gp[head, :, dim : 2 * dim] = self.ka[...].astype(low)
            self.gp[head, :, 2 * dim :] = self.va[...].astype(low)
            self.dq[head] = dot_first(self.gp[head], self.h1[...]).astype(low)
            self.head_one(step, head)

            @pl.when(step == 0)
            def _():
                self.grads_two("u", (3, 0))

            @pl.when(step == 2)
            def _():
                self.grads_two("o")

            @pl.when(step == 1)
            def _():
                for chunk in range(CH):
                    part = self.at_chunk(chunk)
                    summed = self.scatter_chunk(started_down, self.own_b, chunk)
                    self.ox[part, :] = (self.mid[part, :] + summed + bias_down).astype(low)
                self.move_start(self.ox, self.out, False, move[2])

            return carry

        lax.fori_loop(0, heads, attend_back, 0)
        self.swaps["q"] = [self.head_z + step for step in range(3)]
        for step in range(4):
            self.later(lambda: self.cut("q", self.dq, 0, self.span(0)), self.head_y + step)
        for step in range(3):
            self.later(lambda: self.zq.at[0], self.head_z + step)
        started = self.scatter_start(
            lambda quarter: sum(
                jnp.dot(
                    self.gp[head, self.at_quarter(quarter), :],
                    self.wq[head],
                    preferred_element_type=f32,
                )
                for head in range(heads)
            ),
            self.own_a,
            0,
            self.rx.at[0],
        )
        for step in range(3):
            head = (self.z + 1 + step) % 4
            self.head_add(step, head)
            self.head_two(step, head)
        for head in range(heads):
            total = jnp.sum(self.gp[head].astype(f32), axis=0, keepdims=True)
            self.cb[head, 0:1, 0:dim] = total[:, 0:dim]
            self.cb[head, 0:1, dim:] = total[:, 2 * dim :]
            self.cb[head, 3:, :] = jnp.zeros((5, self.part), f32)
        self.grads_three("d")
        self.head_add(3, self.z)
        totals = [0.0] * 2
        for chunk in range(CH):
            part = self.at_chunk(chunk)
            grad_one = self.scatter_chunk(started, self.own_a, chunk)
            normed = self.n1[part, :]
            self.xs[part, :] = (
                self.gm[part, :] + norm_back(grad_one, normed, self.i1[part, :], gain_one)
            ).astype(low)
            for place, value in enumerate((grad_one * normed, grad_one)):
                totals[place] = totals[place] + jnp.sum(value, axis=0, keepdims=True)
        self.sums[0:1, :] = totals[0]
        self.sums[1:2, :] = totals[1]
        self.sums[6:8, :] = jnp.zeros((2, width), f32)
        self.back_one()
        self.move_start(self.xs, self.gtok, False, move[3])
        self.grads_three("u")
        self.grads_three("o")
        self.back_two()
        self.grads_three("q")
        for kind in "duoq":
            self.grads_done(kind)
        self.move_wait(self.ox, self.out, move[2])
        self.back_three()
        self.move_wait(self.xs, self.gtok, move[3])
        self.drain()

    def mask_blocks(self):
        rows = self.rows
        begins = self.lb[2 * self.z + self.y, 6:7, 0:4].astype(jnp.int32)
        for block in range(4):
            down = block * rows + lax.broadcasted_iota(jnp.int32, (rows, 1), 0)
            side = block * rows + lax.broadcasted_iota(jnp.int32, (1, rows), 1)

            def ids(places):
                total = jnp.zeros_like(places)
                for piece in range(4):
                    first = begins[:, piece : piece + 1]
                    inside = (places >= first) & (places < first + PIECE)
                    total = jnp.where(inside, piece + 1, total)
                return total

            mine, theirs = ids(down), ids(side)
            seen = (side <= down) | ((mine == theirs) & (mine > 0))
            self.mk[block] = jnp.where(seen, 0.0, -1e30).astype(jnp.bfloat16)


IN_NAMES = ("tok", "go", "in_q", "in_o", "in_u", "in_d", "si")
OUT_NAMES = ("out", "gtok", "eq", "eo", "eu", "ed", "fs", "fb")


def fused_layer(tok, go, in_q, in_o, in_u, in_d, si):
    rows, width = tok.shape
    heads, dim = 4, width // 16
    hidden = in_u.shape[1] // 4
    part = width // 8
    n = 4 * rows
    low, f32 = jnp.bfloat16, jnp.float32
    scratch = dict(
        xs=((rows, width), low),
        mid_x=((rows, width), low),
        wq=((4, 3 * dim, width), low),
        wo=((4, dim, width), low),
        wu=((4, width, hidden), low),
        wd=((4, hidden, width), low),
        h1=((n, width), low),
        h2=((n, width), low),
        gg=((n, width), low),
        ga=((n, width), low),
        qh=((heads, n, dim), low),
        kh=((heads, n, dim), low),
        vh=((heads, n, dim), low),
        hh=((heads, n, dim), low),
        ho=((n, heads * dim), low),
        gp=((heads, n, 3 * dim), low),
        ka=((n, dim), f32),
        va=((n, dim), f32),
        mk=((4, rows, rows), low),
        n1=((rows, width), f32),
        n2=((rows, width), f32),
        mid=((rows, width), f32),
        gm=((rows, width), f32),
        i1=((rows, 1), f32),
        i2=((rows, 1), f32),
        own_a=((rows, width), f32),
        own_b=((rows, width), f32),
        hid=((n, 4 * hidden), low),
        gu=((n, 4 * hidden), low),
        ox=((rows, width), low),
        rs=((2, 5, rows, width), low),
        rx=((2, rows, width), low),
        dq=((4, 3 * dim, width), low),
        do=((4, dim, width), low),
        du=((4, width, hidden), low),
        dd=((4, hidden, width), low),
        yq=((4, 3 * dim, 4 * part), low),
        yo=((4, dim, 4 * part), low),
        yu=((4, 4 * part, hidden), low),
        yd=((4, hidden, 4 * part), low),
        zq=((3, 3 * dim, 4 * part), low),
        zo=((3, dim, 4 * part), low),
        zu=((3, 4 * part, hidden), low),
        zd=((3, hidden, 4 * part), low),
        fq=((3 * dim, 4 * part), low),
        fo=((dim, 4 * part), low),
        fu=((4 * part, hidden), low),
        fd=((hidden, 4 * part), low),
        small=((8, width), f32),
        sums=((8, width), f32),
        bq=((4, 1, 3 * dim), f32),
        bu=((1, 4 * hidden), f32),
        sma=((4, 5, 8, part), f32),
        lb=((8, 8, part), f32),
        bb=((8, 4, 8, part), f32),
        cs=((8, 8, part), f32),
        cr=((8, 8, part), f32),
        cb=((4, 8, part), f32),
        cd=((8, 4, 8, part), f32),
        es=((4, 8, part), f32),
        ed_small=((4, 4, 8, part), f32),
        eb=((4, 4, 8, part), f32),
    )
    probs = [((heads, rows, (block + 1) * rows), low) for block in range(4)]
    names = IN_NAMES + OUT_NAMES + tuple(scratch)

    def kernel(*refs):
        count = len(names)
        state = Fused(names, refs[:count])
        state.pb = refs[count : count + 4]
        state.ssem, state.rsem, state.lsem = refs[count + 4 :]
        state.run()

    hbm = pl.BlockSpec(memory_space=pl.ANY)
    vmem = pl.BlockSpec(memory_space=pltpu.VMEM)
    return pl.pallas_call(
        kernel,
        out_shape=(
            jax.ShapeDtypeStruct((rows, width), low),
            jax.ShapeDtypeStruct((rows, width), low),
            jax.ShapeDtypeStruct((4, 3 * dim, part), low),
            jax.ShapeDtypeStruct((4, dim, part), low),
            jax.ShapeDtypeStruct((4, part, hidden), low),
            jax.ShapeDtypeStruct((4, hidden, part), low),
            jax.ShapeDtypeStruct((8, part), f32),
            jax.ShapeDtypeStruct((4, 8, part), f32),
        ),
        in_specs=[hbm] * 6 + [vmem],
        out_specs=(hbm,) * 6 + (vmem,) * 2,
        scratch_shapes=[pltpu.VMEM(*spec) for spec in scratch.values()]
        + [pltpu.VMEM(*spec) for spec in probs]
        + [pltpu.SemaphoreType.DMA((SEMS,))] * 3,
        name="fused_layer",
        compiler_params=pltpu.CompilerParams(
            collective_id=0, has_side_effects=True, vmem_limit_bytes=VMEM_LIMIT
        ),
    )(tok, go, in_q, in_o, in_u, in_d, si)


def finish(out, gtok, eq, eo, eu, ed, fs, fb):
    rows, width = out.shape
    part = eq.shape[2]
    bit = part // 4
    f32 = jnp.float32

    def kernel(out_ref, gtok_ref, eq_ref, eo_ref, eu_ref, ed_ref, fs_ref, fb_ref, *ends):
        ends[0][...] = out_ref[...]
        ends[1][...] = gtok_ref[...]
        deep, wide = eq_ref.shape[1], eu_ref.shape[2]
        for member in range(4):
            ends[2][:, member * deep : (member + 1) * deep] = eq_ref[member].astype(f32).T
            ends[4][:, member * wide : (member + 1) * wide] = eu_ref[member].astype(f32)
        ends[3][...] = eo_ref[...].reshape(ends[3].shape).astype(f32)
        ends[5][...] = ed_ref[...].reshape(ends[5].shape).astype(f32)
        z = lax.axis_index("tensor")
        mine = fs_ref[:, 0:bit]
        for plane in range(1, 4):
            mine = jnp.where(z == plane, fs_ref[:, plane * bit : (plane + 1) * bit], mine)
        for row in range(6):
            ends[6 + row][...] = mine[row]
        dp, deep = lax.axis_index("dp"), part // 16
        for end, first, count in ((ends[12], 0, 1), (ends[13], 1, 2)):
            spread = jnp.concatenate(
                [
                    jnp.broadcast_to(fb_ref[member, first + half : first + half + 1, :], (deep, part))
                    for member in range(4)
                    for half in range(count)
                ]
            )
            row = lax.broadcasted_iota(jnp.int32, spread.shape, 0) % deep
            lane = lax.broadcasted_iota(jnp.int32, spread.shape, 1)
            for side in range(2):
                kept = jnp.where(lane == row * 16 + 2 * dp + side, spread, 0.0)
                end[side : side + 1, :] = lax.dot_general(
                    jnp.ones((1, part), f32),
                    kept,
                    (((1,), (1,)), ((), ())),
                    precision=lax.Precision.HIGHEST,
                    preferred_element_type=f32,
                )

    shapes = [
        out,
        gtok,
        jax.ShapeDtypeStruct((part, 4 * eq.shape[1]), f32),
        jax.ShapeDtypeStruct((4 * eo.shape[1], part), f32),
        jax.ShapeDtypeStruct((part, 4 * eu.shape[2]), f32),
        jax.ShapeDtypeStruct((4 * ed.shape[1], part), f32),
    ] + [jax.ShapeDtypeStruct((bit,), f32)] * 6
    shapes += [jax.ShapeDtypeStruct((2, size), f32) for size in (part // 4, part // 2)]
    return pl.pallas_call(
        kernel,
        out_shape=[jax.ShapeDtypeStruct(shape.shape, shape.dtype) for shape in shapes],
        in_specs=[pl.BlockSpec(memory_space=pltpu.VMEM)] * 8,
        out_specs=[pl.BlockSpec(memory_space=pltpu.VMEM)] * 14,
        name="finish",
    )(out, gtok, eq, eo, eu, ed, fs, fb)


SEMS = 256
VMEM_LIMIT = 67043328


def per_device_fused(
    tokens_in, starts, ln1_gain, ln1_bias, w_qkv, b_qv, w_out, b_out,
    ln2_gain, ln2_bias, w_up, b_up, w_down, b_down, grad_out,
):
    rows, width = tokens_in.shape
    f32 = jnp.float32
    dp, z = lax.axis_index("dp"), lax.axis_index("tensor")
    part = width // 8
    dim = width // 16
    hidden = w_up.shape[1] // 4
    bit = ln1_gain.shape[0]
    here = jnp.arange(part) // bit == z
    vectors = jnp.stack([ln1_gain, ln1_bias, b_out, ln2_gain, ln2_bias, b_down])
    vectors = jnp.where(here, jnp.tile(vectors, (1, part // bit)), 0.0)
    begins = jnp.where(z == 0, starts.astype(f32), 0.0)
    begins = jnp.pad(begins, ((0, 1), (0, part - 4)))
    spot = (jnp.arange(8) == dp)[:, None]

    def spread(bias):
        entries = bias.astype(f32).reshape(4, -1, 1, bias.shape[1])
        return jnp.where(spot, entries, 0.0).reshape(4, -1, part)

    biases = jnp.concatenate(
        [spread(b_qv), spread(b_up), jnp.zeros((4, 5, part), f32)], axis=1
    )
    si = jnp.concatenate([jnp.concatenate([vectors, begins])[None], biases])
    in_q = w_qkv.reshape(part, 4, 3 * dim).transpose(1, 2, 0)
    in_o = w_out.reshape(4, dim, part)
    in_d = w_down.reshape(4, hidden, part)
    out, gtok, eq, eo, eu, ed, fs, fb = fused_layer(
        tokens_in, grad_out, in_q, in_o, w_up, in_d, si
    )
    out, gtok, grad_w_qkv, grad_w_out, grad_w_up, grad_w_down, *take = finish(
        out, gtok, eq, eo, eu, ed, fs, fb
    )
    grad_b_qv, grad_b_up = take[6].T, take[7].T
    return (
        out, gtok, take[0], take[1], grad_w_qkv, grad_b_qv, grad_w_out, take[2],
        take[3], take[4], grad_w_up, grad_b_up, grad_w_down, take[5],
    )


def solution(mesh):
    sizes = (mesh.shape["dp"], mesh.shape["tensor"])

    def layer(tokens_in, starts, *others):
        fits = sizes == (8, 4) and tokens_in.shape[0] == PIECE and starts.shape == (1, 4)
        return (per_device_fused if fits else per_device)(tokens_in, starts, *others)

    return jax.shard_map(
        layer,
        mesh=mesh,
        in_specs=(
            P(("dp", "tensor"), None),
            P("dp", None),
            P(("dp", "tensor")),
            P(("dp", "tensor")),
            P("dp", "tensor"),
            P("tensor", "dp"),
            P("tensor", "dp"),
            P(("dp", "tensor")),
            P(("dp", "tensor")),
            P(("dp", "tensor")),
            P("dp", "tensor"),
            P("tensor", "dp"),
            P("tensor", "dp"),
            P(("dp", "tensor")),
            P(("dp", "tensor"), None),
        ),
        out_specs=(
            P(("dp", "tensor"), None),
            P(("dp", "tensor"), None),
            P(("dp", "tensor")),
            P(("dp", "tensor")),
            P("dp", "tensor"),
            P("tensor", "dp"),
            P("tensor", "dp"),
            P(("dp", "tensor")),
            P(("dp", "tensor")),
            P(("dp", "tensor")),
            P("dp", "tensor"),
            P("tensor", "dp"),
            P("tensor", "dp"),
            P(("dp", "tensor")),
        ),
        check_vma=False,
    )
```

```python
import functools

import jax
import jax.numpy as jnp
from jax import lax
from jax.experimental import pallas as pl
from jax.experimental.pallas import tpu as pltpu
from jax.sharding import PartitionSpec as P

HD = 64
PIECE = 256
QBLOCK = 512


EPS = 1e-05
ROOT = 0.7978845608028654


def gelu_tanh(values):
    return 0.5 * values * (1.0 + jnp.tanh(ROOT * (values + 0.044715 * values * values * values)))


def normalize(values):
    center = jnp.mean(values, axis=-1, keepdims=True)
    shifted = values - center
    inverse = lax.rsqrt(jnp.mean(shifted * shifted, axis=-1, keepdims=True) + EPS)
    return (shifted * inverse, inverse)


def norm_back(grad_normed, normed, inverse, gain):
    scaled = grad_normed * gain
    return inverse * (
        scaled
        - jnp.mean(scaled, axis=-1, keepdims=True)
        - normed * jnp.mean(scaled * normed, axis=-1, keepdims=True)
    )


def dot_last(left, right):
    return lax.dot_general(
        left, right, (((1,), (1,)), ((), ())), preferred_element_type=jnp.float32
    )


def dot_first(left, right):
    return lax.dot_general(
        left, right, (((0,), (0,)), ((), ())), preferred_element_type=jnp.float32
    )


def gather_rows(values):
    return lax.all_gather(values, "tensor", axis=0, tiled=True)


def gather_grads(values):
    return lax.all_gather(values, "tensor", axis=0, tiled=True)


def reduce_rows(left, weight, rows):

    def term(start, count):
        return jnp.dot(left, weight, preferred_element_type=jnp.float32)

    return lax.psum_scatter(
        term(jnp.int32(0), lax.axis_size("tensor") * rows).astype(jnp.bfloat16),
        "tensor",
        scatter_dimension=0,
        tiled=True,
    ).astype(jnp.float32)


def reduce_grads(left, weight, rows):

    def term(start, count):
        return dot_last(left, weight)

    return lax.psum_scatter(
        term(jnp.int32(0), lax.axis_size("tensor") * rows).astype(jnp.bfloat16),
        "tensor",
        scatter_dimension=0,
        tiled=True,
    ).astype(jnp.float32)


def piece_ids(start_row, length):
    places = jnp.arange(length, dtype=jnp.int32)
    inside = (places[:, None] >= start_row[None, :]) & (
        places[:, None] < start_row[None, :] + PIECE
    )
    labels = jnp.arange(1, start_row.shape[0] + 1, dtype=jnp.int32)
    return jnp.sum(jnp.where(inside, labels[None, :], 0), axis=1)


def allowed_block(row_ids, row_places, key_ids, key_places):
    causal = key_places[None, :] <= row_places[:, None]
    picture = (row_ids[:, None] == key_ids[None, :]) & (row_ids[:, None] > 0)
    return causal | picture


def block_scores(by_seq, start_rows, block_index):
    length = by_seq.shape[1]
    per_seq = length // QBLOCK
    seq_index = block_index // per_seq
    first_row = block_index % per_seq * QBLOCK
    sequence = lax.dynamic_index_in_dim(by_seq, seq_index, 0, keepdims=False)
    key_ids = piece_ids(lax.dynamic_index_in_dim(start_rows, seq_index, 0, keepdims=False), length)
    query_rows = lax.dynamic_slice_in_dim(sequence, first_row, QBLOCK, 0)[:, :, 0]
    key_rows = sequence[:, :, 1]
    value_rows = sequence[:, :, 2]
    row_ids = lax.dynamic_slice_in_dim(key_ids, first_row, QBLOCK, 0)
    row_places = first_row + jnp.arange(QBLOCK, dtype=jnp.int32)
    scores = (
        jnp.einsum("qhd,khd->hqk", query_rows, key_rows, preferred_element_type=jnp.float32) * 0.125
    )
    places = jnp.arange(length, dtype=jnp.int32)
    scores = jnp.where(allowed_block(row_ids, row_places, key_ids, places)[None], scores, -1e30)
    return (seq_index, first_row, query_rows, key_rows, value_rows, scores)


def attention_forward(by_seq, start_rows):
    total_blocks = by_seq.shape[0] * (by_seq.shape[1] // QBLOCK)

    def attend(block_index):
        _, _, query_rows, key_rows, value_rows, scores = block_scores(
            by_seq, start_rows, block_index
        )
        peak = jnp.max(scores, axis=-1, keepdims=True)
        log_total = peak + jnp.log(jnp.sum(jnp.exp(scores - peak), axis=-1, keepdims=True))
        probs = jnp.exp(scores - log_total)
        heads = jnp.einsum(
            "hqk,khd->qhd",
            probs.astype(jnp.bfloat16),
            value_rows,
            preferred_element_type=jnp.float32,
        )
        return (heads.astype(jnp.bfloat16), log_total)

    return lax.map(attend, jnp.arange(total_blocks, dtype=jnp.int32))


def attention_backward(by_seq, start_rows, log_totals, grad_heads):
    total_blocks = by_seq.shape[0] * (by_seq.shape[1] // QBLOCK)
    empty = jnp.zeros(by_seq.shape[:3] + (HD,), jnp.float32)

    def step(carry, item):
        grad_keys, grad_values = carry
        block_index, log_total = item
        seq_index, first_row, query_rows, key_rows, value_rows, scores = block_scores(
            by_seq, start_rows, block_index
        )
        grad_seq = lax.dynamic_index_in_dim(grad_heads, seq_index, 0, keepdims=False)
        grad_rows = lax.dynamic_slice_in_dim(grad_seq, first_row, QBLOCK, 0)
        probs = jnp.exp(scores - log_total)
        grad_probs = jnp.einsum(
            "qhd,khd->hqk", grad_rows, value_rows, preferred_element_type=jnp.float32
        )
        inner = jnp.sum(probs * grad_probs, axis=-1, keepdims=True)
        grad_scores = (probs * (grad_probs - inner)).astype(jnp.bfloat16)
        grad_query = (
            jnp.einsum("hqk,khd->qhd", grad_scores, key_rows, preferred_element_type=jnp.float32)
            * 0.125
        )
        key_term = (
            jnp.einsum("hqk,qhd->khd", grad_scores, query_rows, preferred_element_type=jnp.float32)
            * 0.125
        )
        value_term = jnp.einsum(
            "hqk,qhd->khd",
            probs.astype(jnp.bfloat16),
            grad_rows,
            preferred_element_type=jnp.float32,
        )
        grad_keys = lax.dynamic_update_index_in_dim(
            grad_keys,
            lax.dynamic_index_in_dim(grad_keys, seq_index, 0, keepdims=False) + key_term,
            seq_index,
            0,
        )
        grad_values = lax.dynamic_update_index_in_dim(
            grad_values,
            lax.dynamic_index_in_dim(grad_values, seq_index, 0, keepdims=False) + value_term,
            seq_index,
            0,
        )
        return ((grad_keys, grad_values), grad_query)

    (grad_keys, grad_values), grad_query = lax.scan(
        step, (empty, empty), (jnp.arange(total_blocks, dtype=jnp.int32), log_totals)
    )
    return (grad_query, grad_keys, grad_values)


def per_device(
    tokens_in,
    starts,
    ln1_gain,
    ln1_bias,
    w_qkv,
    b_qv,
    w_out,
    b_out,
    ln2_gain,
    ln2_bias,
    w_up,
    b_up,
    w_down,
    b_down,
    grad_out,
):
    rows = tokens_in.shape[0]
    gain_one, shift_one, bias_out, gain_two, shift_two, bias_down = (
        lax.all_gather(ln1_gain, ("dp", "tensor"), axis=0, tiled=True),
        lax.all_gather(ln1_bias, ("dp", "tensor"), axis=0, tiled=True),
        lax.all_gather(b_out, ("dp", "tensor"), axis=0, tiled=True),
        lax.all_gather(ln2_gain, ("dp", "tensor"), axis=0, tiled=True),
        lax.all_gather(ln2_bias, ("dp", "tensor"), axis=0, tiled=True),
        lax.all_gather(b_down, ("dp", "tensor"), axis=0, tiled=True),
    )
    weight_qkv, bias_qv, weight_out = (
        lax.all_gather(w_qkv, "dp", axis=0, tiled=True),
        lax.all_gather(b_qv, "dp", axis=1, tiled=True),
        lax.all_gather(w_out, "dp", axis=1, tiled=True),
    )
    weight_up, bias_up, weight_down = (
        lax.all_gather(w_up, "dp", axis=0, tiled=True),
        lax.all_gather(b_up, "dp", axis=1, tiled=True),
        lax.all_gather(w_down, "dp", axis=1, tiled=True),
    )
    local_heads = weight_qkv.shape[1] // (3 * HD)
    seq_count = starts.shape[0]
    inputs = tokens_in.astype(jnp.float32)
    normed_one, inverse_one = normalize(inputs)
    gathered_one = gather_rows((normed_one * gain_one + shift_one).astype(jnp.bfloat16))
    group = gathered_one.shape[0]
    length = group // seq_count
    bias_pair = bias_qv.astype(jnp.float32).reshape(local_heads, 2, HD)
    full_bias = jnp.stack(
        [bias_pair[:, 0], jnp.zeros_like(bias_pair[:, 0]), bias_pair[:, 1]], axis=1
    )
    projected = (
        jnp.dot(gathered_one, weight_qkv, preferred_element_type=jnp.float32).reshape(
            group, local_heads, 3, HD
        )
        + full_bias
    ).astype(jnp.bfloat16)
    by_seq = projected.reshape(seq_count, length, local_heads, 3, HD)
    heads_blocks, log_totals = attention_forward(by_seq, starts)
    heads_out = heads_blocks.reshape(group, local_heads * HD)
    middle = inputs + (reduce_rows(heads_out, weight_out, rows) + bias_out)
    normed_two, inverse_two = normalize(middle)
    rounded_two = (normed_two * gain_two + shift_two).astype(jnp.bfloat16)
    grad_final = grad_out.astype(jnp.float32)
    grad_bias_down = jnp.sum(grad_final, axis=0)
    gathered_two = gather_rows(rounded_two)
    up_proj = jnp.dot(gathered_two, weight_up, preferred_element_type=jnp.float32) + bias_up.astype(
        jnp.float32
    ).reshape(-1)
    hidden_act, gelu_pull = jax.vjp(gelu_tanh, up_proj)
    hidden_low = hidden_act.astype(jnp.bfloat16)
    output = (middle + reduce_rows(hidden_low, weight_down, rows) + bias_down).astype(jnp.bfloat16)
    grad_branch = gather_grads(grad_out)
    grad_w_down = dot_first(hidden_low, grad_branch)
    grad_up = gelu_pull(dot_last(grad_branch, weight_down))[0].astype(jnp.bfloat16)
    grad_b_up = jnp.sum(grad_up, axis=0, dtype=jnp.float32).reshape(bias_up.shape)
    grad_w_up = dot_first(gathered_two, grad_up)
    grad_two = reduce_grads(grad_up, weight_up, rows)
    grad_w_up, grad_b_up, grad_w_down = (
        lax.psum_scatter(
            grad_w_up.astype(jnp.bfloat16), "dp", scatter_dimension=0, tiled=True
        ).astype(jnp.float32),
        lax.psum_scatter(
            grad_b_up.astype(jnp.bfloat16), "dp", scatter_dimension=1, tiled=True
        ).astype(jnp.float32),
        lax.psum_scatter(
            grad_w_down.astype(jnp.bfloat16), "dp", scatter_dimension=1, tiled=True
        ).astype(jnp.float32),
    )
    grad_gain_two = jnp.sum(grad_two * normed_two, axis=0)
    grad_shift_two = jnp.sum(grad_two, axis=0)
    grad_middle = grad_final + norm_back(grad_two, normed_two, inverse_two, gain_two)
    grad_bias_out = jnp.sum(grad_middle, axis=0)
    grad_attn = gather_grads(grad_middle.astype(jnp.bfloat16))
    grad_w_out = dot_first(heads_out, grad_attn)
    grad_heads = (
        dot_last(grad_attn, weight_out)
        .astype(jnp.bfloat16)
        .reshape(seq_count, length, local_heads, HD)
    )
    grad_query, grad_keys, grad_values = attention_backward(by_seq, starts, log_totals, grad_heads)
    grad_proj = jnp.stack(
        [
            grad_query.reshape(group, local_heads, HD),
            grad_keys.reshape(group, local_heads, HD),
            grad_values.reshape(group, local_heads, HD),
        ],
        axis=2,
    ).astype(jnp.bfloat16)
    grad_b_qv = jnp.sum(grad_proj[:, :, 0::2], axis=0, dtype=jnp.float32).reshape(bias_qv.shape)
    grad_flat = grad_proj.reshape(group, 3 * local_heads * HD)
    grad_w_qkv = dot_first(gathered_one, grad_flat)
    grad_one = reduce_grads(grad_flat, weight_qkv, rows)
    grad_w_qkv, grad_b_qv, grad_w_out = (
        lax.psum_scatter(
            grad_w_qkv.astype(jnp.bfloat16), "dp", scatter_dimension=0, tiled=True
        ).astype(jnp.float32),
        lax.psum_scatter(
            grad_b_qv.astype(jnp.bfloat16), "dp", scatter_dimension=1, tiled=True
        ).astype(jnp.float32),
        lax.psum_scatter(
            grad_w_out.astype(jnp.bfloat16), "dp", scatter_dimension=1, tiled=True
        ).astype(jnp.float32),
    )
    grad_gain_one = jnp.sum(grad_one * normed_one, axis=0)
    grad_shift_one = jnp.sum(grad_one, axis=0)
    grad_tokens = (grad_middle + norm_back(grad_one, normed_one, inverse_one, gain_one)).astype(
        jnp.bfloat16
    )
    summed = (
        lax.psum_scatter(grad_gain_one, ("dp", "tensor"), scatter_dimension=0, tiled=True),
        lax.psum_scatter(grad_shift_one, ("dp", "tensor"), scatter_dimension=0, tiled=True),
        lax.psum_scatter(grad_bias_out, ("dp", "tensor"), scatter_dimension=0, tiled=True),
        lax.psum_scatter(grad_gain_two, ("dp", "tensor"), scatter_dimension=0, tiled=True),
        lax.psum_scatter(grad_shift_two, ("dp", "tensor"), scatter_dimension=0, tiled=True),
        lax.psum_scatter(grad_bias_down, ("dp", "tensor"), scatter_dimension=0, tiled=True),
    )
    return (
        output,
        grad_tokens,
        summed[0],
        summed[1],
        grad_w_qkv,
        grad_b_qv,
        grad_w_out,
        summed[2],
        summed[3],
        summed[4],
        grad_w_up,
        grad_b_up,
        grad_w_down,
        summed[5],
    )


MESH = pl.DeviceIdType.MESH
CH = 2
HOPS = 4
RELAYED = "qud"


class Fused:
    def __init__(self, names, refs):
        for name, ref in zip(names, refs):
            setattr(self, name, ref)
        self.next_sem = 0
        self.unsent = []
        self.groups = {0: [], 1: []}
        self.unsent_later = []
        dp, self.z = lax.axis_index("dp"), lax.axis_index("tensor")
        self.y, self.x, self.c = dp // 4, (dp // 2) % 2, dp % 2
        self.j = self.member(self.x, self.c)
        self.q = self.quarter(self.j)
        self.sib = self.dev(self.y, self.x, 1 - self.c, self.z)
        self.across = self.dev(self.y, 1 - self.x, self.c, self.z)
        self.q_sib = self.quarter(self.member(self.x, 1 - self.c))
        self.q_x = self.quarter(self.member(1 - self.x, self.c))
        self.q_d = self.quarter(self.member(1 - self.x, 1 - self.c))
        self.rows = self.tok.shape[0]
        self.width = self.tok.shape[1]
        self.part = self.width // 8

    def dev(self, y, x, c, z):
        return ((y * 2 + x) * 2 + c, z)

    def member(self, x, c):
        return 2 * c + x

    def local(self, member):
        return 2 * (member % 2) + member // 2

    def mate(self, member):
        return self.dev(self.y, member % 2, member // 2, self.z)

    def quarter(self, member):
        return (member - self.z - self.y + 8) % 4

    def sem(self, count=1):
        index = self.next_sem
        self.next_sem += count
        return index

    def copy(self, src, dst, device, index, sent=None):
        return pltpu.make_async_remote_copy(
            src_ref=src,
            dst_ref=dst,
            send_sem=self.ssem.at[index if sent is None else sent],
            recv_sem=self.rsem.at[index],
            device_id=device,
            device_id_type=MESH,
        )

    def send(self, src, dst, device, index, group=None):
        copy = self.copy(src, dst, device, index)
        copy.start()
        (self.unsent if group is None else self.groups[group]).append(copy)

    def later(self, view, sent, when=None):
        self.unsent_later.append((view, sent, when))

    def arrived(self, dst, index):
        self.copy(dst, dst, self.sib, index).wait_recv()

    def drain(self):
        for copy in self.unsent + self.groups[0] + self.groups[1]:
            copy.wait_send()
        for view, sent, when in self.unsent_later:
            copy = self.copy(view(), view(), self.sib, sent)
            if when is None:
                copy.wait_send()
            else:
                pl.when(when())(copy.wait_send)

    def at_quarter(self, quarter, chunk=None):
        if chunk is None:
            return pl.ds(pl.multiple_of(quarter * self.rows, self.rows), self.rows)
        size = self.rows // CH
        return pl.ds(pl.multiple_of(quarter * self.rows + chunk * size, size), size)

    def at_chunk(self, chunk):
        size = self.rows // CH
        return pl.ds(chunk * size, size)

    def barrier(self):
        me = lax.axis_index("dp") * 4 + self.z
        bar = pltpu.get_barrier_semaphore()

        def greet(step, carry):
            other = (me + step) % 32
            pl.semaphore_signal(
                bar, inc=1, device_id=(other // 4, other % 4), device_id_type=MESH
            )
            return carry

        lax.fori_loop(1, 32, greet, 0)
        pl.semaphore_wait(bar, 31)

    def homes(self):
        plane = 2 * self.y + self.x
        member = (plane + self.z + self.c) % 4
        worker = (self.c, member % 2, member // 2, plane)
        owner = (self.z // 2, self.z % 2, self.y, self.q)
        same = (
            (worker[0] == self.y)
            & (worker[1] == self.x)
            & (worker[2] == self.c)
            & (worker[3] == self.z)
        )
        return self.dev(*worker), self.dev(*owner), same

    def move_start(self, src, dst, outward, index):
        worker, owner, same = self.homes()
        copy = self.copy(src, dst, worker if outward else owner, index)
        local = pltpu.make_async_copy(src, dst, self.lsem.at[index])

        @pl.when(jnp.logical_not(same))
        def _():
            copy.start()

        @pl.when(same)
        def _():
            local.start()

    def move_wait(self, src, dst, index):
        same = self.homes()[2]
        copy = self.copy(src, dst, self.sib, index)
        local = pltpu.make_async_copy(src, dst, self.lsem.at[index])

        @pl.when(jnp.logical_not(same))
        def _():
            copy.wait_send()
            copy.wait_recv()

        @pl.when(same)
        def _():
            local.wait()

    def hop_rows(self, chunk):
        size = self.rows // HOPS
        return pl.ds(chunk * size, size)

    def hop_one(self, src, mid, index):
        plane = 2 * self.y + self.x
        member = (plane + self.z + self.c) % 4
        first = self.dev(self.c, member % 2, member // 2, self.z)
        same = (self.c == self.y) & (member % 2 == self.x) & (member // 2 == self.c)
        for chunk in range(HOPS):
            view, there = src.at[self.hop_rows(chunk)], mid.at[self.hop_rows(chunk)]
            copy = self.copy(view, there, first, index + chunk)
            local = pltpu.make_async_copy(view, there, self.lsem.at[index + chunk])
            pl.when(jnp.logical_not(same))(copy.start)
            pl.when(same)(local.start)

    def hop_two(self, src, mid, dst, place, index, onward):
        plane = self.q
        member = (2 * self.y + self.x + self.z + self.c) % 4
        home = (self.c == self.y) & (member % 2 == self.x) & (member // 2 == self.c)
        stay = plane == self.z
        for chunk in range(HOPS):
            rows = self.hop_rows(chunk)
            size = self.rows // HOPS
            there = dst.at[pl.ds(pl.multiple_of(place + chunk * size, size), size)]
            first = self.copy(src.at[rows], mid.at[rows], self.sib, index + chunk)
            local = pltpu.make_async_copy(src.at[rows], mid.at[rows], self.lsem.at[index + chunk])
            pl.when(jnp.logical_not(home))(first.wait_send)
            pl.when(jnp.logical_not(home))(first.wait_recv)
            pl.when(home)(local.wait)
            copy = self.copy(
                mid.at[rows], there, self.dev(self.y, self.x, self.c, plane), onward + chunk
            )
            keep = pltpu.make_async_copy(mid.at[rows], there, self.lsem.at[onward + chunk])
            pl.when(jnp.logical_not(stay))(copy.start)
            pl.when(stay)(keep.start)

    def hop_wait(self, mid, dst, place, onward, half):
        plane = self.q
        stay = plane == self.z
        for chunk in range(half * HOPS // CH, (half + 1) * HOPS // CH):
            rows = self.hop_rows(chunk)
            size = self.rows // HOPS
            there = dst.at[pl.ds(pl.multiple_of(place + chunk * size, size), size)]
            copy = self.copy(mid.at[rows], there, self.sib, onward + chunk)
            keep = pltpu.make_async_copy(mid.at[rows], there, self.lsem.at[onward + chunk])
            pl.when(jnp.logical_not(stay))(copy.wait_send)
            pl.when(jnp.logical_not(stay))(copy.wait_recv)
            pl.when(stay)(keep.wait)

    def span(self, half):
        return pl.ds(pl.multiple_of(half * 4 * self.part, 4 * self.part), 4 * self.part)

    def place(self, source):
        return pl.ds(pl.multiple_of(source * self.part, self.part), self.part)

    def cut(self, kind, ref, zc, where):
        if kind == "u":
            return ref.at[zc, where, :]
        return ref.at[zc, :, where]

    def piece(self, kind, ref, member):
        if kind == "u":
            wide = self.wbuf["u"].shape[2]
            return ref.at[:, pl.ds(pl.multiple_of(member * wide, wide), wide)]
        return ref.at[member]

    def weights_one(self, kind):
        source = 4 * self.y + self.local(self.j)
        here = self.cut(kind, self.wbuf[kind], self.z, self.place(source))
        self.one[kind] = []
        for step in range(1, 4):
            member = (self.j + step) % 4
            index = self.sem()
            self.send(
                self.piece(kind, self.shard[kind], member), here, self.mate(member), index
            )
            sender = 4 * self.y + self.local((self.j - step + 4) % 4)
            self.one[kind].append(
                (self.cut(kind, self.wbuf[kind], self.z, self.place(sender)), index)
            )
        index = self.sem()
        local = pltpu.make_async_copy(
            self.piece(kind, self.shard[kind], self.j), here, self.lsem.at[index]
        )
        local.start()
        self.own[kind] = local
        self.two[kind] = self.sem(4)
        self.three[kind] = self.sem(4)
        self.pass_sem[kind] = self.sem()

    def weights_in(self, kind):
        self.own[kind].wait()
        for view, index in self.one[kind]:
            self.arrived(view, index)
        self.weights_cross(kind, 0)

    def mine(self, kind, plane):
        return self.cut(kind, self.wbuf[kind], plane, self.span(self.y))

    def weights_two(self, kind):
        here = self.mine(kind, self.z)
        near, far = (lambda: self.z != 3), (lambda: self.z != 0)
        if kind not in RELAYED:
            near = far = None
        for step, when in ((2, None), (1, near), (3, far)):
            plane = (self.z + step) % 4
            index = self.two[kind] + step
            copy = self.copy(here, here, self.dev(self.y, self.x, self.c, plane), index)
            if when is None:
                copy.start()
            else:
                pl.when(when())(copy.start)
            self.later(lambda: self.mine(kind, self.z), index, when)

    def weights_relay(self, kind, guard=None):
        if kind not in RELAYED:
            return
        for here, plane, step in ((2, 3, 3), (1, 0, 1)):
            when = self.z == here
            block = self.mine(kind, (here + 2) % 4)
            copy = self.copy(
                block,
                block,
                self.dev(self.y, self.x, self.c, plane),
                self.two[kind] + step,
                self.pass_sem[kind],
            )
            pl.when(when if guard is None else when & guard)(copy.start)

    def relayed(self, kind):
        if kind in RELAYED:
            self.later(
                lambda: self.mine(kind, self.z),
                self.pass_sem[kind],
                lambda: (self.z == 1) | (self.z == 2),
            )
        for step in range(4):
            self.later(lambda: self.mine(kind, self.z), self.three[kind] + step)

    def weights_cross(self, kind, step):
        mine = self.mine(kind, (self.z - step + 4) % 4)
        self.copy(
            mine,
            mine,
            self.dev(1 - self.y, self.x, self.c, self.z),
            self.three[kind] + step,
        ).start()

    def weights_here(self, kind, step):
        self.arrived(self.mine(kind, (self.z - step + 4) % 4), self.two[kind] + step)

    def weights_three(self, kind, steps=(1, 3)):
        for step in steps:
            self.weights_here(kind, step)
            self.weights_cross(kind, step)

    def weights_start_three(self, kind):
        self.weights_here(kind, 2)
        self.weights_relay(kind)
        self.weights_cross(kind, 2)

    def weights_ready(self, kind, step):
        plane = (self.z - step + 4) % 4
        self.arrived(
            self.cut(kind, self.wbuf[kind], plane, self.span(1 - self.y)),
            self.three[kind] + step,
        )

    def weights_done(self, kind):
        for step in range(4):
            self.weights_ready(kind, step)

    def grads_one(self, kind):
        self.swaps[kind] = [self.sem() for _ in range(3)]
        for swap in self.swaps[kind]:
            self.later(lambda: self.zbuf[kind].at[0], swap)
        for turn in (2, 1, 3, 0):
            plane = (self.z + turn) % 4
            away = self.cut(kind, self.dbuf[kind], plane, self.span(1 - self.y))
            there = self.cut(kind, self.ybuf[kind], plane, slice(None))
            use = self.sem()
            self.send(away, there, self.dev(1 - self.y, self.x, self.c, self.z), use)
            self.backs.setdefault(kind, {})[turn] = use

    def grads_two(self, kind, turns=(2, 1, 3, 0)):
        for turn in turns:
            plane = (self.z + turn) % 4
            there = self.cut(kind, self.ybuf[kind], plane, slice(None))
            self.arrived(there, self.backs[kind][turn])
            mine = self.cut(kind, self.dbuf[kind], plane, self.span(self.y))
            mine[...] = (
                mine[...].astype(jnp.float32) + there[...].astype(jnp.float32)
            ).astype(jnp.bfloat16)
            if turn:
                self.copy(
                    mine,
                    self.zbuf[kind].at[turn - 1],
                    self.dev(self.y, self.x, self.c, plane),
                    self.swaps[kind][turn - 1],
                ).start()

    def head_one(self, step, head):
        self.copy(
            self.cut("q", self.dq, head, self.span(1 - self.y)),
            self.cut("q", self.yq, head, slice(None)),
            self.dev(1 - self.y, self.x, self.c, self.z),
            self.head_y + step,
        ).start()

    def head_add(self, step, head):
        there = self.cut("q", self.yq, head, slice(None))
        self.arrived(there, self.head_y + step)
        mine = self.cut("q", self.dq, head, self.span(self.y))
        mine[...] = (mine[...].astype(jnp.float32) + there[...].astype(jnp.float32)).astype(
            jnp.bfloat16
        )

    def head_two(self, step, head):
        self.copy(
            self.cut("q", self.dq, head, self.span(self.y)),
            self.zq.at[step],
            self.dev(self.y, self.x, self.c, head),
            self.head_z + step,
        ).start()

    def grads_three(self, kind):
        mine = self.cut(kind, self.dbuf[kind], self.z, self.span(self.y))
        total = mine[...].astype(jnp.float32)
        for step in range(1, 4):
            there = self.zbuf[kind].at[step - 1]
            self.arrived(there, self.swaps[kind][step - 1])
            total = total + there[...].astype(jnp.float32)
        final = self.fbuf[kind]
        final[...] = total.astype(jnp.bfloat16)
        ends = self.ebuf[kind]
        self.last[kind] = []
        for step in range(1, 4):
            member = (self.j + step) % 4
            index = self.sem()
            self.send(
                self.slab(kind, final, self.local(member)),
                ends.at[self.j],
                self.mate(member),
                index,
            )
            self.last[kind].append(((self.j - step + 4) % 4, index))
        index = self.sem()
        local = pltpu.make_async_copy(
            self.slab(kind, final, self.local(self.j)), ends.at[self.j], self.lsem.at[index]
        )
        local.start()
        self.own[kind] = local

    def slab(self, kind, ref, member):
        where = pl.ds(pl.multiple_of(member * self.part, self.part), self.part)
        if kind == "u":
            return ref.at[where, :]
        return ref.at[:, where]

    def grads_done(self, kind):
        self.own[kind].wait()
        for member, index in self.last[kind]:
            self.arrived(self.ebuf[kind].at[member], index)

    def small_one(self):
        self.sma[self.z] = self.si[...]
        self.small_sem = [self.sem() for _ in range(3)]
        for step in range(1, 4):
            plane = (self.z + step) % 4
            self.send(
                self.si,
                self.sma.at[self.z],
                self.dev(self.y, self.x, self.c, plane),
                self.small_sem[step - 1],
            )

    def around(self, step):
        return (lax.axis_index("dp") + step + 8) % 8

    def small_two(self):
        for step in range(1, 4):
            self.arrived(self.sma.at[(self.z - step + 4) % 4], self.small_sem[step - 1])
        me = self.around(0)
        self.lb[me] = sum(self.sma[plane, 0] for plane in range(4))
        self.bb[me] = self.sma[:, 1 + self.j]
        self.plane_sem = [(self.sem(), self.sem()) for _ in range(7)]
        for step in range(1, 8):
            other = self.around(step)
            member = self.member((other // 2) % 2, other % 2)
            first, second = self.plane_sem[step - 1]
            self.send(self.lb.at[me], self.lb.at[me], (other, self.z), first)
            self.send(self.sma.at[:, 1 + member], self.bb.at[me], (other, self.z), second)

    def small_three(self):
        for step in range(1, 8):
            other = self.around(-step)
            first, second = self.plane_sem[step - 1]
            self.arrived(self.lb.at[other], first)
            self.arrived(self.bb.at[other], second)
        part, dim = self.part, self.qh.shape[2]
        for source in range(8):
            self.small[:, source * part : (source + 1) * part] = self.lb[source]
        bias = sum(self.bb[source] for source in range(8))
        for head in range(4):
            row = bias[head, 0:1]
            self.bq[head, :, 0:dim] = row[:, 0:dim]
            self.bq[head, :, dim : 2 * dim] = jnp.zeros((1, dim), jnp.float32)
            self.bq[head, :, 2 * dim :] = row[:, dim:]
            for half in range(2):
                place = (2 * head + half) * part
                self.bu[:, place : place + part] = bias[head, 1 + half : 2 + half]

    def back_one(self):
        part, me = self.part, self.around(0)
        for target in range(8):
            self.cs[target] = self.sums[:, target * part : (target + 1) * part]
        self.cr[me] = self.cs[me]
        self.cd[me] = self.cb[...]
        self.back_sem = [(self.sem(), self.sem()) for _ in range(7)]
        for step in range(1, 8):
            other = self.around(step)
            first, second = self.back_sem[step - 1]
            self.send(self.cs.at[other], self.cr.at[me], (other, self.z), first)
            self.send(self.cb, self.cd.at[me], (other, self.z), second)

    def back_two(self):
        for step in range(1, 8):
            other = self.around(-step)
            first, second = self.back_sem[step - 1]
            self.arrived(self.cr.at[other], first)
            self.arrived(self.cd.at[other], second)
        self.es[self.z] = sum(self.cr[source] for source in range(8))
        for member in range(4):
            pair = [2 * (member % 2) + member // 2, 4 + 2 * (member % 2) + member // 2]
            self.ed_small[:, member] = self.cd[pair[0]] + self.cd[pair[1]]
        self.eb[self.z] = self.ed_small[self.z]
        self.line_sem = [(self.sem(), self.sem()) for _ in range(3)]
        for step in range(1, 4):
            plane = (self.z + step) % 4
            device = self.dev(self.y, self.x, self.c, plane)
            first, second = self.line_sem[step - 1]
            self.send(self.es.at[self.z], self.es.at[self.z], device, first)
            self.send(self.ed_small.at[plane], self.eb.at[self.z], device, second)

    def back_three(self):
        for step in range(1, 4):
            plane = (self.z - step + 4) % 4
            first, second = self.line_sem[step - 1]
            self.arrived(self.es.at[plane], first)
            self.arrived(self.eb.at[plane], second)
        self.fs[...] = sum(self.es[plane] for plane in range(4))
        self.fb[...] = sum(self.eb[plane] for plane in range(4))

    def gather_plan(self):
        return {kind: [self.sem() for _ in range(CH)] for kind in ("across", "sib", "pass")}

    def gather_send(self, buf, plan, chunk):
        rows = self.at_quarter(self.q, chunk)
        for device, kind in ((self.across, "across"), (self.sib, "sib")):
            self.copy(buf.at[rows], buf.at[rows], device, plan[kind][chunk]).start()
            self.later(lambda: buf.at[self.at_quarter(self.q, 0)], plan[kind][chunk])

    def gather_pass(self, buf, plan):
        for chunk in range(CH):
            rows = self.at_quarter(self.q_x, chunk)
            self.arrived(buf.at[rows], plan["across"][chunk])
            self.send(buf.at[rows], buf.at[rows], self.sib, plan["pass"][chunk])

    def gather_sib(self, buf, plan):
        for chunk in range(CH):
            self.arrived(buf.at[self.at_quarter(self.q_sib, chunk)], plan["sib"][chunk])

    def gather_last(self, buf, plan):
        for chunk in range(CH):
            self.arrived(buf.at[self.at_quarter(self.q_d, chunk)], plan["pass"][chunk])

    def gathered(self, buf, plan, use):
        use(self.q)
        self.gather_sib(buf, plan)
        use(self.q_sib)
        self.gather_pass(buf, plan)
        use(self.q_x)
        self.gather_last(buf, plan)
        use(self.q_d)

    def scatter_start(self, partial, own, which, rx, hold=False):
        sa, ra, sb, sc, rb = (self.rs.at[which, slot] for slot in range(5))
        plan = [[self.sem() for _ in range(CH)] for _ in range(3)]
        low = jnp.bfloat16
        for copy in self.groups[which]:
            copy.wait_send()
        self.groups[which] = []
        sa[...] = partial(self.q_d).astype(low)
        for chunk in range(CH):
            rows = self.at_chunk(chunk)
            self.send(sa.at[rows], ra.at[rows], self.sib, plan[0][chunk], which)
        held = partial(self.q_x)
        for chunk in range(CH):
            self.arrived(ra.at[self.at_chunk(chunk)], plan[0][chunk])
        sb[...] = (held + ra[...].astype(jnp.float32)).astype(low)
        if not hold:
            self.scatter_send((plan, which, rx))
        sc[...] = partial(self.q_sib).astype(low)
        for chunk in range(CH):
            rows = self.at_chunk(chunk)
            self.send(sc.at[rows], rb.at[rows], self.sib, plan[2][chunk], which)
        own[...] = partial(self.q)
        return plan, which, rx

    def scatter_send(self, started):
        plan, which, rx = started
        sb = self.rs.at[which, 2]
        for chunk in range(CH):
            rows = self.at_chunk(chunk)
            self.send(sb.at[rows], rx.at[rows], self.across, plan[1][chunk], which)

    def scatter_chunk(self, started, own, chunk):
        plan, which, rx = started
        rows = self.at_chunk(chunk)
        rb = self.rs.at[which, 4]
        self.arrived(rb.at[rows], plan[2][chunk])
        self.arrived(rx.at[rows], plan[1][chunk])
        return (
            own[rows, :] + rb[rows, :].astype(jnp.float32) + rx[rows, :].astype(jnp.float32)
        )

    def run(self):
        f32, low = jnp.float32, jnp.bfloat16
        rows, width = self.rows, self.width
        quarters = range(4)
        self.wbuf = dict(q=self.wq, o=self.wo, u=self.wu, d=self.wd)
        self.shard = dict(q=self.in_q, o=self.in_o, u=self.in_u, d=self.in_d)
        self.dbuf = dict(q=self.dq, o=self.do, u=self.du, d=self.dd)
        self.ybuf = dict(q=self.yq, o=self.yo, u=self.yu, d=self.yd)
        self.zbuf = dict(q=self.zq, o=self.zo, u=self.zu, d=self.zd)
        self.fbuf = dict(q=self.fq, o=self.fo, u=self.fu, d=self.fd)
        self.ebuf = dict(q=self.eq, o=self.eo, u=self.eu, d=self.ed)
        self.one, self.two, self.three, self.own = {}, {}, {}, {}
        self.back, self.backs, self.swaps, self.last = {}, {}, {}, {}
        self.pass_sem = {}
        heads, dim = self.qh.shape[0], self.qh.shape[2]
        hidden = self.wu.shape[2]

        self.barrier()
        move = [self.sem() for _ in range(4)]
        self.small_one()
        hop = [self.sem(HOPS) for _ in range(4)]
        self.hop_one(self.tok, self.mid_x, hop[0])
        self.hop_one(self.go, self.ox, hop[2])
        self.weights_one("q")
        plan_one, plan_two, plan_go, plan_mid = (self.gather_plan() for _ in range(4))
        self.hop_two(self.tok, self.mid_x, self.xs, 0, hop[0], hop[1])
        self.small_two()
        own_rows = self.at_quarter(self.q)
        self.weights_in("q")
        self.weights_two("q")
        for kind in "ou":
            self.weights_one(kind)
        self.small_three()
        gain_one, shift_one = self.small[0:1, :], self.small[1:2, :]
        bias_out = self.small[2:3, :]
        gain_two, shift_two = self.small[3:4, :], self.small[4:5, :]
        bias_down = self.small[5:6, :]

        for chunk in range(CH):
            part = self.at_chunk(chunk)
            self.hop_wait(self.mid_x, self.xs, 0, hop[1], chunk)
            normed, inverse = normalize(self.xs[part, :].astype(f32))
            self.n1[part, :] = normed
            self.i1[part, :] = inverse
            self.h1[self.at_quarter(self.q, chunk), :] = (normed * gain_one + shift_one).astype(low)
            self.gather_send(self.h1, plan_one, chunk)
        self.mask_blocks()
        near = 1 + 2 * ((3 - self.z) // 3)
        self.gather_sib(self.h1, plan_one)
        self.weights_start_three("q")
        self.weights_in("o")
        self.weights_two("o")
        self.hop_two(self.go, self.ox, self.gg, self.z * rows, hop[2], hop[3])
        self.gather_pass(self.h1, plan_one)
        self.weights_one("d")
        self.weights_three("q", (near,))
        self.gather_last(self.h1, plan_one)

        def parts_of(block):
            return ([(0, block * rows)] if block else []) + [(block * rows, rows)]

        def turn(step):
            late, odd = step // 2, step % 2
            return (1 - late) * 2 * odd + late * (near + odd * (4 - 2 * near))

        def attend(step, carry):
            back = turn(step)
            head = (self.z - back + 4) % 4
            self.weights_ready("q", back)

            def project(block, carry):
                place = pl.ds(pl.multiple_of(block * rows, rows), rows)
                both = dot_last(self.h1[place, :], self.wq[head]) + self.bq[head]
                for slot, ref in enumerate((self.qh, self.kh, self.vh)):
                    value = both[:, slot * dim : (slot + 1) * dim].astype(low)
                    if slot == 0:
                        value = (value.astype(f32) * 0.125).astype(low)
                    ref[head, place, :] = value
                return carry

            lax.fori_loop(0, 4, project, 0)

            @pl.when(step == 0)
            def _():
                self.weights_three("q", (4 - near,))
                self.weights_in("u")
                self.weights_two("u")

            @pl.when(step == 1)
            def _():
                self.weights_start_three("o")

            @pl.when(step == 2)
            def _():
                self.weights_three("o")
                for chunk in range(CH):
                    self.hop_wait(self.ox, self.gg, self.q * rows, hop[3], chunk)
                    self.gather_send(self.gg, plan_go, chunk)

            @pl.when(step == 3)
            def _():
                self.weights_start_three("u")

            for block in quarters:
                place = pl.ds(block * rows, rows)
                query = self.qh[head, place, :]
                scores = []
                for first, count in parts_of(block):
                    value = dot_last(query, self.kh[head, pl.ds(first, count), :])
                    if first == block * rows:
                        value = value + self.mk[block].astype(f32)
                    scores.append(value)
                peak = functools.reduce(
                    jnp.maximum, [jnp.max(value, axis=1, keepdims=True) for value in scores]
                )
                powers = [jnp.exp(value - peak) for value in scores]
                total = sum(jnp.sum(value, axis=1, keepdims=True) for value in powers)
                scale = 1.0 / total
                result = 0.0
                for (first, count), value in zip(parts_of(block), powers):
                    probs = (value * scale).astype(low)
                    self.pb[block][head, :, pl.ds(first, count)] = probs
                    result = result + jnp.dot(
                        probs,
                        self.vh[head, pl.ds(first, count), :],
                        preferred_element_type=f32,
                    )
                self.hh[head, place, :] = result.astype(low)
            return carry

        lax.fori_loop(0, heads, attend, 0)
        for kind in "qou":
            self.relayed(kind)

        def assemble(target, refs, count):
            def one(block, carry):
                place = pl.ds(pl.multiple_of(block * rows, rows), rows)
                pieces = [ref[head, place, :] for ref in refs for head in range(count)]
                target[place, :] = jnp.concatenate(pieces, axis=1)
                return carry

            lax.fori_loop(0, 4, one, 0)

        assemble(self.ho, (self.hh,), heads)
        self.weights_done("o")

        flat_out = lambda: self.wo[...].reshape(heads * dim, width)
        started = self.scatter_start(
            lambda quarter: jnp.dot(
                self.ho[self.at_quarter(quarter), :], flat_out(), preferred_element_type=f32
            ),
            self.own_a,
            0,
            self.rx.at[0],
        )
        self.weights_in("d")
        self.weights_two("d")
        self.weights_three("u")
        for chunk in range(CH):
            part = self.at_chunk(chunk)
            summed = self.scatter_chunk(started, self.own_a, chunk)
            middle = self.xs[part, :].astype(f32) + (summed + bias_out)
            self.mid[part, :] = middle
            normed, inverse = normalize(middle)
            self.n2[part, :] = normed
            self.i2[part, :] = inverse
            self.h2[self.at_quarter(self.q, chunk), :] = (normed * gain_two + shift_two).astype(low)
            self.gather_send(self.h2, plan_two, chunk)
        self.gather_sib(self.gg, plan_go)
        self.gather_pass(self.gg, plan_go)
        self.weights_start_three("d")
        self.relayed("d")
        self.weights_done("u")

        def up(quarter):
            place = self.at_quarter(quarter)

            for block in range(4):
                lanes = pl.ds(block * hidden, hidden)
                value = (
                    jnp.dot(self.h2[place, :], self.wu[block], preferred_element_type=f32)
                    + self.bu[:, lanes]
                )
                square = value * value
                bend = jnp.tanh(ROOT * (value + 0.044715 * value * square))
                self.hid[place, lanes] = (0.5 * value * (1.0 + bend)).astype(low)
                slope = 0.5 * (1.0 + bend) + 0.5 * value * (1.0 - bend * bend) * ROOT * (
                    1.0 + 3.0 * 0.044715 * square
                )
                self.gu[place, lanes] = slope.astype(low)

        up(self.q)
        self.gather_sib(self.h2, plan_two)
        up(self.q_sib)
        self.weights_three("d", (near,))
        self.gather_pass(self.h2, plan_two)
        up(self.q_x)
        self.weights_three("d", (4 - near,))
        self.gather_last(self.h2, plan_two)
        up(self.q_d)
        flat_down = lambda: self.wd[...].reshape(4 * hidden, width)
        grad_out = self.gg[own_rows, :].astype(f32)
        self.sums[5:6, :] = jnp.sum(grad_out, axis=0, keepdims=True)
        self.gather_last(self.gg, plan_go)

        def down_grad(block, carry):
            lanes = pl.ds(pl.multiple_of(block * hidden, hidden), hidden)
            self.dd[block] = dot_first(self.hid[:, lanes], self.gg[...]).astype(low)
            return carry

        lax.fori_loop(0, 4, down_grad, 0)
        self.grads_one("d")
        self.weights_done("d")

        def to_up(quarter):
            place = self.at_quarter(quarter)
            value = dot_last(self.gg[place, :], flat_down())
            self.gu[place, :] = (self.gu[place, :].astype(f32) * value).astype(low)

        for quarter in (self.q_d, self.q_x, self.q_sib, self.q):
            to_up(quarter)
        self.grads_two("d", (2,))

        def two_part(quarter):
            place = self.at_quarter(quarter)
            return sum(
                dot_last(self.gu[place, pl.ds(block * hidden, hidden)], self.wu[block])
                for block in range(4)
            )

        started = self.scatter_start(two_part, self.own_a, 0, self.rx.at[0])

        self.grads_two("d", (1,))
        step = width // 4

        def up_grad(block, carry):
            lanes = pl.ds(pl.multiple_of(block * step, step), step)
            value = dot_first(self.h2[:, lanes], self.gu[...]).astype(low)
            for plane in range(4):
                self.du[plane, lanes, :] = value[:, plane * hidden : (plane + 1) * hidden]
            return carry

        lax.fori_loop(0, 4, up_grad, 0)
        self.grads_one("u")
        started_down = self.scatter_start(
            lambda quarter: jnp.dot(
                self.hid[self.at_quarter(quarter), :], flat_down(), preferred_element_type=f32
            ),
            self.own_b,
            1,
            self.rx.at[1],
            hold=True,
        )
        self.grads_two("d", (3, 0))
        totals = [0.0] * 3
        for chunk in range(CH):
            part = self.at_chunk(chunk)
            grad_two = self.scatter_chunk(started, self.own_a, chunk)
            normed = self.n2[part, :]
            middle = self.gg[self.at_quarter(self.q, chunk), :].astype(f32) + norm_back(
                grad_two, normed, self.i2[part, :], gain_two
            )
            self.gm[part, :] = middle
            self.ga[self.at_quarter(self.q, chunk), :] = middle.astype(low)
            self.gather_send(self.ga, plan_mid, chunk)
            for place, value in enumerate((grad_two * normed, grad_two, middle)):
                totals[place] = totals[place] + jnp.sum(value, axis=0, keepdims=True)
        self.sums[3:4, :] = totals[0]
        self.sums[4:5, :] = totals[1]
        self.sums[2:3, :] = totals[2]
        self.scatter_send(started_down)
        up_sum = jnp.sum(self.gu[...].astype(f32), axis=0, keepdims=True)
        lanes = self.part
        for place in range(8):
            self.cb[place // 2, 1 + place % 2 : 2 + place % 2, :] = up_sum[
                :, place * lanes : (place + 1) * lanes
            ]
        def to_heads(quarter):
            place = self.at_quarter(quarter)
            value = dot_last(self.ga[place, :], flat_out()).astype(low)
            for head in range(heads):
                self.hh[head, place, :] = value[:, head * dim : (head + 1) * dim]

        to_heads(self.q)
        self.gather_sib(self.ga, plan_mid)
        to_heads(self.q_sib)
        self.grads_two("u", (2,))
        self.gather_pass(self.ga, plan_mid)
        to_heads(self.q_x)
        self.grads_two("u", (1,))
        self.gather_last(self.ga, plan_mid)
        to_heads(self.q_d)
        self.do[...] = dot_first(self.ho[...], self.ga[...]).astype(low).reshape(self.do.shape)
        self.grads_one("o")

        self.head_y, self.head_z = self.sem(4), self.sem(3)

        def attend_back(step, carry):
            head = (self.z + 1 + step) % 4
            self.ka[...] = jnp.zeros_like(self.ka)
            self.va[...] = jnp.zeros_like(self.va)
            for block in quarters:
                place = pl.ds(block * rows, rows)
                query = self.qh[head, place, :]
                grads = self.hh[head, place, :]
                probs, values = [], []
                inner = 0.0
                for first, count in parts_of(block):
                    span = pl.ds(first, count)
                    prob = self.pb[block][head, :, span]
                    value = dot_last(grads, self.vh[head, span, :])
                    self.va[span, :] += dot_first(prob, grads)
                    prob = prob.astype(f32)
                    inner = inner + jnp.sum(prob * value, axis=1, keepdims=True)
                    probs.append(prob)
                    values.append(value)
                result = 0.0
                for (first, count), prob, value in zip(parts_of(block), probs, values):
                    span = pl.ds(first, count)
                    score = (prob * (value - inner)).astype(low)
                    result = result + jnp.dot(
                        score, self.kh[head, span, :], preferred_element_type=f32
                    )
                    self.ka[span, :] += dot_first(score, query)
                self.qh[head, place, :] = (result * 0.125).astype(low)
            self.gp[head, :, 0:dim] = self.qh[head]
            self.gp[head, :, dim : 2 * dim] = self.ka[...].astype(low)
            self.gp[head, :, 2 * dim :] = self.va[...].astype(low)
            self.dq[head] = dot_first(self.gp[head], self.h1[...]).astype(low)
            self.head_one(step, head)

            @pl.when(step == 0)
            def _():
                self.grads_two("u", (3, 0))

            @pl.when(step == 2)
            def _():
                self.grads_two("o")

            @pl.when(step == 1)
            def _():
                for chunk in range(CH):
                    part = self.at_chunk(chunk)
                    summed = self.scatter_chunk(started_down, self.own_b, chunk)
                    self.ox[part, :] = (self.mid[part, :] + summed + bias_down).astype(low)
                self.move_start(self.ox, self.out, False, move[2])

            return carry

        lax.fori_loop(0, heads, attend_back, 0)
        self.swaps["q"] = [self.head_z + step for step in range(3)]
        for step in range(4):
            self.later(lambda: self.cut("q", self.dq, 0, self.span(0)), self.head_y + step)
        for step in range(3):
            self.later(lambda: self.zq.at[0], self.head_z + step)
        started = self.scatter_start(
            lambda quarter: sum(
                jnp.dot(
                    self.gp[head, self.at_quarter(quarter), :],
                    self.wq[head],
                    preferred_element_type=f32,
                )
                for head in range(heads)
            ),
            self.own_a,
            0,
            self.rx.at[0],
        )
        for step in range(3):
            head = (self.z + 1 + step) % 4
            self.head_add(step, head)
            self.head_two(step, head)
        for head in range(heads):
            total = jnp.sum(self.gp[head].astype(f32), axis=0, keepdims=True)
            self.cb[head, 0:1, 0:dim] = total[:, 0:dim]
            self.cb[head, 0:1, dim:] = total[:, 2 * dim :]
            self.cb[head, 3:, :] = jnp.zeros((5, self.part), f32)
        self.grads_three("d")
        self.head_add(3, self.z)
        totals = [0.0] * 2
        for chunk in range(CH):
            part = self.at_chunk(chunk)
            grad_one = self.scatter_chunk(started, self.own_a, chunk)
            normed = self.n1[part, :]
            self.xs[part, :] = (
                self.gm[part, :] + norm_back(grad_one, normed, self.i1[part, :], gain_one)
            ).astype(low)
            for place, value in enumerate((grad_one * normed, grad_one)):
                totals[place] = totals[place] + jnp.sum(value, axis=0, keepdims=True)
        self.sums[0:1, :] = totals[0]
        self.sums[1:2, :] = totals[1]
        self.sums[6:8, :] = jnp.zeros((2, width), f32)
        self.back_one()
        self.move_start(self.xs, self.gtok, False, move[3])
        self.grads_three("u")
        self.grads_three("o")
        self.back_two()
        self.grads_three("q")
        for kind in "duoq":
            self.grads_done(kind)
        self.move_wait(self.ox, self.out, move[2])
        self.back_three()
        self.move_wait(self.xs, self.gtok, move[3])
        self.drain()

    def mask_blocks(self):
        rows = self.rows
        begins = self.lb[2 * self.z + self.y, 6:7, 0:4].astype(jnp.int32)
        for block in range(4):
            down = block * rows + lax.broadcasted_iota(jnp.int32, (rows, 1), 0)
            side = block * rows + lax.broadcasted_iota(jnp.int32, (1, rows), 1)

            def ids(places):
                total = jnp.zeros_like(places)
                for piece in range(4):
                    first = begins[:, piece : piece + 1]
                    inside = (places >= first) & (places < first + PIECE)
                    total = jnp.where(inside, piece + 1, total)
                return total

            mine, theirs = ids(down), ids(side)
            seen = (side <= down) | ((mine == theirs) & (mine > 0))
            self.mk[block] = jnp.where(seen, 0.0, -1e30).astype(jnp.bfloat16)


IN_NAMES = ("tok", "go", "in_q", "in_o", "in_u", "in_d", "si")
OUT_NAMES = ("out", "gtok", "eq", "eo", "eu", "ed", "fs", "fb")


def fused_layer(tok, go, in_q, in_o, in_u, in_d, si):
    rows, width = tok.shape
    heads, dim = 4, width // 16
    hidden = in_u.shape[1] // 4
    part = width // 8
    n = 4 * rows
    low, f32 = jnp.bfloat16, jnp.float32
    scratch = dict(
        xs=((rows, width), low),
        mid_x=((rows, width), low),
        wq=((4, 3 * dim, width), low),
        wo=((4, dim, width), low),
        wu=((4, width, hidden), low),
        wd=((4, hidden, width), low),
        h1=((n, width), low),
        h2=((n, width), low),
        gg=((n, width), low),
        ga=((n, width), low),
        qh=((heads, n, dim), low),
        kh=((heads, n, dim), low),
        vh=((heads, n, dim), low),
        hh=((heads, n, dim), low),
        ho=((n, heads * dim), low),
        gp=((heads, n, 3 * dim), low),
        ka=((n, dim), f32),
        va=((n, dim), f32),
        mk=((4, rows, rows), low),
        n1=((rows, width), f32),
        n2=((rows, width), f32),
        mid=((rows, width), f32),
        gm=((rows, width), f32),
        i1=((rows, 1), f32),
        i2=((rows, 1), f32),
        own_a=((rows, width), f32),
        own_b=((rows, width), f32),
        hid=((n, 4 * hidden), low),
        gu=((n, 4 * hidden), low),
        ox=((rows, width), low),
        rs=((2, 5, rows, width), low),
        rx=((2, rows, width), low),
        dq=((4, 3 * dim, width), low),
        do=((4, dim, width), low),
        du=((4, width, hidden), low),
        dd=((4, hidden, width), low),
        yq=((4, 3 * dim, 4 * part), low),
        yo=((4, dim, 4 * part), low),
        yu=((4, 4 * part, hidden), low),
        yd=((4, hidden, 4 * part), low),
        zq=((3, 3 * dim, 4 * part), low),
        zo=((3, dim, 4 * part), low),
        zu=((3, 4 * part, hidden), low),
        zd=((3, hidden, 4 * part), low),
        fq=((3 * dim, 4 * part), low),
        fo=((dim, 4 * part), low),
        fu=((4 * part, hidden), low),
        fd=((hidden, 4 * part), low),
        small=((8, width), f32),
        sums=((8, width), f32),
        bq=((4, 1, 3 * dim), f32),
        bu=((1, 4 * hidden), f32),
        sma=((4, 5, 8, part), f32),
        lb=((8, 8, part), f32),
        bb=((8, 4, 8, part), f32),
        cs=((8, 8, part), f32),
        cr=((8, 8, part), f32),
        cb=((4, 8, part), f32),
        cd=((8, 4, 8, part), f32),
        es=((4, 8, part), f32),
        ed_small=((4, 4, 8, part), f32),
        eb=((4, 4, 8, part), f32),
    )
    probs = [((heads, rows, (block + 1) * rows), low) for block in range(4)]
    names = IN_NAMES + OUT_NAMES + tuple(scratch)

    def kernel(*refs):
        count = len(names)
        state = Fused(names, refs[:count])
        state.pb = refs[count : count + 4]
        state.ssem, state.rsem, state.lsem = refs[count + 4 :]
        state.run()

    hbm = pl.BlockSpec(memory_space=pl.ANY)
    vmem = pl.BlockSpec(memory_space=pltpu.VMEM)
    return pl.pallas_call(
        kernel,
        out_shape=(
            jax.ShapeDtypeStruct((rows, width), low),
            jax.ShapeDtypeStruct((rows, width), low),
            jax.ShapeDtypeStruct((4, 3 * dim, part), low),
            jax.ShapeDtypeStruct((4, dim, part), low),
            jax.ShapeDtypeStruct((4, part, hidden), low),
            jax.ShapeDtypeStruct((4, hidden, part), low),
            jax.ShapeDtypeStruct((8, part), f32),
            jax.ShapeDtypeStruct((4, 8, part), f32),
        ),
        in_specs=[hbm] * 6 + [vmem],
        out_specs=(hbm,) * 6 + (vmem,) * 2,
        scratch_shapes=[pltpu.VMEM(*spec) for spec in scratch.values()]
        + [pltpu.VMEM(*spec) for spec in probs]
        + [pltpu.SemaphoreType.DMA((SEMS,))] * 3,
        name="fused_layer",
        compiler_params=pltpu.CompilerParams(
            collective_id=0, has_side_effects=True, vmem_limit_bytes=VMEM_LIMIT
        ),
    )(tok, go, in_q, in_o, in_u, in_d, si)


def finish(out, gtok, eq, eo, eu, ed, fs, fb):
    rows, width = out.shape
    part = eq.shape[2]
    bit = part // 4
    f32 = jnp.float32

    def kernel(out_ref, gtok_ref, eq_ref, eo_ref, eu_ref, ed_ref, fs_ref, fb_ref, *ends):
        ends[0][...] = out_ref[...]
        ends[1][...] = gtok_ref[...]
        deep, wide = eq_ref.shape[1], eu_ref.shape[2]
        for member in range(4):
            ends[2][:, member * deep : (member + 1) * deep] = eq_ref[member].astype(f32).T
            ends[4][:, member * wide : (member + 1) * wide] = eu_ref[member].astype(f32)
        ends[3][...] = eo_ref[...].reshape(ends[3].shape).astype(f32)
        ends[5][...] = ed_ref[...].reshape(ends[5].shape).astype(f32)
        z = lax.axis_index("tensor")
        mine = fs_ref[:, 0:bit]
        for plane in range(1, 4):
            mine = jnp.where(z == plane, fs_ref[:, plane * bit : (plane + 1) * bit], mine)
        for row in range(6):
            ends[6 + row][...] = mine[row]
        dp, deep = lax.axis_index("dp"), part // 16
        for end, first, count in ((ends[12], 0, 1), (ends[13], 1, 2)):
            spread = jnp.concatenate(
                [
                    jnp.broadcast_to(fb_ref[member, first + half : first + half + 1, :], (deep, part))
                    for member in range(4)
                    for half in range(count)
                ]
            )
            row = lax.broadcasted_iota(jnp.int32, spread.shape, 0) % deep
            lane = lax.broadcasted_iota(jnp.int32, spread.shape, 1)
            for side in range(2):
                kept = jnp.where(lane == row * 16 + 2 * dp + side, spread, 0.0)
                end[side : side + 1, :] = lax.dot_general(
                    jnp.ones((1, part), f32),
                    kept,
                    (((1,), (1,)), ((), ())),
                    precision=lax.Precision.HIGHEST,
                    preferred_element_type=f32,
                )

    shapes = [
        out,
        gtok,
        jax.ShapeDtypeStruct((part, 4 * eq.shape[1]), f32),
        jax.ShapeDtypeStruct((4 * eo.shape[1], part), f32),
        jax.ShapeDtypeStruct((part, 4 * eu.shape[2]), f32),
        jax.ShapeDtypeStruct((4 * ed.shape[1], part), f32),
    ] + [jax.ShapeDtypeStruct((bit,), f32)] * 6
    shapes += [jax.ShapeDtypeStruct((2, size), f32) for size in (part // 4, part // 2)]
    return pl.pallas_call(
        kernel,
        out_shape=[jax.ShapeDtypeStruct(shape.shape, shape.dtype) for shape in shapes],
        in_specs=[pl.BlockSpec(memory_space=pltpu.VMEM)] * 8,
        out_specs=[pl.BlockSpec(memory_space=pltpu.VMEM)] * 14,
        name="finish",
    )(out, gtok, eq, eo, eu, ed, fs, fb)


SEMS = 256
VMEM_LIMIT = 67043328


def per_device_fused(
    tokens_in, starts, ln1_gain, ln1_bias, w_qkv, b_qv, w_out, b_out,
    ln2_gain, ln2_bias, w_up, b_up, w_down, b_down, grad_out,
):
    rows, width = tokens_in.shape
    f32 = jnp.float32
    dp, z = lax.axis_index("dp"), lax.axis_index("tensor")
    part = width // 8
    dim = width // 16
    hidden = w_up.shape[1] // 4
    bit = ln1_gain.shape[0]
    here = jnp.arange(part) // bit == z
    vectors = jnp.stack([ln1_gain, ln1_bias, b_out, ln2_gain, ln2_bias, b_down])
    vectors = jnp.where(here, jnp.tile(vectors, (1, part // bit)), 0.0)
    begins = jnp.where(z == 0, starts.astype(f32), 0.0)
    begins = jnp.pad(begins, ((0, 1), (0, part - 4)))
    spot = (jnp.arange(8) == dp)[:, None]

    def spread(bias):
        entries = bias.astype(f32).reshape(4, -1, 1, bias.shape[1])
        return jnp.where(spot, entries, 0.0).reshape(4, -1, part)

    biases = jnp.concatenate(
        [spread(b_qv), spread(b_up), jnp.zeros((4, 5, part), f32)], axis=1
    )
    si = jnp.concatenate([jnp.concatenate([vectors, begins])[None], biases])
    in_q = w_qkv.reshape(part, 4, 3 * dim).transpose(1, 2, 0)
    in_o = w_out.reshape(4, dim, part)
    in_d = w_down.reshape(4, hidden, part)
    out, gtok, eq, eo, eu, ed, fs, fb = fused_layer(
        tokens_in, grad_out, in_q, in_o, w_up, in_d, si
    )
    out, gtok, grad_w_qkv, grad_w_out, grad_w_up, grad_w_down, *take = finish(
        out, gtok, eq, eo, eu, ed, fs, fb
    )
    grad_b_qv, grad_b_up = take[6].T, take[7].T
    return (
        out, gtok, take[0], take[1], grad_w_qkv, grad_b_qv, grad_w_out, take[2],
        take[3], take[4], grad_w_up, grad_b_up, grad_w_down, take[5],
    )


def solution(mesh):
    sizes = (mesh.shape["dp"], mesh.shape["tensor"])

    def layer(tokens_in, starts, *others):
        fits = sizes == (8, 4) and tokens_in.shape[0] == PIECE and starts.shape == (1, 4)
        return (per_device_fused if fits else per_device)(tokens_in, starts, *others)

    return jax.shard_map(
        layer,
        mesh=mesh,
        in_specs=(
            P(("dp", "tensor"), None),
            P("dp", None),
            P(("dp", "tensor")),
            P(("dp", "tensor")),
            P("dp", "tensor"),
            P("tensor", "dp"),
            P("tensor", "dp"),
            P(("dp", "tensor")),
            P(("dp", "tensor")),
            P(("dp", "tensor")),
            P("dp", "tensor"),
            P("tensor", "dp"),
            P("tensor", "dp"),
            P(("dp", "tensor")),
            P(("dp", "tensor"), None),
        ),
        out_specs=(
            P(("dp", "tensor"), None),
            P(("dp", "tensor"), None),
            P(("dp", "tensor")),
            P(("dp", "tensor")),
            P("dp", "tensor"),
            P("tensor", "dp"),
            P("tensor", "dp"),
            P(("dp", "tensor")),
            P(("dp", "tensor")),
            P(("dp", "tensor")),
            P("dp", "tensor"),
            P("tensor", "dp"),
            P("tensor", "dp"),
            P(("dp", "tensor")),
        ),
        check_vma=False,
    )
```
